128 devices in a mesh: dp: 1, cp: 128 (over z, y, x, core).
Axes of the slice: x: 4, y: 4, z: 4, core: 2. Of those that a mesh axis runs over, the one named last changes fastest.
Arguments:
- query: bfloat16 [6, 4096, 16, 128], P('dp', 'cp')
- key: bfloat16 [6, 4096, 128], P('dp', 'cp')
- value: bfloat16 [6, 4096, 128], P('dp', 'cp')
- positions: int32 [4096], P(('dp', 'cp'))
- grad_out: bfloat16 [6, 4096, 16, 128], P('dp', 'cp')
Outputs:
- output 1: bfloat16 [6, 4096, 16, 128], P('dp', 'cp')
- output 2: bfloat16 [6, 4096, 16, 128], P('dp', 'cp')
- output 3: bfloat16 [6, 4096, 128], P('dp', 'cp')
- output 4: bfloat16 [6, 4096, 128], P('dp', 'cp')
All inputs are finite; a program needn't handle non-finite values.
Results may differ from the reference program's by a relative error of at most 0.00808827.
Values are sent between devices in bfloat16 or wider.
A program may use at most 1 GiB of HBM per device.

```python
import jax
import jax.numpy as jnp
from jax import lax

BATCH = 6
SEQ = 4096
HEADS = 16
HEAD = 128
QROWS = 8
ROPE_BASE = 10000


def setup_inputs(seed: int = 0, part: int = 0) -> dict:
    part_key = jax.random.fold_in(jax.random.key(seed), part)
    rng_keys = jax.random.split(part_key, 6)
    query = jax.random.normal(rng_keys[0], (BATCH, SEQ, HEADS, HEAD), jnp.float32)
    key = jax.random.normal(rng_keys[1], (BATCH, SEQ, HEAD), jnp.float32)
    value = jax.random.normal(rng_keys[2], (BATCH, SEQ, HEAD), jnp.float32)
    start = jax.random.randint(rng_keys[3], (), 0, 256)
    increments = jax.random.randint(rng_keys[4], (SEQ,), 0, 2)
    positions = (start + jnp.cumsum(increments)).astype(jnp.int32)
    grad_out = jax.random.normal(rng_keys[5], (BATCH, SEQ, HEADS, HEAD), jnp.float32)
    return {'query': query.astype(jnp.bfloat16), 'key': key.astype(jnp.bfloat16), 'value': value.astype(jnp.bfloat16), 'positions': positions, 'grad_out': grad_out.astype(jnp.bfloat16)}


def rope_tables(positions):
    half_dim = HEAD // 2
    inv_freq = jnp.power(jnp.float32(ROPE_BASE), -2.0 * jnp.arange(half_dim, dtype=jnp.float32) / HEAD)
    angles = positions.astype(jnp.float32)[..., None] * inv_freq
    angles = jnp.concatenate([angles, angles], axis=-1)
    return jnp.cos(angles), jnp.sin(angles)


def rotate(values, cos_tab, sin_tab):
    half_dim = values.shape[-1] // 2
    turned = jnp.concatenate([-values[..., half_dim:], values[..., :half_dim]], axis=-1)
    return values * cos_tab + turned * sin_tab


def reference(query, key, value, positions, grad_out):
    cos_tab, sin_tab = rope_tables(positions)
    cos_q = cos_tab[None, :, None, :]
    sin_q = sin_tab[None, :, None, :]
    query_rot = rotate(query.astype(jnp.float32), cos_q, sin_q).astype(jnp.bfloat16)
    key_rot = rotate(key.astype(jnp.float32), cos_tab[None], sin_tab[None]).astype(jnp.bfloat16)
    scale = HEAD ** -0.5
    key_f = key_rot.astype(jnp.float32)
    value_f = value.astype(jnp.float32)
    key_idx = jnp.arange(SEQ)
    block_count = SEQ // QROWS
    query_blocks = query_rot.reshape(BATCH, block_count, QROWS, HEADS, HEAD).transpose(1, 0, 2, 3, 4)
    grad_blocks = grad_out.reshape(BATCH, block_count, QROWS, HEADS, HEAD).transpose(1, 0, 2, 3, 4)

    def one_block(carry, block):
        dkey_acc, dvalue_acc = carry
        query_blk, grad_blk, block_idx = block
        query_f = query_blk.astype(jnp.float32)
        grad_f = grad_blk.astype(jnp.float32)
        query_idx = block_idx * QROWS + jnp.arange(QROWS)
        causal_mask = (key_idx[None, :] <= query_idx[:, None])[None, :, None, :]
        scores = jnp.where(causal_mask, jnp.einsum('bqhd,bkd->bqhk', query_f, key_f) * scale, -jnp.inf)
        row_max = jnp.max(scores, axis=-1, keepdims=True)
        weights = jnp.exp(scores - row_max)
        row_sum = jnp.sum(weights, axis=-1, keepdims=True)
        attn_f = jnp.einsum('bqhk,bkd->bqhd', weights.astype(jnp.bfloat16).astype(jnp.float32), value_f) / row_sum
        attn_blk = attn_f.astype(jnp.bfloat16)
        probs_f = jnp.exp(scores - (row_max + jnp.log(row_sum)))
        delta = jnp.sum(grad_f * attn_blk.astype(jnp.float32), axis=-1, keepdims=True)
        dprobs = jnp.einsum('bqhd,bkd->bqhk', grad_f, value_f)
        dscore = (probs_f * (dprobs - delta)).astype(jnp.bfloat16).astype(jnp.float32)
        dquery_blk = jnp.einsum('bqhk,bkd->bqhd', dscore, key_f) * scale
        dkey_acc = dkey_acc + jnp.einsum('bqhk,bqhd->bkd', dscore, query_f) * scale
        dvalue_acc = dvalue_acc + jnp.einsum('bqhk,bqhd->bkd', probs_f.astype(jnp.bfloat16).astype(jnp.float32), grad_f)
        return (dkey_acc, dvalue_acc), (attn_blk, dquery_blk)

    zero_kv = jnp.zeros((BATCH, SEQ, HEAD), jnp.float32)
    sums, outs = lax.scan(one_block, (zero_kv, zero_kv), (query_blocks, grad_blocks, jnp.arange(block_count)))
    attn_out = outs[0].transpose(1, 0, 2, 3, 4).reshape(BATCH, SEQ, HEADS, HEAD)
    dquery_rot = outs[1].transpose(1, 0, 2, 3, 4).reshape(BATCH, SEQ, HEADS, HEAD)
    grad_query = rotate(dquery_rot, cos_q, -sin_q).astype(jnp.bfloat16)
    grad_key = rotate(sums[0], cos_tab[None], -sin_tab[None]).astype(jnp.bfloat16)
    grad_value = sums[1].astype(jnp.bfloat16)
    return (attn_out, grad_query, grad_key, grad_value)
```

```python
import jax
import jax.numpy as jnp
from jax import lax
from jax.experimental import pallas as pl
from jax.experimental.pallas import tpu as pltpu
from jax.sharding import PartitionSpec as PS

ROPE_BASE = 10000
SEQS, HEADS, HEAD, BLK = 6, 16, 128, 32
ROWS = BLK * HEADS
CK = 256
STEPS = 17
NC = 16
UF, UB = 4, 4
SCALE = HEAD ** -0.5
C2 = SCALE * 1.4426950408889634
BIG = 1e30
BF, F32 = jnp.bfloat16, jnp.float32
MESH = pl.DeviceIdType.MESH

PLACE = [int(d, 16) for d in 'E45C2760D389FA1B']
ORDER = [[int(d, 16) for d in row] for row in (
    '530142768E9ADBCF',
    'CD8907162534BAFE',
    'F9E8A54BDC263701',
    'A52B34867901FDCE',
    'F9BAE538201746DC',
    'ABCD452130F867E9')]
PIECES = 4
PP = 16 // PIECES


def _tables():
    work = {}
    dest = [[0] * 16 for _ in range(SEQS)]
    limit = {}
    slots = {}
    for s in range(SEQS):
        for i, j in enumerate(ORDER[s]):
            q = 16 * (s % 3) + i
            f, g = divmod(q, 3)
            big_c = 8 * (s // 3) + f // 2
            slot = s % 3 - (6 * (f // 2)) // 16
            slots[big_c, s] = slot
            work[PLACE[big_c], f % 2, g] = (s, j, slot)
            dest[s][j] = PLACE[big_c] * 8 + (f % 2) * 4 + g
            limit[big_c, s] = max(limit.get((big_c, s), 0), ((31 - j) // 2) // PP)
    chips = [[(PLACE[c], slots[c, t], limit[c, t]) for (c, t) in sorted(slots) if t == s] for s in range(SEQS)]
    lim = [[-1] * 16, [-1] * 16]
    seq = [[0] * 16, [0] * 16]
    nth = [[0] * 16, [0] * 16]
    for s in range(SEQS):
        for n, (place, slot, last) in enumerate(chips[s]):
            lim[slot][place], seq[slot][place], nth[slot][place] = last, s, n
    meta = []
    for p in range(32):
        w = [work[p // 2, p % 2, g] for g in range(3)]
        meta.append([t[1] for t in w] + [t[2] for t in w] + [2 if lim[1][p // 2] >= 0 else 1] + [t[0] for t in w])
    return dest, chips, lim, seq, nth, meta


DEST, CHIPS, LIM, SEQ, NTH, META = _tables()
NCH = max(len(c) for c in CHIPS)


def lut(index, table):
    value = jnp.int32(table[0])
    for n in range(1, len(table)):
        if table[n] != table[n - 1]:
            value = jnp.where(index >= n, jnp.int32(table[n]), value)
    return value


def place_of():
    me = lax.axis_index('cp')
    return me, me % 2, (me // 2) % 4, me // 8


def send(src, dst, ssem, rsem, dev, me):
    @pl.when(dev != me)
    def _():
        pltpu.make_async_remote_copy(src, dst, ssem, rsem, device_id={'cp': dev}, device_id_type=MESH).start()

    @pl.when(dev == me)
    def _():
        pltpu.make_async_copy(src, dst, rsem).start()


def landed(ref, sem):
    pltpu.make_async_copy(ref, ref, sem).wait()


def exchange_in(q, do, kv, cs, qr, dor, csr, kvr, ts, tr, s1, r1, s2, r2, s3, r3):
    me, c, x, place = place_of()
    p = 2 * place + c
    j = jnp.minimum(p, 31 - p)
    hi = p // 16
    lims = [lut(place, LIM[slot]) for slot in range(2)]
    piece_me = place // PP

    n = 0
    for s in range(SEQS):
        for (chip, slot, last) in CHIPS[s]:
            @pl.when(piece_me <= last)
            def _(s=s, chip=chip, slot=slot, n=n):
                send(kv.at[s], kvr.at[slot, place, x, c], s1.at[n], r1.at[slot, piece_me], chip * 8 + 2 * x + c, me)
            n += 1
    for s in range(SEQS):
        code = lut(j, DEST[s])
        k = 2 * (code % 4) + hi
        dev = (code // 8) * 8 + 2 * x + (code // 4) % 2
        send(q.at[s], qr.at[k], ts.at[s, 0], tr.at[k, 0], dev, me)
        send(do.at[s], dor.at[k], ts.at[s, 1], tr.at[k, 1], dev, me)
        send(cs, csr.at[k], ts.at[s, 2], tr.at[k, 2], dev, me)

    def mine(slot, i, xx, cc):
        return kvr.at[slot, pl.ds(PP * i, PP), xx, cc]

    def both(slot, i, cc):
        return kvr.at[slot, pl.ds(PP * i, PP), :, cc]

    for i in range(PIECES):
        for slot in range(2):
            @pl.when(i <= lims[slot])
            def _(i=i, slot=slot):
                landed(mine(slot, i, x, c), r1.at[slot, i])
                for d in range(1, 4):
                    pltpu.make_async_remote_copy(
                        mine(slot, i, x, c), mine(slot, i, x, c), s2.at[slot, i, d - 1], r2.at[slot, i, d - 1],
                        device_id={'cp': place * 8 + 2 * ((x + d) % 4) + c}, device_id_type=MESH).start()
    for i in range(PIECES):
        for slot in range(2):
            @pl.when(i <= lims[slot])
            def _(i=i, slot=slot):
                for d in range(1, 4):
                    landed(mine(slot, i, (x + 4 - d) % 4, c), r2.at[slot, i, d - 1])
                pltpu.make_async_remote_copy(
                    both(slot, i, c), both(slot, i, c), s3.at[slot, i], r3.at[slot, i],
                    device_id={'cp': me + 1 - 2 * c}, device_id_type=MESH).start()
    for k in range(6):
        landed(qr.at[k], tr.at[k, 0])
        landed(dor.at[k], tr.at[k, 1])
        landed(csr.at[k], tr.at[k, 2])
    for i in range(PIECES):
        for slot in range(2):
            @pl.when(i <= lims[slot])
            def _(i=i, slot=slot):
                landed(both(slot, i, 1 - c), r3.at[slot, i])
                for d in range(1, 4):
                    landed(mine(slot, i, x, c), s2.at[slot, i, d - 1])
                landed(both(slot, i, c), s3.at[slot, i])
    n = 0
    for s in range(SEQS):
        for (chip, slot, last) in CHIPS[s]:
            @pl.when((piece_me <= last) & (place != chip))
            def _(s=s, n=n):
                landed(kv.at[s], s1.at[n])
            n += 1
    for s in range(SEQS):
        code = lut(j, DEST[s])
        dev = (code // 8) * 8 + 2 * x + (code // 4) % 2

        @pl.when(dev != me)
        def _(s=s):
            landed(q.at[s], ts.at[s, 0])
            landed(do.at[s], ts.at[s, 1])
            landed(cs, ts.at[s, 2])


def run_in(q, do, kv, cs):
    dma = pltpu.SemaphoreType.DMA
    n_kv = sum(len(c) for c in CHIPS)
    any_ = pl.BlockSpec(memory_space=pl.ANY)
    return pl.pallas_call(
        exchange_in,
        in_specs=[any_] * 4, out_specs=[any_] * 4,
        out_shape=[
            jax.ShapeDtypeStruct((6, ROWS, HEAD), BF), jax.ShapeDtypeStruct((6, ROWS, HEAD), BF),
            jax.ShapeDtypeStruct((6, BLK, HEAD), F32), jax.ShapeDtypeStruct((2, 16, 4, 2, BLK, 2 * HEAD), BF)],
        scratch_shapes=[dma((6, 3)), dma((6, 3)), dma((n_kv,)), dma((2, PIECES)), dma((2, PIECES, 3)), dma((2, PIECES, 3)),
                        dma((2, PIECES)), dma((2, PIECES))],
        compiler_params=pltpu.CompilerParams(has_side_effects=True, vmem_limit_bytes=63 << 20),
        name='exchange_in')(q, do, kv, cs)


def dot(a, b):
    return jnp.dot(a, b, preferred_element_type=F32)


def dot_nt(a, b):
    return lax.dot_general(a, b, (((1,), (1,)), ((), ())), preferred_element_type=F32)


def max8(v):
    return jnp.broadcast_to(jnp.max(v, axis=0, keepdims=True), (8, ROWS))


def sum8(v):
    return jnp.broadcast_to(jnp.sum(v, axis=0, keepdims=True), (8, ROWS))


def sub8(a, b):
    return a.reshape(-1, 8, ROWS) - b[None]


def turn(v, cs, sign):
    cos = jnp.concatenate([cs[:, :64], cs[:, :64]], axis=1)
    sin = jnp.concatenate([-cs[:, 64:], cs[:, 64:]], axis=1)
    v = v.reshape(BLK, HEADS, HEAD)
    other = jnp.concatenate([v[..., 64:], v[..., :64]], axis=-1)
    if sign > 0:
        out = v * cos[:, None, :] + other * sin[:, None, :]
    else:
        out = v * cos[:, None, :] - other * sin[:, None, :]
    return out.astype(BF).reshape(ROWS, HEAD)


def attend(meta, q_ref, do_ref, cs_ref, kv_ref, o_ref, dq_ref, dkv_ref,
           kt, vt, dkt, dvt, p_ref, mx, qa, dot_t, ot, dqt, mst, lst, dst, dp_ref, mk):
    g = pl.program_id(0)
    xw = meta[7]

    def rows(ch):
        return pl.ds(pl.multiple_of(ch * CK, CK), CK)

    @pl.when(g == 0)
    def _():
        @pl.loop(0, NC * meta[6])
        def _(i):
            s = i // NC
            ch = i % NC
            kt[s, ch] = kv_ref[s, rows(ch), :HEAD].T
            vt[s, ch] = kv_ref[s, rows(ch), HEAD:].T
            dkt[s, ch] = jnp.zeros((HEAD, CK), F32)
            dvt[s, ch] = jnp.zeros((HEAD, CK), F32)
        row = lax.broadcasted_iota(jnp.int32, (HEAD, ROWS), 0)
        col = lax.broadcasted_iota(jnp.int32, (HEAD, ROWS), 1)
        onehot = jnp.where(col // HEADS == row, 1.0, 0.0).astype(BF)
        for tl in range(2):
            qa[tl, HEAD:, :] = onehot
        ki = lax.broadcasted_iota(jnp.int32, (CK, HEAD), 0)
        di = lax.broadcasted_iota(jnp.int32, (CK, HEAD), 1)
        mk[0] = jnp.zeros((CK, HEAD), BF)
        for cc in range(2):
            mk[1 + cc] = jnp.where((di < BLK) & (ki > di + 64 * xw + BLK * cc), -BIG, 0.0).astype(BF)

    j = meta[g]
    slot = meta[3 + g]
    a = j // 2 + 1

    def tlch(i):
        tl = (i >= a).astype(jnp.int32)
        return tl, i - a * tl

    @pl.loop(0, 2)
    def _(tl):
        qa[tl, :HEAD, :] = turn(q_ref[tl].astype(F32), cs_ref[tl], 1).T
        dot_t[tl] = do_ref[tl].T
        ot[tl] = jnp.zeros((HEAD, ROWS), F32)
        dqt[tl] = jnp.zeros((HEAD, ROWS), F32)
        mst[tl] = jnp.full((8, ROWS), -BIG, F32)
        lst[tl] = jnp.zeros((8, ROWS), F32)

    def s_step(i, pb, pu):
        tl, ch = tlch(i)
        diag = ch == jnp.where(tl == 0, a - 1, NC - a)
        sel = jnp.where(diag, 1 + lax.rem(j + tl, 2), 0)
        ka = jnp.concatenate([kv_ref[slot, rows(ch), :HEAD], mk[sel]], axis=1)
        s = dot(ka, qa[tl]) * C2
        p_ref[pb, pu] = s
        mx[i] = jnp.max(s.reshape(CK // 8, 8, ROWS), axis=0)

    def o_step(i, pb, pu):
        tl, ch = tlch(i)
        mo = mst[tl]
        mn = jnp.maximum(mo, max8(mx[i]))
        al = jnp.exp2(mo - mn)
        e = jnp.exp2(sub8(p_ref[pb, pu], mn))
        mst[tl] = mn
        lst[tl] = lst[tl] * al + jnp.sum(e, axis=0)
        ot[tl] = (ot[tl].reshape(-1, 8, ROWS) * al[None]).reshape(HEAD, ROWS) + dot(vt[slot, ch], e.reshape(CK, ROWS).astype(BF))

    s_step(jnp.int32(0), 0, 0)

    @pl.loop(0, 16 // UF)
    def _(b):
        for u in range(UF):
            i = b * UF + u
            s_step(i + 1, b + (u + 1) // UF, (u + 1) % UF)
            o_step(i, b, u)
    o_step(jnp.int32(16), 16 // UF, 0)

    @pl.loop(0, 2)
    def _(tl):
        l = sum8(lst[tl])
        o = (ot[tl].reshape(-1, 8, ROWS) / l[None]).reshape(HEAD, ROWS).astype(BF)
        o_ref[tl] = o.T
        dst[tl] = sum8(jnp.sum((o.astype(F32) * dot_t[tl].astype(F32)).reshape(-1, 8, ROWS), axis=0))
        mst[tl] = mst[tl] + jnp.log2(l)

    def d_step(i, b):
        tl, ch = tlch(i)
        dp_ref[b] = dot(kv_ref[slot, rows(ch), HEAD:], dot_t[tl])

    def g_step(i, b, pb, pu, ahead):
        tl, ch = tlch(i)
        pr = jnp.exp2(sub8(p_ref[pb, pu], mst[tl]))
        prb = pr.reshape(CK, ROWS).astype(BF)
        dvt[slot, ch] += dot_nt(dot_t[tl], prb)
        ahead()
        ds = (pr * sub8(dp_ref[b], dst[tl])).reshape(CK, ROWS).astype(BF)
        dqt[tl] += dot(kt[slot, ch], ds)
        dkt[slot, ch] += dot_nt(qa[tl, :HEAD, :], ds)

    d_step(jnp.int32(0), 0)

    @pl.loop(0, 16 // UB)
    def _(b):
        for u in range(UB):
            i = b * UB + u
            g_step(i, u % 2, b, u, lambda: d_step(i + 1, (u + 1) % 2))
    g_step(jnp.int32(16), 0, 16 // UF, 0, lambda: None)

    @pl.loop(0, 2)
    def _(tl):
        dq_ref[tl] = turn((dqt[tl] * SCALE).T, cs_ref[tl], -1)

    @pl.when(g == 2)
    def _():
        @pl.loop(0, NC * meta[6])
        def _(i):
            s = i // NC
            ch = i % NC
            dkv_ref[s, rows(ch), :HEAD] = dkt[s, ch].T
            dkv_ref[s, rows(ch), HEAD:] = dvt[s, ch].T


def run_attend(meta, q, do, cs, kv):
    tile = pl.BlockSpec((2, ROWS, HEAD), lambda i, _: (i, 0, 0))
    whole = pl.BlockSpec((2, NC * CK, 2 * HEAD), lambda i, _: (0, 0, 0), pipeline_mode=pl.Buffered(1))
    v = pltpu.VMEM
    return pl.pallas_call(
        attend,
        grid_spec=pltpu.PrefetchScalarGridSpec(
            num_scalar_prefetch=1, grid=(3,),
            in_specs=[tile, tile, pl.BlockSpec((2, BLK, HEAD), lambda i, _: (i, 0, 0)), whole],
            out_specs=[tile, tile, whole],
            scratch_shapes=[
                v((2, NC, HEAD, CK), BF), v((2, NC, HEAD, CK), BF), v((2, NC, HEAD, CK), F32), v((2, NC, HEAD, CK), F32),
                v((16 // UF + 1, UF, CK, ROWS), F32), v((STEPS, 8, ROWS), F32), v((2, 2 * HEAD, ROWS), BF), v((2, HEAD, ROWS), BF),
                v((2, HEAD, ROWS), F32), v((2, HEAD, ROWS), F32), v((2, 8, ROWS), F32), v((2, 8, ROWS), F32),
                v((2, 8, ROWS), F32), v((2, CK, ROWS), F32), v((3, CK, HEAD), BF)]),
        out_shape=[jax.ShapeDtypeStruct((6, ROWS, HEAD), BF)] * 2 + [jax.ShapeDtypeStruct((2, NC * CK, 2 * HEAD), F32)],
        compiler_params=pltpu.CompilerParams(vmem_limit_bytes=60 << 20),
        name='attend')(meta, q, do, cs, kv)


def exchange_out(o, dq, dkv, cs, att, gq, gk, gv, own, peer, xr, zs, home,
                 ls, ts, tr, s1, r1, s2, r2, s3, r3):
    me, c, x, place = place_of()
    p = 2 * place + c
    lims = [lut(place, LIM[slot]) for slot in range(2)]
    for k in range(6):
        g, tl = divmod(k, 2)
        s = lut(p, [META[n][7 + g] for n in range(32)])
        j = lut(p, [META[n][g] for n in range(32)])
        src = j if tl == 0 else 31 - j
        dev = (src // 2) * 8 + 2 * x + src % 2
        send(o.at[k], att.at[s], ts.at[k, 0], tr.at[s, 0], dev, me)
        send(dq.at[k], gq.at[s], ts.at[k, 1], tr.at[s, 1], dev, me)

    def part(slot, i):
        return pl.ds(PP * i, PP)

    for i in reversed(range(PIECES)):
        for slot in range(2):
            @pl.when(i <= lims[slot])
            def _(i=i, slot=slot):
                pltpu.make_async_remote_copy(
                    dkv.at[slot, part(slot, i), :, 1 - c], peer.at[slot, part(slot, i)], s1.at[slot, i], r1.at[slot, i],
                    device_id={'cp': me + 1 - 2 * c}, device_id_type=MESH).start()
                pltpu.make_async_copy(dkv.at[slot, part(slot, i), :, c], own.at[slot, part(slot, i)], ls.at[slot, i]).start()
    for i in reversed(range(PIECES)):
        for slot in range(2):
            @pl.when(i <= lims[slot])
            def _(i=i, slot=slot):
                landed(own.at[slot, part(slot, i)], ls.at[slot, i])
                landed(peer.at[slot, part(slot, i)], r1.at[slot, i])
                own[slot, part(slot, i)] += peer[slot, part(slot, i)]
                for d in range(1, 4):
                    pltpu.make_async_remote_copy(
                        own.at[slot, part(slot, i), (x + d) % 4], xr.at[slot, d - 1, part(slot, i)],
                        s2.at[slot, i, d - 1], r2.at[slot, i, d - 1],
                        device_id={'cp': place * 8 + 2 * ((x + d) % 4) + c}, device_id_type=MESH).start()
    seqs = [lut(place, SEQ[slot]) for slot in range(2)]
    nths = [lut(place, NTH[slot]) for slot in range(2)]
    for i in reversed(range(PIECES)):
        for slot in range(2):
            @pl.when(i <= lims[slot])
            def _(i=i, slot=slot):
                for d in range(1, 4):
                    landed(xr.at[slot, d - 1, part(slot, i)], r2.at[slot, i, d - 1])
                zs[slot, part(slot, i)] = (own[slot, part(slot, i), x] + xr[slot, 0, part(slot, i)]
                                           + xr[slot, 1, part(slot, i)] + xr[slot, 2, part(slot, i)])
                for u in range(PP):
                    to = PP * i + u
                    send(zs.at[slot, to], home.at[seqs[slot], nths[slot]], s3.at[slot, to], r3.at[seqs[slot], nths[slot]],
                         to * 8 + 2 * x + c, me)
    cos = jnp.concatenate([cs[:, :64], cs[:, :64]], axis=1)
    sin = jnp.concatenate([-cs[:, 64:], cs[:, 64:]], axis=1)
    piece_me = place // PP
    for s in range(SEQS):
        for n, (chip, slot, last) in enumerate(CHIPS[s]):
            @pl.when(piece_me <= last)
            def _(s=s, n=n):
                landed(home.at[s, n], r3.at[s, n])

            @pl.when(piece_me > last)
            def _(s=s, n=n):
                home[s, n] = jnp.zeros((BLK, 2 * HEAD), F32)
        total = home[s, 0]
        for n in range(1, len(CHIPS[s])):
            total = total + home[s, n]
        dk = total[:, :HEAD] * SCALE
        other = jnp.concatenate([dk[:, 64:], dk[:, :64]], axis=1)
        gk[s] = (dk * cos - other * sin).astype(BF)
        gv[s] = total[:, HEAD:].astype(BF)
    for s in range(SEQS):
        landed(att.at[s], tr.at[s, 0])
        landed(gq.at[s], tr.at[s, 1])
    for k in range(6):
        g, tl = divmod(k, 2)
        j = lut(p, [META[n][g] for n in range(32)])
        src = j if tl == 0 else 31 - j

        @pl.when(src != p)
        def _(k=k):
            landed(o.at[k], ts.at[k, 0])
            landed(dq.at[k], ts.at[k, 1])
    for i in range(PIECES):
        for slot in range(2):
            @pl.when(i <= lims[slot])
            def _(i=i, slot=slot):
                landed(peer.at[slot, part(slot, i)], s1.at[slot, i])
                for d in range(1, 4):
                    landed(xr.at[slot, d - 1, part(slot, i)], s2.at[slot, i, d - 1])
                for u in range(PP):
                    to = PP * i + u

                    @pl.when(to != place)
                    def _(to=to):
                        landed(zs.at[slot, to], s3.at[slot, to])


def run_out(o, dq, dkv, cs):
    dma = pltpu.SemaphoreType.DMA
    any_ = pl.BlockSpec(memory_space=pl.ANY)
    vm = pl.BlockSpec(memory_space=pltpu.VMEM)
    v = pltpu.VMEM
    return pl.pallas_call(
        exchange_out,
        in_specs=[any_] * 3 + [vm], out_specs=[any_, any_, vm, vm],
        out_shape=[
            jax.ShapeDtypeStruct((6, ROWS, HEAD), BF), jax.ShapeDtypeStruct((6, ROWS, HEAD), BF),
            jax.ShapeDtypeStruct((6, BLK, HEAD), BF), jax.ShapeDtypeStruct((6, BLK, HEAD), BF)],
        scratch_shapes=[
            v((2, 16, 4, BLK, 2 * HEAD), F32), v((2, 16, 4, BLK, 2 * HEAD), F32), v((2, 3, 16, BLK, 2 * HEAD), F32),
            v((2, 16, BLK, 2 * HEAD), F32), v((SEQS, NCH, BLK, 2 * HEAD), F32),
            dma((2, PIECES)), dma((6, 2)), dma((6, 2)), dma((2, PIECES)), dma((2, PIECES)), dma((2, PIECES, 3)), dma((2, PIECES, 3)),
            dma((2, 16)), dma((SEQS, NCH))],
        compiler_params=pltpu.CompilerParams(has_side_effects=True, vmem_limit_bytes=63 << 20),
        name='exchange_out')(o, dq, dkv, cs)


def solution(mesh):
    query_spec = PS('dp', 'cp', None, None)
    kv_spec = PS('dp', 'cp', None)
    pos_spec = PS(('dp', 'cp'))

    def per_device(query, key, value, positions, grad_out):
        me = lax.axis_index('cp')
        inv_freq = jnp.power(jnp.float32(ROPE_BASE), -2.0 * jnp.arange(HEAD // 2, dtype=F32) / HEAD)
        angles = positions.astype(F32)[:, None] * inv_freq
        cos, sin = jnp.cos(angles), jnp.sin(angles)
        cs = jnp.concatenate([cos, sin], axis=1)
        k1, k2 = key[..., :64].astype(F32), key[..., 64:].astype(F32)
        kv = jnp.concatenate([(k1 * cos - k2 * sin).astype(BF), (k2 * cos + k1 * sin).astype(BF), value], axis=-1)
        place = me // 8
        row = lax.dynamic_index_in_dim(jnp.array(META, jnp.int32), 2 * place + me % 2, 0, keepdims=False)
        meta = row.at[7].set((me // 2) % 4)
        q, do, csr, kvr = run_in(query.reshape(6, ROWS, HEAD), grad_out.reshape(6, ROWS, HEAD), kv, cs)
        o, dq, dkv = run_attend(meta, q, do, csr, kvr.reshape(2, NC * CK, 2 * HEAD))
        att, gq, gk, gv = run_out(o, dq, dkv.reshape(2, 16, 4, 2, BLK, 2 * HEAD), cs)
        return att.reshape(query.shape), gq.reshape(query.shape), gk, gv

    return jax.shard_map(per_device, mesh=mesh, in_specs=(query_spec, kv_spec, kv_spec, pos_spec, query_spec),
                         out_specs=(query_spec, query_spec, kv_spec, kv_spec), check_vma=False)
```

```python
import jax
import jax.numpy as jnp
from jax import lax
from jax.experimental import pallas as pl
from jax.experimental.pallas import tpu as pltpu
from jax.sharding import PartitionSpec as PS

ROPE_BASE = 10000
SEQS, HEADS, HEAD, BLK = 6, 16, 128, 32
ROWS = BLK * HEADS
CK = 256
ENT = 24
SLOT1 = 12
SIDX = 56
SCALE = HEAD ** -0.5
C2 = SCALE * 1.4426950408889634
BIG = 1e30
BF, F32 = jnp.bfloat16, jnp.float32
MESH = pl.DeviceIdType.MESH

PLACE = [int(d, 16) for d in 'E45C2760D389FA1B']
ORDER = [[int(d, 16) for d in row] for row in (
    '530142768E9ADBCF',
    'CD8907162534BAFE',
    'F9E8A54BDC263701',
    'A52B34867901FDCE',
    'F9BAE538201746DC',
    'ABCD452130F867E9')]
PIECES = 4
PP = 16 // PIECES


def _tables():
    work = {}
    dest = [[0] * 16 for _ in range(SEQS)]
    limit = {}
    slots = {}
    for s in range(SEQS):
        for i, j in enumerate(ORDER[s]):
            q = 16 * (s % 3) + i
            f, g = divmod(q, 3)
            big_c = 8 * (s // 3) + f // 2
            slot = s % 3 - (6 * (f // 2)) // 16
            slots[big_c, s] = slot
            work[PLACE[big_c], f % 2, g] = (s, j, slot)
            dest[s][j] = PLACE[big_c] * 8 + (f % 2) * 4 + g
            limit[big_c, s] = max(limit.get((big_c, s), 0), ((31 - j) // 2) // PP)
    chips = [[(PLACE[c], slots[c, t], limit[c, t]) for (c, t) in sorted(slots) if t == s] for s in range(SEQS)]
    lim = [[-1] * 16, [-1] * 16]
    seq = [[0] * 16, [0] * 16]
    nth = [[0] * 16, [0] * 16]
    for s in range(SEQS):
        for n, (place, slot, last) in enumerate(chips[s]):
            lim[slot][place], seq[slot][place], nth[slot][place] = last, s, n
    meta = []
    for p in range(32):
        w = [work[p // 2, p % 2, g] for g in range(3)]
        meta.append([t[1] for t in w] + [t[2] for t in w] + [2 if lim[1][p // 2] >= 0 else 1] + [t[0] for t in w])
    return dest, chips, lim, seq, nth, meta


DEST, CHIPS, LIM, SEQ, NTH, META = _tables()
NCH = max(len(c) for c in CHIPS)


def lut(index, table):
    value = jnp.int32(table[0])
    for n in range(1, len(table)):
        if table[n] != table[n - 1]:
            value = jnp.where(index >= n, jnp.int32(table[n]), value)
    return value


def place_of():
    me = lax.axis_index('cp')
    return me, me % 2, (me // 2) % 4, me // 8


def send(src, dst, ssem, rsem, dev, me):
    @pl.when(dev != me)
    def _():
        pltpu.make_async_remote_copy(src, dst, ssem, rsem, device_id={'cp': dev}, device_id_type=MESH).start()

    @pl.when(dev == me)
    def _():
        pltpu.make_async_copy(src, dst, rsem).start()


def dot(a, b):
    return jnp.dot(a, b, preferred_element_type=F32)


def dot_nt(a, b):
    return lax.dot_general(a, b, (((1,), (1,)), ((), ())), preferred_element_type=F32)


def max8(v):
    return jnp.broadcast_to(jnp.max(v, axis=0, keepdims=True), (8, ROWS))


def sum8(v):
    return jnp.broadcast_to(jnp.sum(v, axis=0, keepdims=True), (8, ROWS))


def sub8(a, b):
    return a.reshape(-1, 8, ROWS) - b[None]


def turn(v, cs, sign):
    cos = jnp.concatenate([cs[:, :64], cs[:, :64]], axis=1)
    sin = jnp.concatenate([-cs[:, 64:], cs[:, 64:]], axis=1)
    v = v.reshape(BLK, HEADS, HEAD)
    other = jnp.concatenate([v[..., 64:], v[..., :64]], axis=-1)
    if sign > 0:
        out = v * cos[:, None, :] + other * sin[:, None, :]
    else:
        out = v * cos[:, None, :] - other * sin[:, None, :]
    return out.astype(BF).reshape(ROWS, HEAD)


def landed(ref, sem):
    pltpu.make_async_copy(ref, ref, sem).wait()


def sel(t, values):
    out = values[0]
    for k in range(1, len(values)):
        out = jnp.where(t == k, values[k], out)
    return out


def whole_step(q, do, kv, cs, att, gq, gk, gv,
               qraw, dor, csr, kvr, qn, qa, dot_t, hot, mk, kt, vt, sc, mx, mst, lst, dst, ot, dp_ref, osend, dqsend, csl,
               acc, peer, xr, zs, home,
               ks1, kr1, ks2, kr2, ks3, kr3, ts, tr, os_, or_, as1, ar1, as2, ar2, as3, ar3, cl):
    me, c, x, place = place_of()
    p = 2 * place + c
    jme = jnp.minimum(p, 31 - p)
    hi = p // 16
    lims = [lut(place, LIM[slot]) for slot in range(2)]
    seqs = [lut(place, SEQ[slot]) for slot in range(2)]
    nths = [lut(place, NTH[slot]) for slot in range(2)]
    piece_me = place // PP
    jg = [lut(p, [META[n][g] for n in range(32)]) for g in range(3)]
    slot_g = [lut(p, [META[n][3 + g] for n in range(32)]) for g in range(3)]
    seq_g = [lut(p, [META[n][7 + g] for n in range(32)]) for g in range(3)]
    pos = [v for g in range(3) for v in (jg[g], 31 - jg[g])]
    nch = [v // 2 + 1 for v in pos]
    par = [v % 2 for v in pos]
    ebase = [SLOT1 * slot_g[t // 2] for t in range(6)]
    partner = me + 1 - 2 * c

    def remote(src, dst, ssem, rsem, dev):
        return pltpu.make_async_remote_copy(src, dst, ssem, rsem, device_id={'cp': dev}, device_id_type=MESH)

    n = 0
    for s in range(SEQS):
        for (chip, slot, last) in CHIPS[s]:
            @pl.when(piece_me <= last)
            def _(s=s, chip=chip, slot=slot, n=n):
                send(kv.at[s], kvr.at[SLOT1 * slot + place, x, c], ks1.at[n], kr1.at[slot, piece_me], chip * 8 + 2 * x + c, me)
            n += 1
    for a in range(3):
        here, there = ((q, qraw), (cs, csr), (do, dor))[a]
        for s in range(SEQS):
            code = lut(jme, DEST[s])
            k = 2 * (code % 4) + hi
            dev = (code // 8) * 8 + 2 * x + (code // 4) % 2
            send(cs if a == 1 else here.at[s], there.at[k], ts.at[s, a], tr.at[k, a], dev, me)
    pltpu.make_async_copy(cs, csl, cl).start()

    @pl.loop(0, ENT)
    def _(e):
        acc[e] = jnp.zeros((4, 2, BLK, 2 * HEAD), F32)
    row = lax.broadcasted_iota(jnp.int32, (HEAD, ROWS), 0)
    col = lax.broadcasted_iota(jnp.int32, (HEAD, ROWS), 1)
    hot[...] = jnp.where(col // HEADS == row, 1.0, 0.0).astype(BF)
    ki = lax.broadcasted_iota(jnp.int32, (CK, HEAD), 0)
    di = lax.broadcasted_iota(jnp.int32, (CK, HEAD), 1)
    mk[0] = jnp.zeros((CK, HEAD), BF)
    for cc in range(2):
        mk[1 + cc] = jnp.where((di < BLK) & (ki > di + 64 * x + BLK * cc), -BIG, 0.0).astype(BF)

    @pl.loop(0, 6)
    def _(t):
        ot[t] = jnp.zeros((HEAD, ROWS), F32)
        mst[t] = jnp.full((8, ROWS), -BIG, F32)
        lst[t] = jnp.zeros((8, ROWS), F32)

    def ents(slot, i):
        return pl.ds(SLOT1 * slot + PP * i, PP)

    def relay_x(i):
        for slot in range(2):
            @pl.when(i <= lims[slot])
            def _(slot=slot):
                mine = kvr.at[ents(slot, i), x, c]
                landed(mine, kr1.at[slot, i])
                for d in range(1, 4):
                    remote(mine, mine, ks2.at[slot, i, d - 1], kr2.at[slot, i, d - 1], place * 8 + 2 * ((x + d) % 4) + c).start()

    def relay_core(i):
        for slot in range(2):
            @pl.when(i <= lims[slot])
            def _(slot=slot):
                for d in range(1, 4):
                    landed(kvr.at[ents(slot, i), (x + 4 - d) % 4, c], kr2.at[slot, i, d - 1])
                both = kvr.at[ents(slot, i), :, c]
                remote(both, both, ks3.at[slot, i], kr3.at[slot, i], partner).start()

    @pl.loop(0, PIECES)
    def _(i):
        relay_x(i)
    relay_core(0)

    @pl.loop(0, 6)
    def _(t):
        landed(qraw.at[t], tr.at[t, 0])
        landed(csr.at[t], tr.at[t, 1])
        rq = turn(qraw[t].astype(F32), csr[t], 1)
        qn[t] = rq
        qa[t] = rq.T

    def phase(pc):
        cum = [jnp.int32(0)]
        for t in range(6):
            cum.append(cum[-1] + jnp.minimum(jnp.maximum(nch[t] - PP * pc, 0), PP))

        def dec(i):
            t = jnp.int32(0)
            for k in range(1, 6):
                t = t + (i >= cum[k]).astype(jnp.int32)
            ch = PP * pc + i - sel(t, cum[:6])
            return t, ch, sel(t, ebase) + ch
        return cum[6], dec

    def run(count, pair, last):
        quads = (count - 1) // 4

        @pl.loop(0, quads)
        def _(b):
            for u in range(4):
                pair(4 * b + u, 4 * b, u)
        rest = (count - 1) % 4
        for r in range(4):
            @pl.when(rest == r)
            def _(r=r):
                for u in range(r):
                    pair(4 * quads + u, 4 * quads, u)
                last(4 * quads + r, 4 * quads, r)

    def keys(e):
        return kvr[e, :, :, :, :HEAD].reshape(CK, HEAD)

    def values(e):
        return kvr[e, :, :, :, HEAD:].reshape(CK, HEAD)

    base = [jnp.int32(0)]
    for pc in range(PIECES):
        base.append(base[-1] + phase(pc)[0])

    @pl.loop(0, PIECES)
    def _(pc):
        @pl.when(pc < PIECES - 1)
        def _():
            relay_core(pc + 1)
        for slot in range(2):
            @pl.when(pc <= lims[slot])
            def _(slot=slot):
                landed(kvr.at[ents(slot, pc), :, 1 - c], kr3.at[slot, pc])

                @pl.loop(0, PP)
                def _(v):
                    e = SLOT1 * slot + PP * pc + v
                    kt[e] = keys(e).T
                    vt[e] = values(e).T
        count, dec = phase(pc)
        start = sel(pc, base[:PIECES])

        def s_step(i, sb, u):
            t, ch, e = dec(i)
            mask = jnp.where(ch == sel(t, nch) - 1, 1 + sel(t, par), 0)
            ka = jnp.concatenate([keys(e), mk[mask]], axis=1)
            qh = jnp.concatenate([qa[t], hot[...]], axis=0)
            sv = dot(ka, qh) * C2
            sc.at[pl.ds(sb, 5)][u] = sv
            mx.at[pl.ds(sb, 5)][u] = jnp.max(sv.reshape(CK // 8, 8, ROWS), axis=0)

        def o_step(i, sb, u):
            t, ch, e = dec(i)
            mo = mst[t]
            mn = jnp.maximum(mo, max8(mx.at[pl.ds(sb, 5)][u]))
            al = jnp.exp2(mo - mn)
            ev = jnp.exp2(sub8(sc.at[pl.ds(sb, 5)][u], mn))
            mst[t] = mn
            lst[t] = lst[t] * al + jnp.sum(ev, axis=0)
            ot[t] = (ot[t].reshape(-1, 8, ROWS) * al[None]).reshape(HEAD, ROWS) + dot(vt[e], ev.reshape(CK, ROWS).astype(BF))

        def pair(i, b, u):
            s_step(i + 1, start + b, u + 1)
            o_step(i, start + b, u)

        @pl.when(count > 0)
        def _():
            s_step(jnp.int32(0), start, 0)
            run(count, pair, lambda i, b, u: o_step(i, start + b, u))

    for t in range(6):
        landed(dor.at[t], tr.at[t, 2])
        dot_t[t] = dor[t].T
        l = sum8(lst[t])
        o = (ot[t].reshape(-1, 8, ROWS) / l[None]).reshape(HEAD, ROWS).astype(BF)
        osend[t] = o.T
        dev = (pos[t] // 2) * 8 + 2 * x + par[t]
        send(osend.at[t], att.at[seq_g[t // 2]], os_.at[t, 0], or_.at[seq_g[t // 2], 0], dev, me)
        dst[t] = sum8(jnp.sum((o.astype(F32) * dot_t[t].astype(F32)).reshape(-1, 8, ROWS), axis=0))
        mst[t] = mst[t] + jnp.log2(l)
        ot[t] = jnp.zeros((HEAD, ROWS), F32)

    def sum_core(i):
        for slot in range(2):
            @pl.when(i <= lims[slot])
            def _(slot=slot):
                remote(acc.at[ents(slot, i), :, 1 - c], peer.at[ents(slot, i)], as1.at[slot, i], ar1.at[slot, i], partner).start()

    def sum_x(i):
        for slot in range(2):
            @pl.when(i <= lims[slot])
            def _(slot=slot):
                landed(peer.at[ents(slot, i)], ar1.at[slot, i])

                @pl.loop(0, PP)
                def _(v):
                    e = SLOT1 * slot + PP * i + v
                    acc[e, :, c] += peer[e]
                for d in range(1, 4):
                    remote(acc.at[ents(slot, i), (x + d) % 4, c], xr.at[d - 1, ents(slot, i)],
                           as2.at[slot, i, d - 1], ar2.at[slot, i, d - 1], place * 8 + 2 * ((x + d) % 4) + c).start()

    def sum_home(i):
        for slot in range(2):
            @pl.when(i <= lims[slot])
            def _(slot=slot):
                for d in range(1, 4):
                    landed(xr.at[d - 1, ents(slot, i)], ar2.at[slot, i, d - 1])
                for v in range(PP):
                    to = PP * i + v
                    e = SLOT1 * slot + to
                    zs[e] = acc[e, x, c] + xr[0, e] + xr[1, e] + xr[2, e]
                    send(zs.at[e], home.at[seqs[slot], nths[slot]], as3.at[e], ar3.at[seqs[slot], nths[slot]],
                         to * 8 + 2 * x + c, me)

    @pl.loop(0, PIECES)
    def _(back):
        pc = PIECES - 1 - back
        count, dec = phase(pc)
        start = sel(pc, base[:PIECES])

        def d_step(i, u):
            t, ch, e = dec(i)
            dp_ref[u % 4] = dot(values(e), dot_t[t])

        def g_step(i, sb, u, ahead):
            t, ch, e = dec(i)
            pr = jnp.exp2(sub8(sc.at[pl.ds(sb, 5)][u], mst[t]))
            prb = pr.reshape(CK, ROWS).astype(BF)
            acc[e, :, :, :, HEAD:] += dot(prb, dor[t]).reshape(4, 2, BLK, HEAD)
            ahead()
            ds = (pr * sub8(dp_ref[u % 4], dst[t])).reshape(CK, ROWS).astype(BF)
            ot[t] += dot(kt[e], ds)
            acc[e, :, :, :, :HEAD] += dot(ds, qn[t]).reshape(4, 2, BLK, HEAD)

        @pl.when(count > 0)
        def _():
            d_step(jnp.int32(0), 0)
            run(count, lambda i, b, u: g_step(i, start + b, u, lambda: d_step(i + 1, u + 1)),
                lambda i, b, u: g_step(i, start + b, u, lambda: None))
        sum_core(pc)

        @pl.when(back >= 1)
        def _():
            sum_x(pc + 1)

        @pl.when(back >= 2)
        def _():
            sum_home(pc + 2)

    for t in range(6):
        dqsend[t] = turn((ot[t] * SCALE).T, csr[t], -1)
        dev = (pos[t] // 2) * 8 + 2 * x + par[t]
        send(dqsend.at[t], gq.at[seq_g[t // 2]], os_.at[t, 1], or_.at[seq_g[t // 2], 1], dev, me)
    sum_x(0)
    sum_home(1)
    sum_home(0)

    pltpu.make_async_copy(cs, csl, cl).wait()
    tab = csl[...]
    cos = jnp.concatenate([tab[:, :64], tab[:, :64]], axis=1)
    sin = jnp.concatenate([-tab[:, 64:], tab[:, 64:]], axis=1)
    for s in range(SEQS):
        for m, (chip, slot, last) in enumerate(CHIPS[s]):
            @pl.when(piece_me <= last)
            def _(s=s, m=m):
                landed(home.at[s, m], ar3.at[s, m])

            @pl.when(piece_me > last)
            def _(s=s, m=m):
                home[s, m] = jnp.zeros((BLK, 2 * HEAD), F32)
        total = home[s, 0]
        for m in range(1, len(CHIPS[s])):
            total = total + home[s, m]
        dk = total[:, :HEAD] * SCALE
        other = jnp.concatenate([dk[:, 64:], dk[:, :64]], axis=1)
        gk[s] = (dk * cos - other * sin).astype(BF)
        gv[s] = total[:, HEAD:].astype(BF)

    for s in range(SEQS):
        landed(att.at[s], or_.at[s, 0])
        landed(gq.at[s], or_.at[s, 1])
    n = 0
    for s in range(SEQS):
        for (chip, slot, last) in CHIPS[s]:
            @pl.when((piece_me <= last) & (place != chip))
            def _(s=s, n=n):
                landed(kv.at[s], ks1.at[n])
            n += 1
    for s in range(SEQS):
        code = lut(jme, DEST[s])
        dev = (code // 8) * 8 + 2 * x + (code // 4) % 2

        @pl.when(dev != me)
        def _(s=s):
            landed(q.at[s], ts.at[s, 0])
            landed(cs, ts.at[s, 1])
            landed(do.at[s], ts.at[s, 2])
    for t in range(6):
        @pl.when(pos[t] != p)
        def _(t=t):
            landed(osend.at[t], os_.at[t, 0])
            landed(dqsend.at[t], os_.at[t, 1])
    for slot in range(2):
        @pl.loop(0, lims[slot] + 1)
        def _(i, slot=slot):
            for d in range(1, 4):
                landed(kvr.at[ents(slot, i), x, c], ks2.at[slot, i, d - 1])
                landed(xr.at[d - 1, ents(slot, i)], as2.at[slot, i, d - 1])
            landed(kvr.at[ents(slot, i), :, c], ks3.at[slot, i])
            landed(peer.at[ents(slot, i)], as1.at[slot, i])
            for v in range(PP):
                to = PP * i + v

                @pl.when(to != place)
                def _(to=to):
                    landed(zs.at[SLOT1 * slot + to], as3.at[SLOT1 * slot + to])


def run_whole(q, do, kv, cs):
    dma = pltpu.SemaphoreType.DMA
    n_kv = sum(len(c) for c in CHIPS)
    any_ = pl.BlockSpec(memory_space=pl.ANY)
    vm = pl.BlockSpec(memory_space=pltpu.VMEM)
    v = pltpu.VMEM
    two = 2 * HEAD
    return pl.pallas_call(
        whole_step,
        in_specs=[any_] * 4, out_specs=[any_, any_, vm, vm],
        out_shape=[
            jax.ShapeDtypeStruct((6, ROWS, HEAD), BF), jax.ShapeDtypeStruct((6, ROWS, HEAD), BF),
            jax.ShapeDtypeStruct((6, BLK, HEAD), BF), jax.ShapeDtypeStruct((6, BLK, HEAD), BF)],
        scratch_shapes=[
            v((6, ROWS, HEAD), BF), v((6, ROWS, HEAD), BF), v((6, BLK, HEAD), F32), v((ENT, 4, 2, BLK, two), BF),
            v((6, ROWS, HEAD), BF), v((6, HEAD, ROWS), BF), v((6, HEAD, ROWS), BF), v((HEAD, ROWS), BF), v((3, CK, HEAD), BF),
            v((ENT, HEAD, CK), BF), v((ENT, HEAD, CK), BF),
            v((SIDX, CK, ROWS), F32), v((SIDX, 8, ROWS), F32), v((6, 8, ROWS), F32), v((6, 8, ROWS), F32), v((6, 8, ROWS), F32),
            v((6, HEAD, ROWS), F32), v((4, CK, ROWS), F32), v((6, ROWS, HEAD), BF), v((6, ROWS, HEAD), BF), v((BLK, HEAD), F32),
            v((ENT, 4, 2, BLK, two), F32), v((ENT, 4, BLK, two), F32), v((3, ENT, BLK, two), F32), v((ENT, BLK, two), F32),
            v((SEQS, NCH, BLK, two), F32),
            dma((n_kv,)), dma((2, PIECES)), dma((2, PIECES, 3)), dma((2, PIECES, 3)), dma((2, PIECES)), dma((2, PIECES)),
            dma((6, 3)), dma((6, 3)), dma((6, 2)), dma((6, 2)),
            dma((2, PIECES)), dma((2, PIECES)), dma((2, PIECES, 3)), dma((2, PIECES, 3)), dma((ENT,)), dma((SEQS, NCH)), dma(())],
        compiler_params=pltpu.CompilerParams(has_side_effects=True, vmem_limit_bytes=67043328),
        name='whole_step')(q, do, kv, cs)


def solution(mesh):
    query_spec = PS('dp', 'cp', None, None)
    kv_spec = PS('dp', 'cp', None)
    pos_spec = PS(('dp', 'cp'))

    def per_device(query, key, value, positions, grad_out):
        inv_freq = jnp.power(jnp.float32(ROPE_BASE), -2.0 * jnp.arange(HEAD // 2, dtype=F32) / HEAD)
        angles = positions.astype(F32)[:, None] * inv_freq
        cos, sin = jnp.cos(angles), jnp.sin(angles)
        cs = jnp.concatenate([cos, sin], axis=1)
        k1, k2 = key[..., :64].astype(F32), key[..., 64:].astype(F32)
        kv = jnp.concatenate([(k1 * cos - k2 * sin).astype(BF), (k2 * cos + k1 * sin).astype(BF), value], axis=-1)
        att, gq, gk, gv = run_whole(query.reshape(6, ROWS, HEAD), grad_out.reshape(6, ROWS, HEAD), kv, cs)
        return att.reshape(query.shape), gq.reshape(query.shape), gk, gv

    return jax.shard_map(per_device, mesh=mesh, in_specs=(query_spec, kv_spec, kv_spec, pos_spec, query_spec),
                         out_specs=(query_spec, query_spec, kv_spec, kv_spec), check_vma=False)
```

```python
import jax
import jax.numpy as jnp
from jax import lax
from jax.experimental import pallas as pl
from jax.experimental.pallas import tpu as pltpu
from jax.sharding import PartitionSpec as PS

ROPE_BASE = 10000
SEQS, HEADS, HEAD, BLK = 6, 16, 128, 32
ROWS = BLK * HEADS
CK = 256
ENT = 24
SLOT1 = 12
SIDX = 55
SCALE = HEAD ** -0.5
C2 = SCALE * 1.4426950408889634
BIG = 1e30
HH, TWO = HEAD // 2, 2 * HEAD
BF, F32 = jnp.bfloat16, jnp.float32
MESH = pl.DeviceIdType.MESH

PLACE = [int(d, 16) for d in 'E47B1560328CDA9F']
ORDER = [[int(d, 16) for d in row] for row in (
    '5304218A67B9FDCE',
    'EF69BA87215304DC',
    'CEFDBA5498037126',
    '169078BA4325DCFE',
    'FE167980B53A42CD',
    'CDFEB5894A173260')]
PIECES = 4
PP = 16 // PIECES
HALF = PP // 2
HALVES = 16 // HALF


def _tables():
    work = {}
    dest = [[0] * 16 for _ in range(SEQS)]
    limit = {}
    slots = {}
    for s in range(SEQS):
        for i, j in enumerate(ORDER[s]):
            q = 16 * (s % 3) + i
            f, core, g = q // 6, q % 2, q % 6 // 2
            big_c = 8 * (s // 3) + f
            slot = s % 3 - (6 * f) // 16
            slots[big_c, s] = slot
            work[PLACE[big_c], core, g] = (s, j, slot)
            dest[s][j] = PLACE[big_c] * 8 + core * 4 + g
            limit[big_c, s] = max(limit.get((big_c, s), 0), ((31 - j) // 2) // HALF)
    chips = [[(PLACE[c], slots[c, t], limit[c, t]) for (c, t) in sorted(slots) if t == s] for s in range(SEQS)]
    lim = [[-1] * 16, [-1] * 16]
    seq = [[0] * 16, [0] * 16]
    nth = [[0] * 16, [0] * 16]
    for s in range(SEQS):
        for n, (place, slot, last) in enumerate(chips[s]):
            lim[slot][place], seq[slot][place], nth[slot][place] = last, s, n
    meta = []
    for p in range(32):
        w = [work[p // 2, p % 2, g] for g in range(3)]
        meta.append([t[1] for t in w] + [t[2] for t in w] + [2 if lim[1][p // 2] >= 0 else 1] + [t[0] for t in w])
    return dest, chips, lim, seq, nth, meta


DEST, CHIPS, LIM, SEQ, NTH, META = _tables()
NCH = max(len(c) for c in CHIPS)


def lut(index, table):
    value = jnp.int32(table[0])
    for n in range(1, len(table)):
        if table[n] != table[n - 1]:
            value = jnp.where(index >= n, jnp.int32(table[n]), value)
    return value


def device(place, x, core):
    return place * 8 + 2 * x + core


def place_of():
    me = lax.axis_index('cp')
    return me, me % 2, (me // 2) % 4, me // 8


def send(src, dst, ssem, rsem, dev, me):
    @pl.when(dev != me)
    def _():
        pltpu.make_async_remote_copy(src, dst, ssem, rsem, device_id={'cp': dev}, device_id_type=MESH).start()

    @pl.when(dev == me)
    def _():
        pltpu.make_async_copy(src, dst, rsem).start()


def dot(a, b):
    return jnp.dot(a, b, preferred_element_type=F32)


def dot_nt(a, b):
    return lax.dot_general(a, b, (((1,), (1,)), ((), ())), preferred_element_type=F32)


def max8(v):
    return jnp.broadcast_to(jnp.max(v, axis=0, keepdims=True), (8, ROWS))


def sum8(v):
    return jnp.broadcast_to(jnp.sum(v, axis=0, keepdims=True), (8, ROWS))


def sub8(a, b):
    return a.reshape(-1, 8, ROWS) - b[None]


def turn(v, cs, sign):
    cos = jnp.concatenate([cs[:, :HH], cs[:, :HH]], axis=1)
    sin = jnp.concatenate([-cs[:, HH:], cs[:, HH:]], axis=1)
    v = v.reshape(BLK, HEADS, HEAD)
    other = jnp.concatenate([v[..., HH:], v[..., :HH]], axis=-1)
    if sign > 0:
        out = v * cos[:, None, :] + other * sin[:, None, :]
    else:
        out = v * cos[:, None, :] - other * sin[:, None, :]
    return out.astype(BF).reshape(ROWS, HEAD)


def landed(ref, sem):
    pltpu.make_async_copy(ref, ref, sem).wait()


def sel(t, values):
    out = values[0] + jnp.int32(0)
    for k in range(1, len(values)):
        out = jnp.where(t == k, values[k], out)
    return out


def whole_step(q, do, key, value, pos32, freq, att, gq, gk, gv,
               qraw, dor, csr, kvr, qn, qa, dot_t, hot, mk, kt, vt, sc, mx, mst, lst, dst, ot, dp_ref, csl,
               acc, peer, xr, zs, home, keyl, kv, posl,
               ks1, kr1, ks2, kr2, ks3, kr3, ts, tr, os_, or_, as1, ar1, as2, ar2, as3, ar3, cl, kl):
    me, c, x, place = place_of()
    p = 2 * place + c
    jme = jnp.minimum(p, 31 - p)
    hi = p // 16
    lims = [lut(place, LIM[slot]) for slot in range(2)]
    seqs = [lut(place, SEQ[slot]) for slot in range(2)]
    nths = [lut(place, NTH[slot]) for slot in range(2)]
    half_me = place // HALF
    jg = [lut(p, [META[n][g] for n in range(len(META))]) for g in range(3)]
    slot_g = [lut(p, [META[n][3 + g] for n in range(len(META))]) for g in range(3)]
    seq_g = [lut(p, [META[n][7 + g] for n in range(len(META))]) for g in range(3)]
    pos = [v for g in range(3) for v in (jg[g], 31 - jg[g])]
    nch = [v // 2 + 1 for v in pos]
    par = [v % 2 for v in pos]
    ebase = [SLOT1 * slot_g[t // 2] for t in range(6)]
    partner = me + 1 - 2 * c

    def remote(src, dst, ssem, rsem, dev):
        return pltpu.make_async_remote_copy(src, dst, ssem, rsem, device_id={'cp': dev}, device_id_type=MESH)

    fetch = [pltpu.make_async_copy(pos32, posl, cl), pltpu.make_async_copy(key, keyl, kl.at[0]),
             pltpu.make_async_copy(value, kv.at[:, :, HEAD:], kl.at[1])]
    for copy in fetch:
        copy.start()
    barrier = pltpu.get_barrier_semaphore()

    def greet(dev):
        pl.semaphore_signal(barrier, inc=1, device_id={'cp': dev}, device_id_type=MESH)

    @pl.loop(0, 16)
    def _(other):
        greet(device(other, x, 1 - c))

        @pl.when(other != place)
        def _():
            greet(device(other, x, c))
    for d in range(1, 4):
        greet(device(place, (x + d) % 4, c))
    for copy in fetch:
        copy.wait()
    inv = freq[...]
    for t in range(BLK):
        csl[t:t + 1, :HH] = posl[t].astype(F32) * inv
    ang = csl[:, :HH]
    csl[:, :HH] = jnp.cos(ang)
    csl[:, HH:] = jnp.sin(ang)
    tab = csl[...]
    cos = jnp.concatenate([tab[:, :HH], tab[:, :HH]], axis=1)
    sin = jnp.concatenate([-tab[:, HH:], tab[:, HH:]], axis=1)
    for s in range(SEQS):
        kf = keyl[s].astype(F32)
        kv[s, :, :HEAD] = (kf * cos + jnp.concatenate([kf[:, HH:], kf[:, :HH]], axis=1) * sin).astype(BF)
    pl.semaphore_wait(barrier, 34)

    def work_of(s):
        code = lut(jme, DEST[s])
        return code % 4, 2 * (code % 4) + hi, device(code // 8, x, (code // 4) % 2)

    def send_q():
        for g in range(3):
            for s in range(SEQS):
                when, k, dev = work_of(s)

                @pl.when(when == g)
                def _(s=s, k=k, dev=dev):
                    send(q.at[s], qraw.at[k], ts.at[s, 0], tr.at[k, 0], dev, me)
                    send(csl, csr.at[k], ts.at[s, 1], tr.at[k, 1], dev, me)

    def send_do():
        for s in range(SEQS):
            _, k, dev = work_of(s)
            send(do.at[s], dor.at[k], ts.at[s, 2], tr.at[k, 2], dev, me)

    n = 0
    for s in range(SEQS):
        for (chip, slot, last) in CHIPS[s]:
            @pl.when(half_me <= last)
            def _(s=s, chip=chip, slot=slot, n=n):
                send(kv.at[s], kvr.at[SLOT1 * slot + place, x, c], ks1.at[n], kr1.at[slot, half_me], device(chip, x, c), me)
            n += 1

    @pl.loop(0, ENT)
    def _(e):
        acc[e] = jnp.zeros((4, 2, BLK, TWO), F32)
    row = lax.broadcasted_iota(jnp.int32, (HEAD, ROWS), 0)
    col = lax.broadcasted_iota(jnp.int32, (HEAD, ROWS), 1)
    hot[...] = jnp.where(col // HEADS == row, 1.0, 0.0).astype(BF)
    ki = lax.broadcasted_iota(jnp.int32, (CK, HEAD), 0)
    di = lax.broadcasted_iota(jnp.int32, (CK, HEAD), 1)
    mk[0] = jnp.zeros((CK, HEAD), BF)
    for cc in range(2):
        mk[1 + cc] = jnp.where((di < BLK) & (ki > di + 64 * x + BLK * cc), -BIG, 0.0).astype(BF)

    @pl.loop(0, 6)
    def _(t):
        ot[t] = jnp.zeros((HEAD, ROWS), F32)
        mst[t] = jnp.full((8, ROWS), -BIG, F32)
        lst[t] = jnp.zeros((8, ROWS), F32)

    right = device(place, (x + 1) % 4, c)
    left = device(place, (x + 3) % 4, c)

    def halves(i):
        return [u for h in range(2) for u in half(i, h)]

    def half(i, h):
        slots = 1 if isinstance(i, int) and i == PIECES - 1 else 2
        return [(slot, h, 2 * i + h) for slot in range(slots)]

    def ents(slot, n):
        return pl.ds(SLOT1 * slot + HALF * n, HALF)

    def relay_x(i):
        for slot, h, n in halves(i):
            @pl.when(n <= lims[slot])
            def _(slot=slot, n=n):
                mine = kvr.at[ents(slot, n), x, c]
                landed(mine, kr1.at[slot, n])
                remote(mine, mine, ks2.at[slot, n, 0], kr2.at[slot, n, 0], right).start()
                remote(mine, mine, ks2.at[slot, n, 1], kr2.at[slot, n, 1], left).start()

    def relay_x2(i):
        for slot, h, n in halves(i):
            @pl.when(n <= lims[slot])
            def _(slot=slot, h=h, n=n):
                theirs = kvr.at[ents(slot, n), (x + 3 - 2 * h) % 4, c]
                landed(theirs, kr2.at[slot, n, h])
                remote(theirs, theirs, ks2.at[slot, n, 2], kr2.at[slot, n, 2], left if h else right).start()

    def relay_core(i):
        for slot, h, n in halves(i):
            @pl.when(n <= lims[slot])
            def _(slot=slot, h=h, n=n):
                landed(kvr.at[ents(slot, n), x, c], kr2.at[slot, n, 1 - h])
                landed(kvr.at[ents(slot, n), x, c], kr2.at[slot, n, 2])
                both = kvr.at[ents(slot, n), :, c]
                remote(both, both, ks3.at[slot, n], kr3.at[slot, n], partner).start()

    relay_x(0)
    relay_x(1)
    send_q()
    relay_x(2)
    relay_x(3)
    relay_x2(0)
    relay_x2(1)
    relay_core(0)

    def prep_q(t):
        landed(qraw.at[t], tr.at[t, 0])
        landed(csr.at[t], tr.at[t, 1])
        rq = turn(qraw[t].astype(F32), csr[t], 1)
        qn[t] = rq
        qa[t] = rq.T

    def phase(pc):
        cum = [jnp.int32(0)]
        for t in range(6):
            cum.append(cum[-1] + jnp.minimum(jnp.maximum(nch[t] - PP * pc, 0), PP))
        return cum

    base = [jnp.int32(0)]
    for pc in range(PIECES):
        base.append(base[-1] + phase(pc)[6])

    def segment(k):
        pc = jnp.maximum(k - 2, 0)
        cum = phase(pc)
        part = jnp.minimum(k, 3)
        first = sel(part, [cum[0], cum[2], cum[4], cum[0]])
        count = sel(part, [cum[2], cum[4], cum[6], cum[6]]) - first

        def dec(i):
            i = i + first
            t = jnp.int32(0)
            for n in range(1, 6):
                t = t + (i >= cum[n]).astype(jnp.int32)
            ch = PP * pc + i - sel(t, cum[:6])
            return t, ch, sel(t, ebase) + ch
        return pc, sel(pc, base[:PIECES]) + first, count, dec

    def run(count, pair, last, between=None):
        quads = (count - 1) // 4

        def quad(b):
            for u in range(4):
                pair(4 * b + u, 4 * b, u)
        if between is None:
            pl.loop(0, quads)(quad)
        else:
            @pl.loop(0, quads)
            def _(b):
                @pl.when(b == 2)
                def _():
                    between()
                quad(b)

            @pl.when(quads <= 2)
            def _():
                between()
        rest = (count - 1) % 4
        for r in range(4):
            @pl.when(rest == r)
            def _(r=r):
                for u in range(r):
                    pair(4 * quads + u, 4 * quads, u)
                last(4 * quads + r, 4 * quads, r)

    def keys(e):
        return kvr[e, :, :, :, :HEAD].reshape(CK, HEAD)

    def values(e):
        return kvr[e, :, :, :, HEAD:].reshape(CK, HEAD)

    @pl.loop(0, 6)
    def _(k):
        @pl.when((k >= 1) & (k <= 3))
        def _():
            relay_core(k)
        @pl.when(k < 3)
        def _():
            prep_q(2 * k)
            prep_q(2 * k + 1)
        @pl.when(k == 0)
        def _():
            send_do()
            relay_x2(2)
            relay_x2(3)
        pc, start, count, dec = segment(k)
        for slot, h, n in halves(pc):
            @pl.when((n <= lims[slot]) & ((k == 0) | (k > 2)))
            def _(slot=slot, n=n):
                landed(kvr.at[ents(slot, n), :, 1 - c], kr3.at[slot, n])
                for v in range(HALF):
                    e = SLOT1 * slot + HALF * n + v
                    kt[e] = keys(e).T
                    vt[e] = values(e).T

        def s_step(i, sb, u):
            t, ch, e = dec(i)
            mask = jnp.where(ch == sel(t, nch) - 1, 1 + sel(t, par), 0)
            ka = jnp.concatenate([keys(e), mk[mask]], axis=1)
            qh = jnp.concatenate([qa[t], hot[...]], axis=0)
            sv = dot(ka, qh) * C2
            sc.at[pl.ds(sb, 5)][u] = sv
            mx.at[pl.ds(sb, 5)][u] = jnp.max(sv.reshape(CK // 8, 8, ROWS), axis=0)

        def o_step(i, sb, u):
            t, ch, e = dec(i)
            mo = mst[t]
            mn = jnp.maximum(mo, max8(mx.at[pl.ds(sb, 5)][u]))
            al = jnp.exp2(mo - mn)
            ev = jnp.exp2(sub8(sc.at[pl.ds(sb, 5)][u], mn))
            mst[t] = mn
            lst[t] = lst[t] * al + jnp.sum(ev, axis=0)
            ot[t] = (ot[t].reshape(-1, 8, ROWS) * al[None]).reshape(HEAD, ROWS) + dot(vt[e], ev.reshape(CK, ROWS).astype(BF))

        def pair(i, b, u):
            s_step(i + 1, start + b, u + 1)
            o_step(i, start + b, u)

        @pl.when(count > 0)
        def _():
            s_step(jnp.int32(0), start, 0)
            run(count, pair, lambda i, b, u: o_step(i, start + b, u))

    for t in range(6):
        landed(dor.at[t], tr.at[t, 2])
        dot_t[t] = dor[t].T
        l = sum8(lst[t])
        o = (ot[t].reshape(-1, 8, ROWS) / l[None]).reshape(HEAD, ROWS).astype(BF)
        qraw[t] = o.T
        dev = device(pos[t] // 2, x, par[t])
        send(qraw.at[t], att.at[seq_g[t // 2]], os_.at[t, 0], or_.at[seq_g[t // 2], 0], dev, me)
        dst[t] = sum8(jnp.sum((o.astype(F32) * dot_t[t].astype(F32)).reshape(-1, 8, ROWS), axis=0))
        mst[t] = mst[t] + jnp.log2(l)
        ot[t] = jnp.zeros((HEAD, ROWS), F32)

    def sum_core(units):
        for slot, h, n in units:
            @pl.when(n <= lims[slot])
            def _(slot=slot, n=n):
                remote(acc.at[ents(slot, n), :, 1 - c], peer.at[ents(slot, n)], as1.at[slot, n], ar1.at[slot, n], partner).start()

    def sum_x(units):
        for slot, h, n in units:
            @pl.when(n <= lims[slot])
            def _(slot=slot, h=h, n=n):
                es = ents(slot, n)
                landed(peer.at[es], ar1.at[slot, n])
                for v in range(HALF):
                    e = SLOT1 * slot + HALF * n + v
                    acc[e, :, c] += peer[e]
                one, other = (left, right) if h else (right, left)
                remote(acc.at[es, (x + 2) % 4, c], xr.at[2, es], as2.at[slot, n, 0], ar2.at[slot, n, 0], one).start()
                remote(acc.at[es, (x + 3 - 2 * h) % 4, c], xr.at[1 - h, es], as2.at[slot, n, 1], ar2.at[slot, n, 1], other).start()

    def sum_x2(units):
        for slot, h, n in units:
            @pl.when(n <= lims[slot])
            def _(slot=slot, h=h, n=n):
                es = ents(slot, n)
                to = (x + 1 + 2 * h) % 4
                landed(xr.at[2, es], ar2.at[slot, n, 0])
                acc[es, to, c] += xr[2, es]
                remote(acc.at[es, to, c], xr.at[h, es], as2.at[slot, n, 2], ar2.at[slot, n, 2], left if h else right).start()

    def sum_home(units):
        for slot, h, n in units:
            @pl.when(n <= lims[slot])
            def _(slot=slot, h=h, n=n):
                landed(xr.at[1 - h, ents(slot, n)], ar2.at[slot, n, 1])
                landed(xr.at[h, ents(slot, n)], ar2.at[slot, n, 2])
                for v in range(HALF):
                    to = HALF * n + v
                    e = SLOT1 * slot + to
                    zs[e] = acc[e, x, c] + xr[0, e] + xr[1, e]
                    send(zs.at[e], home.at[seqs[slot], nths[slot]], as3.at[e], ar3.at[seqs[slot], nths[slot]],
                         device(to, x, c), me)

    cum0 = phase(0)

    def upto(t, lo, hi):
        return jnp.minimum(jnp.maximum(nch[t] - lo, 0), hi - lo)

    @pl.loop(0, 7)
    def _(back):
        pc = jnp.maximum(3 - back, 0)
        lo = sel(back, [12, 8, 4, 2, 0, 0, 0])
        hi = sel(back, [16, 12, 8, 4, 2, 2, 2])
        starts = sel(pc, base[:PIECES])
        cum = phase(pc)
        steps = [jnp.int32(0)]
        for t in range(6):
            wanted = (back < 4) | (back == 4 + t // 2)
            steps.append(steps[-1] + jnp.where(wanted, upto(t, lo, hi), 0))
        count = steps[6]

        def dec(i):
            t = jnp.int32(0)
            for n in range(1, 6):
                t = t + (i >= steps[n]).astype(jnp.int32)
            ch = lo + i - sel(t, steps[:6])
            return t, ch, sel(t, ebase) + ch, starts + sel(t, cum[:6]) + ch - PP * pc

        def between():
            @pl.when((back >= 1) & (back <= 3))
            def _():
                @pl.when(back >= 2)
                def _():
                    sum_x2(halves(5 - back))
                sum_x(halves(4 - back))

            @pl.when(back == 4)
            def _():
                sum_home(halves(3))

            @pl.when(back == 5)
            def _():
                sum_x(half(0, 1))

            @pl.when(back == 6)
            def _():
                sum_x2(halves(1))
                sum_home(halves(2))

        def d_step(i, u):
            t, ch, e, si = dec(i)
            dp_ref[u % 2] = dot(values(e), dot_t[t])

        def g_step(i, u, ahead):
            t, ch, e, si = dec(i)
            pr = jnp.exp2(sub8(sc[si], mst[t]))
            prb = pr.reshape(CK, ROWS).astype(BF)
            acc[e, :, :, :, HEAD:] += dot(prb, dor[t]).reshape(4, 2, BLK, HEAD)
            ahead()
            ds = (pr * sub8(dp_ref[u % 2], dst[t])).reshape(CK, ROWS).astype(BF)
            ot[t] += dot(kt[e], ds)
            acc[e, :, :, :, :HEAD] += dot(ds, qn[t]).reshape(4, 2, BLK, HEAD)

        @pl.when(count > 0)
        def _():
            d_step(jnp.int32(0), 0)
            run(count, lambda i, b, u: g_step(i, u, lambda: d_step(i + 1, u + 1)),
                lambda i, b, u: g_step(i, u, lambda: None), between)
        @pl.when(back < 3)
        def _():
            sum_core(halves(pc))

        @pl.when(back == 3)
        def _():
            sum_core(half(0, 1))

        @pl.when(back == 6)
        def _():
            sum_core(half(0, 0))

        @pl.when(back >= 4)
        def _():
            for tl in range(2):
                t = 2 * (back - 4) + tl
                seq = sel(back - 4, seq_g)
                qn[t] = turn((ot[t] * SCALE).T, csr[t], -1)
                dev = device(sel(t, pos) // 2, x, sel(t, par))
                send(qn.at[t], gq.at[seq], os_.at[t, 1], or_.at[seq, 1], dev, me)

    sum_x(half(0, 0))
    sum_x2(half(0, 1))
    sum_home(halves(1))
    sum_x2(half(0, 0))
    sum_home(half(0, 1))
    sum_home(half(0, 0))
    for s in range(SEQS):
        for m, (chip, slot, last) in enumerate(CHIPS[s]):
            @pl.when(half_me <= last)
            def _(s=s, m=m):
                landed(home.at[s, m], ar3.at[s, m])

            @pl.when(half_me > last)
            def _(s=s, m=m):
                home[s, m] = jnp.zeros((BLK, TWO), F32)
        total = home[s, 0]
        for m in range(1, len(CHIPS[s])):
            total = total + home[s, m]
        dk = total[:, :HEAD] * SCALE
        other = jnp.concatenate([dk[:, HH:], dk[:, :HH]], axis=1)
        gk[s] = (dk * cos - other * sin).astype(BF)
        gv[s] = total[:, HEAD:].astype(BF)

    for s in range(SEQS):
        landed(att.at[s], or_.at[s, 0])
        landed(gq.at[s], or_.at[s, 1])
    n = 0
    for s in range(SEQS):
        for (chip, slot, last) in CHIPS[s]:
            @pl.when((half_me <= last) & (place != chip))
            def _(s=s, n=n):
                landed(kv.at[s], ks1.at[n])
            n += 1
    for s in range(SEQS):
        _, _, dev = work_of(s)

        @pl.when(dev != me)
        def _(s=s):
            landed(q.at[s], ts.at[s, 0])
            landed(csl, ts.at[s, 1])
            landed(do.at[s], ts.at[s, 2])
    for t in range(6):
        @pl.when(pos[t] != p)
        def _(t=t):
            landed(qraw.at[t], os_.at[t, 0])
            landed(qn.at[t], os_.at[t, 1])
    for slot in range(2):
        @pl.loop(0, lims[slot] + 1)
        def _(n, slot=slot):
            for d in range(3):
                landed(kvr.at[ents(slot, n), x, c], ks2.at[slot, n, d])
                landed(zs.at[ents(slot, n)], as2.at[slot, n, d])
            landed(kvr.at[ents(slot, n), :, c], ks3.at[slot, n])
            landed(peer.at[ents(slot, n)], as1.at[slot, n])
            for v in range(HALF):
                to = HALF * n + v

                @pl.when(to != place)
                def _(to=to):
                    landed(zs.at[SLOT1 * slot + to], as3.at[SLOT1 * slot + to])


def run_whole(q, do, key, value, pos32, freq):
    dma = pltpu.SemaphoreType.DMA
    n_kv = sum(len(c) for c in CHIPS)
    any_ = pl.BlockSpec(memory_space=pl.ANY)
    vm = pl.BlockSpec(memory_space=pltpu.VMEM)
    v = pltpu.VMEM
    return pl.pallas_call(
        whole_step,
        in_specs=[any_] * 5 + [vm], out_specs=[vm] * 4,
        out_shape=[v((6, ROWS, HEAD), BF), v((6, ROWS, HEAD), BF), v((6, BLK, HEAD), BF), v((6, BLK, HEAD), BF)],
        scratch_shapes=[
            v((6, ROWS, HEAD), BF), v((6, ROWS, HEAD), BF), v((6, BLK, HEAD), F32), v((ENT, 4, 2, BLK, TWO), BF),
            v((6, ROWS, HEAD), BF), v((6, HEAD, ROWS), BF), v((6, HEAD, ROWS), BF), v((HEAD, ROWS), BF), v((3, CK, HEAD), BF),
            v((ENT, HEAD, CK), BF), v((ENT, HEAD, CK), BF),
            v((SIDX, CK, ROWS), F32), v((SIDX, 8, ROWS), F32), v((6, 8, ROWS), F32), v((6, 8, ROWS), F32), v((6, 8, ROWS), F32),
            v((6, HEAD, ROWS), F32), v((2, CK, ROWS), F32), v((BLK, HEAD), F32),
            v((ENT, 4, 2, BLK, TWO), F32), v((ENT, 4, BLK, TWO), F32), v((3, ENT, BLK, TWO), F32), v((ENT, BLK, TWO), F32),
            v((SEQS, NCH, BLK, TWO), F32), v((SEQS, BLK, HEAD), BF), v((SEQS, BLK, TWO), BF), pltpu.SMEM((BLK,), jnp.int32),
            dma((n_kv,)), dma((2, HALVES)), dma((2, HALVES, 3)), dma((2, HALVES, 3)), dma((2, HALVES)), dma((2, HALVES)),
            dma((6, 3)), dma((6, 3)), dma((6, 2)), dma((6, 2)),
            dma((2, HALVES)), dma((2, HALVES)), dma((2, HALVES, 3)), dma((2, HALVES, 3)), dma((ENT,)), dma((SEQS, NCH)), dma(()), dma((2,))],
        compiler_params=pltpu.CompilerParams(has_side_effects=True, collective_id=0, vmem_limit_bytes=62500000),
        name='whole_step')(q, do, key, value, pos32, pltpu.with_memory_space_constraint(freq, pltpu.VMEM))


def put(*refs):
    here, there, sem = refs[:4], refs[4:8], refs[8]
    copies = [pltpu.make_async_copy(a, b, sem.at[n]) for n, (a, b) in enumerate(zip(here, there))]
    for copy in copies:
        copy.start()
    for copy in copies:
        copy.wait()


def run_put(*arrays):
    any_ = pl.BlockSpec(memory_space=pl.ANY)
    return pl.pallas_call(
        put, in_specs=[any_] * 4, out_specs=[any_] * 4,
        out_shape=[jax.ShapeDtypeStruct(a.shape, a.dtype) for a in arrays],
        scratch_shapes=[pltpu.SemaphoreType.DMA((4,))], name='put')(*[pltpu.with_memory_space_constraint(a, pltpu.VMEM) for a in arrays])


def solution(mesh):
    query_spec = PS('dp', 'cp', None, None)
    kv_spec = PS('dp', 'cp', None)
    pos_spec = PS(('dp', 'cp'))

    def per_device(query, key, value, positions, grad_out):
        inv_freq = jnp.power(jnp.float32(ROPE_BASE), -2.0 * jnp.arange(HH, dtype=F32) / HEAD)
        att, gq, gk, gv = run_whole(query.reshape(6, ROWS, HEAD), grad_out.reshape(6, ROWS, HEAD), key, value, positions, inv_freq[None])
        att, gq, gk, gv = run_put(att, gq, gk, gv)
        return att.reshape(query.shape), gq.reshape(query.shape), gk, gv

    return jax.shard_map(per_device, mesh=mesh, in_specs=(query_spec, kv_spec, kv_spec, pos_spec, query_spec),
                         out_specs=(query_spec, query_spec, kv_spec, kv_spec), check_vma=False)
```

```python
import jax
import jax.numpy as jnp
from jax import lax
from jax.experimental import pallas as pl
from jax.experimental.pallas import tpu as pltpu
from jax.sharding import PartitionSpec as PS

ROPE_BASE = 10000
SEQS, HEADS, HEAD, BLK = 6, 16, 128, 32
ROWS = BLK * HEADS
CK = 256
ENT = 20
SLOT1 = 10
SIDX = 55
SCALE = HEAD ** -0.5
C2 = SCALE * 1.4426950408889634
BIG = 1e30
HH, TWO = HEAD // 2, 2 * HEAD
BF, F32 = jnp.bfloat16, jnp.float32
MESH = pl.DeviceIdType.MESH

PLACE = [int(d, 16) for d in 'E47B1560328CDA9F']
ORDER = [[int(d, 16) for d in row] for row in (
    '5423018967BAFECD',
    'EF8967BA542301DC',
    'CDFEBA9854760123',
    '1076982345BAFEDC',
    'FE1076893245BACD',
    'CDFEBA8945671032')]
PIECES = 4
PP = 16 // PIECES
HALF = PP // 2
HALVES = 16 // HALF


def _tables():
    work = {}
    dest = [[0] * 16 for _ in range(SEQS)]
    limit = {}
    slots = {}
    for s in range(SEQS):
        for i, j in enumerate(ORDER[s]):
            q = 16 * (s % 3) + i
            f, core, g = q // 6, q % 2, q % 6 // 2
            big_c = 8 * (s // 3) + f
            slot = s % 3 - (6 * f) // 16
            slots[big_c, s] = slot
            work[PLACE[big_c], core, g] = (s, j, slot)
            dest[s][j] = PLACE[big_c] * 8 + core * 4 + g
            limit[big_c, s] = max(limit.get((big_c, s), 0), ((31 - j) // 2) // HALF)
    chips = [[(PLACE[c], slots[c, t], limit[c, t]) for (c, t) in sorted(slots) if t == s] for s in range(SEQS)]
    lim = [[-1] * 16, [-1] * 16]
    seq = [[0] * 16, [0] * 16]
    nth = [[0] * 16, [0] * 16]
    for s in range(SEQS):
        for n, (place, slot, last) in enumerate(chips[s]):
            lim[slot][place], seq[slot][place], nth[slot][place] = last, s, n
    meta = []
    for p in range(32):
        w = [work[p // 2, p % 2, g] for g in range(3)]
        meta.append([t[1] for t in w] + [t[2] for t in w] + [2 if lim[1][p // 2] >= 0 else 1] + [t[0] for t in w])
    return dest, chips, lim, seq, nth, meta


DEST, CHIPS, LIM, SEQ, NTH, META = _tables()
N_HOME = [sum(n // HALF <= last for row in CHIPS for _, _, last in row) for n in range(16)]
N_KV = [N_HOME[n] - sum(n // HALF <= last for row in CHIPS for chip, _, last in row if chip == n) for n in range(16)]
N_SUMS = [sum(HALF * (row[n] + 1) - (n < HALF * (row[n] + 1)) for row in LIM) for n in range(16)]
NCH = max(len(c) for c in CHIPS)


def lut(index, table):
    value = jnp.int32(table[0])
    for n in range(1, len(table)):
        if table[n] != table[n - 1]:
            value = jnp.where(index >= n, jnp.int32(table[n]), value)
    return value


def device(place, x, core):
    return place * 8 + 2 * x + core


def place_of():
    me = lax.axis_index('cp')
    return me, me % 2, (me // 2) % 4, me // 8


def send(src, dst, ssem, rsem, dev, me):
    @pl.when(dev != me)
    def _():
        pltpu.make_async_remote_copy(src, dst, ssem, rsem, device_id={'cp': dev}, device_id_type=MESH).start()

    @pl.when(dev == me)
    def _():
        pltpu.make_async_copy(src, dst, rsem).start()


def dot(a, b):
    return jnp.dot(a, b, preferred_element_type=F32)


def dot_nt(a, b):
    return lax.dot_general(a, b, (((1,), (1,)), ((), ())), preferred_element_type=F32)


def max8(v):
    return jnp.broadcast_to(jnp.max(v, axis=0, keepdims=True), (8, ROWS))


def sum8(v):
    return jnp.broadcast_to(jnp.sum(v, axis=0, keepdims=True), (8, ROWS))


def sub8(a, b):
    return a.reshape(-1, 8, ROWS) - b[None]


def turn(v, cs, sign):
    cos = jnp.concatenate([cs[:, :HH], cs[:, :HH]], axis=1)
    sin = jnp.concatenate([-cs[:, HH:], cs[:, HH:]], axis=1)
    v = v.reshape(BLK, HEADS, HEAD)
    other = jnp.concatenate([v[..., HH:], v[..., :HH]], axis=-1)
    if sign > 0:
        out = v * cos[:, None, :] + other * sin[:, None, :]
    else:
        out = v * cos[:, None, :] - other * sin[:, None, :]
    return out.astype(BF).reshape(ROWS, HEAD)


def nr(slot, n):
    return SLOT1 // HALF * slot + n


def landed(ref, sem):
    pltpu.make_async_copy(ref, ref, sem).wait()


def sel(t, values):
    out = values[0] + jnp.int32(0)
    for k in range(1, len(values)):
        out = jnp.where(t == k, values[k], out)
    return out


def whole_step(q, do, key, value, pos32, freq, att, gq, gk, gv,
               qraw, dor, csr, kvr, qn, qa, dot_t, hot, mk, kt, vt, sc, mx, mst, lst, dst, ot, dp_ref, csl,
               acc, peer, xr, zs, home, keyl, kv, posl,
               kr1, kr2, kr3, ts, tr, os_, ar1, ar2, s_one, s_x, s_core, or_, ar3, kl):
    me, c, x, place = place_of()
    p = 2 * place + c
    jme = jnp.minimum(p, 31 - p)
    hi = p // 16
    lims = [lut(place, LIM[slot]) for slot in range(2)]
    seqs = [lut(place, SEQ[slot]) for slot in range(2)]
    nths = [lut(place, NTH[slot]) for slot in range(2)]
    half_me = place // HALF
    jg = [lut(p, [META[n][g] for n in range(len(META))]) for g in range(3)]
    slot_g = [lut(p, [META[n][3 + g] for n in range(len(META))]) for g in range(3)]
    seq_g = [lut(p, [META[n][7 + g] for n in range(len(META))]) for g in range(3)]
    pos = [v for g in range(3) for v in (jg[g], 31 - jg[g])]
    nch = [v // 2 + 1 for v in pos]
    par = [v % 2 for v in pos]
    ebase = [SLOT1 * slot_g[t // 2] for t in range(6)]
    partner = me + 1 - 2 * c

    def landed_many(ref, counts, sem):
        many = lut(place, counts)
        for k in sorted(set(counts)):
            @pl.when(many == k)
            def _(k=k):
                landed(ref.at[pl.ds(0, k)], sem)

    def remote(src, dst, ssem, rsem, dev):
        return pltpu.make_async_remote_copy(src, dst, ssem, rsem, device_id={'cp': dev}, device_id_type=MESH)

    fetch = [pltpu.make_async_copy(pos32, posl, kl.at[2]), pltpu.make_async_copy(key, keyl, kl.at[0]),
             pltpu.make_async_copy(value, kv.at[:, :, HEAD:], kl.at[1])]
    for copy in fetch:
        copy.start()
    barrier = pltpu.get_barrier_semaphore()

    def greet(dev):
        pl.semaphore_signal(barrier, inc=1, device_id={'cp': dev}, device_id_type=MESH)

    @pl.loop(0, 16)
    def _(other):
        greet(device(other, x, 1 - c))

        @pl.when(other != place)
        def _():
            greet(device(other, x, c))
    for d in range(1, 4):
        greet(device(place, (x + d) % 4, c))
    for copy in fetch:
        copy.wait()
    inv = freq[...]
    for t in range(BLK):
        csl[t:t + 1, :HH] = posl[t].astype(F32) * inv
    ang = csl[:, :HH]
    csl[:, :HH] = jnp.cos(ang)
    csl[:, HH:] = jnp.sin(ang)
    tab = csl[...]
    cos = jnp.concatenate([tab[:, :HH], tab[:, :HH]], axis=1)
    sin = jnp.concatenate([-tab[:, HH:], tab[:, HH:]], axis=1)
    for s in range(SEQS):
        kf = keyl[s].astype(F32)
        kv[s, :, :HEAD] = (kf * cos + jnp.concatenate([kf[:, HH:], kf[:, :HH]], axis=1) * sin).astype(BF)
    pl.semaphore_wait(barrier, 34)

    def work_of(s):
        code = lut(jme, DEST[s])
        return code % 4, 2 * (code % 4) + hi, device(code // 8, x, (code // 4) % 2)

    def send_q():
        for g in range(3):
            for s in range(SEQS):
                when, k, dev = work_of(s)

                @pl.when(when == g)
                def _(s=s, k=k, dev=dev):
                    send(q.at[s], qraw.at[k], ts.at[s, 0], tr.at[k, 0], dev, me)
                    send(csl, csr.at[k], ts.at[s, 1], tr.at[k, 1], dev, me)

    def send_do():
        for s in range(SEQS):
            _, k, dev = work_of(s)
            send(do.at[s], dor.at[k], ts.at[s, 0], tr.at[k, 2], dev, me)

    for s in range(SEQS):
        for (chip, slot, last) in CHIPS[s]:
            @pl.when(half_me <= last)
            def _(s=s, chip=chip, slot=slot):
                send(kv.at[s], kvr.at[SLOT1 * slot + place, x, c], s_one, kr1.at[nr(slot, half_me)], device(chip, x, c), me)
    send_q()

    @pl.loop(0, ENT)
    def _(e):
        acc[e] = jnp.zeros((4, 2, BLK, TWO), F32)
    row = lax.broadcasted_iota(jnp.int32, (HEAD, ROWS), 0)
    col = lax.broadcasted_iota(jnp.int32, (HEAD, ROWS), 1)
    hot[...] = jnp.where(col // HEADS == row, 1.0, 0.0).astype(BF)
    ki = lax.broadcasted_iota(jnp.int32, (CK, HEAD), 0)
    di = lax.broadcasted_iota(jnp.int32, (CK, HEAD), 1)
    mk[0] = jnp.zeros((CK, HEAD), BF)
    for cc in range(2):
        mk[1 + cc] = jnp.where((di < BLK) & (ki > di + 64 * x + BLK * cc), -BIG, 0.0).astype(BF)

    @pl.loop(0, 6)
    def _(t):
        ot[t] = jnp.zeros((HEAD, ROWS), F32)
        mst[t] = jnp.full((8, ROWS), -BIG, F32)
        lst[t] = jnp.zeros((8, ROWS), F32)

    right = device(place, (x + 1) % 4, c)
    left = device(place, (x + 3) % 4, c)

    def halves(i):
        return [u for h in range(2) for u in half(i, h)]

    def half(i, h):
        slots = 1 if isinstance(i, int) and HALF * (2 * i + h) >= SLOT1 else 2
        return [(slot, h, 2 * i + h) for slot in range(slots)]


    def ents(slot, n):
        return pl.ds(SLOT1 * slot + HALF * n, HALF)

    def relay_x(i):
        for slot, h, n in halves(i):
            @pl.when(n <= lims[slot])
            def _(slot=slot, n=n):
                mine = kvr.at[ents(slot, n), x, c]
                landed(mine, kr1.at[nr(slot, n)])
                remote(mine, mine, s_x.at[nr(slot, n)], kr2.at[nr(slot, n), 0], right).start()
                remote(mine, mine, s_x.at[nr(slot, n)], kr2.at[nr(slot, n), 1], left).start()

    def relay_x2(i):
        for slot, h, n in halves(i):
            @pl.when(n <= lims[slot])
            def _(slot=slot, h=h, n=n):
                theirs = kvr.at[ents(slot, n), (x + 3 - 2 * h) % 4, c]
                landed(theirs, kr2.at[nr(slot, n), h])
                remote(theirs, theirs, s_x.at[nr(slot, n)], kr2.at[nr(slot, n), 1 - h], left if h else right).start()

    def relay_core(i):
        for slot, h, n in halves(i):
            @pl.when(n <= lims[slot])
            def _(slot=slot, h=h, n=n):
                landed(kvr.at[ents(slot, n), pl.ds(0, 2), c], kr2.at[nr(slot, n), 1 - h])
                both = kvr.at[ents(slot, n), :, c]
                remote(both, both, s_core.at[nr(slot, n)], kr3.at[nr(slot, n)], partner).start()

    relay_x(0)
    relay_x(1)
    relay_x2(0)
    relay_x(2)
    relay_core(0)
    relay_x2(1)
    relay_x(3)

    def prep_q(t):
        landed(qraw.at[t], tr.at[t, 0])
        landed(csr.at[t], tr.at[t, 1])
        rq = turn(qraw[t].astype(F32), csr[t], 1)
        qn[t] = rq
        qa[t] = rq.T

    def upto(t, lo, hi):
        return jnp.minimum(jnp.maximum(nch[t] - lo, 0), hi - lo)

    def sums(counts):
        out = [jnp.int32(0)]
        for v in counts:
            out.append(out[-1] + v)
        return out

    def tile_of(i, ends):
        t = jnp.int32(0)
        for n in range(1, 6):
            t = t + (i >= ends[n]).astype(jnp.int32)
        return t

    low = sums([upto(t, 0, PP) for t in range(6)])
    high = sums([upto(t, PP, 16) for t in range(6)])

    def run(count, pair, last, between=None):
        quads = (count - 1) // 4

        def quad(b):
            for u in range(4):
                pair(4 * b + u, 4 * b, u)
        if between is None:
            pl.loop(0, quads)(quad)
        else:
            @pl.loop(0, quads)
            def _(b):
                @pl.when(b == 2)
                def _():
                    between()
                quad(b)

            @pl.when(quads <= 2)
            def _():
                between()
        rest = (count - 1) % 4
        for r in range(4):
            @pl.when(rest == r)
            def _(r=r):
                for u in range(r):
                    pair(4 * quads + u, 4 * quads, u)
                last(4 * quads + r, 4 * quads, r)

    def keys(e):
        return kvr[e, :, :, :, :HEAD].reshape(CK, HEAD)

    def values(e):
        return kvr[e, :, :, :, HEAD:].reshape(CK, HEAD)

    @pl.loop(0, 4)
    def _(k):
        @pl.when((k >= 1) & (k <= 2))
        def _():
            relay_x2(k + 1)

        @pl.when((k >= 1) & (k <= 3))
        def _():
            relay_core(k)
        @pl.when(k < 3)
        def _():
            prep_q(2 * k)
            prep_q(2 * k + 1)
        @pl.when(k == 1)
        def _():
            send_do()
        for i in range(PIECES):
            for slot, h, n in halves(i):
                @pl.when((n <= lims[slot]) & (k == (0 if i == 0 else 3)))
                def _(slot=slot, n=n):
                    landed(kvr.at[ents(slot, n), :, 1 - c], kr3.at[nr(slot, n)])
                    for v in range(HALF):
                        e = SLOT1 * slot + HALF * n + v
                        kt[e] = keys(e).T
                        vt[e] = values(e).T

        first = sel(k, [low[0], low[2], low[4], low[6]])
        start = first
        count = sel(k, [low[2], low[4], low[6], low[6] + high[6]]) - first

        def dec(i):
            i = i + jnp.where(k < 3, first, 0)
            ends = [jnp.where(k < 3, low[t], high[t]) for t in range(6)]
            t = tile_of(i, ends)
            ch = jnp.where(k < 3, 0, PP) + i - sel(t, ends)
            return t, ch, sel(t, ebase) + ch

        def s_step(i, sb, u):
            t, ch, e = dec(i)
            mask = jnp.where(ch == sel(t, nch) - 1, 1 + sel(t, par), 0)
            ka = jnp.concatenate([keys(e), mk[mask]], axis=1)
            qh = jnp.concatenate([qa[t], hot[...]], axis=0)
            sv = dot(ka, qh) * C2
            sc.at[pl.ds(sb, 5)][u] = sv
            mx.at[pl.ds(sb, 5)][u] = jnp.max(sv.reshape(CK // 8, 8, ROWS), axis=0)

        def o_step(i, sb, u):
            t, ch, e = dec(i)
            mo = mst[t]
            mn = jnp.maximum(mo, max8(mx.at[pl.ds(sb, 5)][u]))
            al = jnp.exp2(mo - mn)
            ev = jnp.exp2(sub8(sc.at[pl.ds(sb, 5)][u], mn))
            mst[t] = mn
            lst[t] = lst[t] * al + jnp.sum(ev, axis=0)
            ot[t] = (ot[t].reshape(-1, 8, ROWS) * al[None]).reshape(HEAD, ROWS) + dot(vt[e], ev.reshape(CK, ROWS).astype(BF))

        def pair(i, b, u):
            s_step(i + 1, start + b, u + 1)
            o_step(i, start + b, u)

        @pl.when(count > 0)
        def _():
            s_step(jnp.int32(0), start, 0)
            run(count, pair, lambda i, b, u: o_step(i, start + b, u))

    landed_many(mx, N_KV, s_one)
    for slot in range(2):
        @pl.loop(0, lims[slot] + 1)
        def _(n, slot=slot):
            landed(kvr.at[ents(slot, n), pl.ds(0, 3), c], s_x.at[nr(slot, n)])
            landed(kvr.at[ents(slot, n), :, c], s_core.at[nr(slot, n)])

    for t in range(6):
        landed(dor.at[t], tr.at[t, 2])
        dot_t[t] = dor[t].T
        l = sum8(lst[t])
        o = (ot[t].reshape(-1, 8, ROWS) / l[None]).reshape(HEAD, ROWS).astype(BF)
        qraw[t] = o.T
        dev = device(pos[t] // 2, x, par[t])
        send(qraw.at[t], att.at[seq_g[t // 2]], os_.at[t], or_, dev, me)
        dst[t] = sum8(jnp.sum((o.astype(F32) * dot_t[t].astype(F32)).reshape(-1, 8, ROWS), axis=0))
        mst[t] = mst[t] + jnp.log2(l)
        ot[t] = jnp.zeros((HEAD, ROWS), F32)

    def sum_core(units):
        for slot, h, n in units:
            @pl.when(n <= lims[slot])
            def _(slot=slot, n=n):
                remote(acc.at[ents(slot, n), :, 1 - c], peer.at[ents(slot, n)], s_core.at[nr(slot, n)], ar1.at[nr(slot, n)], partner).start()

    def sum_x(units):
        for slot, h, n in units:
            @pl.when(n <= lims[slot])
            def _(slot=slot, h=h, n=n):
                es = ents(slot, n)
                add_peer(slot, n)
                one, other = (left, right) if h else (right, left)
                remote(acc.at[es, (x + 2) % 4, c], xr.at[2, es], s_x.at[nr(slot, n)], ar2.at[nr(slot, n), 0], one).start()
                remote(acc.at[es, (x + 3 - 2 * h) % 4, c], xr.at[1 - h, es], s_x.at[nr(slot, n)], ar2.at[nr(slot, n), 1], other).start()

    def add_peer(slot, n):
        landed(peer.at[ents(slot, n)], ar1.at[nr(slot, n)])
        for v in range(HALF):
            e = SLOT1 * slot + HALF * n + v
            acc[e, :, c] += peer[e]

    def sum_direct(units):
        for slot, h, n in units:
            @pl.when(n <= lims[slot])
            def _(slot=slot, n=n):
                es = ents(slot, n)
                add_peer(slot, n)
                for d in range(3):
                    to = (x + d + 1) % 4
                    remote(acc.at[es, to, c], xr.at[d, es], s_x.at[nr(slot, n)], ar2.at[nr(slot, n), 1], device(place, to, c)).start()

    def home_direct(units):
        for slot, h, n in units:
            @pl.when(n <= lims[slot])
            def _(slot=slot, n=n):
                landed(xr.at[:, ents(slot, n)], ar2.at[nr(slot, n), 1])
                go_home(slot, n, (0, 1, 2))

    def go_home(slot, n, parts):
        for v in range(HALF):
            to = HALF * n + v
            e = SLOT1 * slot + to
            total = acc[e, x, c]
            for d in parts:
                total = total + xr[d, e]
            zs[e] = total
            send(zs.at[e], home.at[seqs[slot], nths[slot]], s_one, ar3, device(to, x, c), me)

    def sum_x2(units):
        for slot, h, n in units:
            @pl.when(n <= lims[slot])
            def _(slot=slot, h=h, n=n):
                es = ents(slot, n)
                to = (x + 1 + 2 * h) % 4
                landed(xr.at[2, es], ar2.at[nr(slot, n), 0])
                acc[es, to, c] += xr[2, es]
                remote(acc.at[es, to, c], xr.at[h, es], s_x.at[nr(slot, n)], ar2.at[nr(slot, n), 1], left if h else right).start()

    def sum_home(units):
        for slot, h, n in units:
            @pl.when(n <= lims[slot])
            def _(slot=slot, h=h, n=n):
                landed(xr.at[pl.ds(0, 2), ents(slot, n)], ar2.at[nr(slot, n), 1])
                go_home(slot, n, (0, 1))

    at = [half(n // 2, n % 2) for n in range(HALVES)]
    FROM = (12, 8, 2, 0, 4, 6)
    CORE = (at[7] + at[6], at[5] + at[4], at[1], at[0], at[2], (), (), at[3])
    HOOKS = (
        (), ((sum_x, at[7] + at[6]),), ((sum_x2, at[7] + at[6]), (sum_x, at[5] + at[4])),
        ((sum_x2, at[5] + at[4]), (sum_x, at[1])), ((sum_home, at[7] + at[6]), (sum_x2, at[1]), (sum_x, at[0])),
        ((sum_home, at[5] + at[4]),), ((sum_x2, at[0]), (sum_direct, at[2])), ((sum_home, at[1]),))

    @pl.loop(0, 8)
    def _(back):
        lo = sel(jnp.minimum(back, 5), FROM)
        hi = lo + jnp.where(back < 2, 4, 2)
        steps = sums([jnp.where((back < 5) | (back == 5 + t // 2), upto(t, lo, hi), 0) for t in range(6)])
        count = steps[6]

        def dec(i):
            t = tile_of(i, steps)
            ch = lo + i - sel(t, steps[:6])
            where = jnp.where(lo < PP, sel(t, low[:6]), low[6] + sel(t, high[:6]) - PP)
            return t, ch, sel(t, ebase) + ch, where + ch

        def between():
            for n in range(1, 8):
                @pl.when(back == n)
                def _(n=n):
                    for job, units in HOOKS[n]:
                        job(units)

        def d_step(i, u):
            t, ch, e, si = dec(i)
            dp_ref[u % 2] = dot(values(e), dot_t[t])

        def g_step(i, u, ahead):
            t, ch, e, si = dec(i)
            pr = jnp.exp2(sub8(sc[si], mst[t]))
            prb = pr.reshape(CK, ROWS).astype(BF)
            acc[e, :, :, :, HEAD:] += dot(prb, dor[t]).reshape(4, 2, BLK, HEAD)
            ahead()
            ds = (pr * sub8(dp_ref[u % 2], dst[t])).reshape(CK, ROWS).astype(BF)
            ot[t] += dot(kt[e], ds)
            acc[e, :, :, :, :HEAD] += dot(ds, qn[t]).reshape(4, 2, BLK, HEAD)

        @pl.when(count > 0)
        def _():
            d_step(jnp.int32(0), 0)
            run(count, lambda i, b, u: g_step(i, u, lambda: d_step(i + 1, u + 1)),
                lambda i, b, u: g_step(i, u, lambda: None), between)
        for n in range(8):
            @pl.when(back == n)
            def _(n=n):
                sum_core(CORE[n])

        @pl.when(back >= 5)
        def _():
            for tl in range(2):
                t = 2 * (back - 5) + tl
                seq = sel(back - 5, seq_g)
                qn[t] = turn((ot[t] * SCALE).T, csr[t], -1)
                dev = device(sel(t, pos) // 2, x, sel(t, par))
                send(qn.at[t], gq.at[seq], os_.at[t], or_, dev, me)

    sum_direct(at[3])
    sum_home(at[0])
    for s in range(SEQS):
        _, _, dev = work_of(s)

        @pl.when(dev != me)
        def _(s=s):
            landed(q.at[pl.ds(0, 2)], ts.at[s, 0])
            landed(csl, ts.at[s, 1])
    home_direct(at[2])
    home_direct(at[3])
    landed_many(zs, N_HOME, ar3)
    for s in range(SEQS):
        for m, (chip, slot, last) in enumerate(CHIPS[s]):
            @pl.when(half_me > last)
            def _(s=s, m=m):
                home[s, m] = jnp.zeros((BLK, TWO), F32)
        total = home[s, 0]
        for m in range(1, len(CHIPS[s])):
            total = total + home[s, m]
        dk = total[:, :HEAD] * SCALE
        other = jnp.concatenate([dk[:, HH:], dk[:, :HH]], axis=1)
        gk[s] = (dk * cos - other * sin).astype(BF)
        gv[s] = total[:, HEAD:].astype(BF)

    landed(sc.at[pl.ds(0, 3)], or_)
    for slot in range(2):
        @pl.loop(0, lims[slot] + 1)
        def _(n, slot=slot):
            landed(peer.at[ents(slot, n)], s_core.at[nr(slot, n)])
            landed(xr.at[:, ents(slot, n)], s_x.at[nr(slot, n)])
    landed_many(zs, N_SUMS, s_one)
    for t in range(6):
        @pl.when(pos[t] != p)
        def _(t=t):
            landed(qraw.at[pl.ds(0, 2)], os_.at[t])


def run_whole(q, do, key, value, pos32, freq):
    dma = pltpu.SemaphoreType.DMA
    nh = ENT // HALF
    any_ = pl.BlockSpec(memory_space=pl.ANY)
    vm = pl.BlockSpec(memory_space=pltpu.VMEM)
    v = pltpu.VMEM
    return pl.pallas_call(
        whole_step,
        in_specs=[any_] * 5 + [vm], out_specs=[vm] * 4,
        out_shape=[v((6, ROWS, HEAD), BF), v((6, ROWS, HEAD), BF), v((6, BLK, HEAD), BF), v((6, BLK, HEAD), BF)],
        scratch_shapes=[
            v((6, ROWS, HEAD), BF), v((6, ROWS, HEAD), BF), v((6, BLK, HEAD), F32), v((ENT, 4, 2, BLK, TWO), BF),
            v((6, ROWS, HEAD), BF), v((6, HEAD, ROWS), BF), v((6, HEAD, ROWS), BF), v((HEAD, ROWS), BF), v((3, CK, HEAD), BF),
            v((ENT, HEAD, CK), BF), v((ENT, HEAD, CK), BF),
            v((SIDX, CK, ROWS), F32), v((SIDX, 8, ROWS), F32), v((6, 8, ROWS), F32), v((6, 8, ROWS), F32), v((6, 8, ROWS), F32),
            v((6, HEAD, ROWS), F32), v((2, CK, ROWS), F32), v((BLK, HEAD), F32),
            v((ENT, 4, 2, BLK, TWO), F32), v((ENT, 4, BLK, TWO), F32), v((3, ENT, BLK, TWO), F32), v((ENT, BLK, TWO), F32),
            v((SEQS, NCH, BLK, TWO), F32), v((SEQS, BLK, HEAD), BF), v((SEQS, BLK, TWO), BF), pltpu.SMEM((BLK,), jnp.int32),
            dma((nh,)), dma((nh, 2)), dma((nh,)), dma((6, 2)), dma((6, 3)), dma((6,)), dma((nh,)), dma((nh, 2)),
            dma(()), dma((nh,)), dma((nh,)), dma(()), dma(()), dma((3,))],
        compiler_params=pltpu.CompilerParams(has_side_effects=True, collective_id=0, vmem_limit_bytes=62500000),
        name='whole_step')(q, do, key, value, pos32, pltpu.with_memory_space_constraint(freq, pltpu.VMEM))


def put(*refs):
    here, there, sem = refs[:4], refs[4:8], refs[8]
    copies = [pltpu.make_async_copy(a, b, sem.at[n]) for n, (a, b) in enumerate(zip(here, there))]
    for copy in copies:
        copy.start()
    for copy in copies:
        copy.wait()


def run_put(*arrays):
    any_ = pl.BlockSpec(memory_space=pl.ANY)
    return pl.pallas_call(
        put, in_specs=[any_] * 4, out_specs=[any_] * 4,
        out_shape=[jax.ShapeDtypeStruct(a.shape, a.dtype) for a in arrays],
        scratch_shapes=[pltpu.SemaphoreType.DMA((4,))], name='put')(*[pltpu.with_memory_space_constraint(a, pltpu.VMEM) for a in arrays])


def solution(mesh):
    query_spec = PS('dp', 'cp', None, None)
    kv_spec = PS('dp', 'cp', None)
    pos_spec = PS(('dp', 'cp'))

    def per_device(query, key, value, positions, grad_out):
        inv_freq = jnp.power(jnp.float32(ROPE_BASE), -2.0 * jnp.arange(HH, dtype=F32) / HEAD)
        att, gq, gk, gv = run_whole(query.reshape(6, ROWS, HEAD), grad_out.reshape(6, ROWS, HEAD), key, value, positions, inv_freq[None])
        att, gq, gk, gv = run_put(att, gq, gk, gv)
        return att.reshape(query.shape), gq.reshape(query.shape), gk, gv

    return jax.shard_map(per_device, mesh=mesh, in_specs=(query_spec, kv_spec, kv_spec, pos_spec, query_spec),
                         out_specs=(query_spec, query_spec, kv_spec, kv_spec), check_vma=False)
```

```python
import jax
import jax.numpy as jnp
from jax import lax
from jax.experimental import pallas as pl
from jax.experimental.pallas import tpu as pltpu
from jax.sharding import PartitionSpec as PS

ROPE_BASE = 10000
SEQS, HEADS, HEAD, BLK = 6, 16, 128, 32
ROWS = BLK * HEADS
CK = 256
ENT = 20
SLOT1 = 10
SIDX = 55
SCALE = HEAD ** -0.5
C2 = SCALE * 1.4426950408889634
BIG = 1e30
HH, TWO = HEAD // 2, 2 * HEAD
BF, F32 = jnp.bfloat16, jnp.float32
MESH = pl.DeviceIdType.MESH

PLACE = [int(d, 16) for d in 'E47B1560328CDA9F']
ORDER = [[int(d, 16) for d in row] for row in (
    '5423018967BAFECD',
    'EF8967BA542301DC',
    'CDFEBA9854760123',
    '1076982345BAFEDC',
    'FE1076893245BACD',
    'CDFEBA8945671032')]
PIECES = 4
PP = 16 // PIECES
HALF = PP // 2
HALVES = 16 // HALF


def _tables():
    work = {}
    dest = [[0] * 16 for _ in range(SEQS)]
    limit = {}
    slots = {}
    for s in range(SEQS):
        for i, j in enumerate(ORDER[s]):
            q = 16 * (s % 3) + i
            f, core, g = q // 6, q % 2, q % 6 // 2
            big_c = 8 * (s // 3) + f
            slot = s % 3 - (6 * f) // 16
            slots[big_c, s] = slot
            work[PLACE[big_c], core, g] = (s, j, slot)
            dest[s][j] = PLACE[big_c] * 8 + core * 4 + g
            limit[big_c, s] = max(limit.get((big_c, s), 0), ((31 - j) // 2) // HALF)
    chips = [[(PLACE[c], slots[c, t], limit[c, t]) for (c, t) in sorted(slots) if t == s] for s in range(SEQS)]
    lim = [[-1] * 16, [-1] * 16]
    seq = [[0] * 16, [0] * 16]
    nth = [[0] * 16, [0] * 16]
    for s in range(SEQS):
        for n, (place, slot, last) in enumerate(chips[s]):
            lim[slot][place], seq[slot][place], nth[slot][place] = last, s, n
    meta = []
    for p in range(32):
        w = [work[p // 2, p % 2, g] for g in range(3)]
        meta.append([t[1] for t in w] + [t[2] for t in w] + [2 if lim[1][p // 2] >= 0 else 1] + [t[0] for t in w])
    return dest, chips, lim, seq, nth, meta


DEST, CHIPS, LIM, SEQ, NTH, META = _tables()
SWAP = [PLACE.index(n) // 8 for n in range(16)]
N_HOME = [sum(n // HALF <= last for row in CHIPS for _, _, last in row) for n in range(16)]
N_KV = [N_HOME[n] - sum(n // HALF <= last for row in CHIPS for chip, _, last in row if chip == n) for n in range(16)]
N_SUMS = [sum(HALF * (row[n] + 1) - (n < HALF * (row[n] + 1)) for row in LIM) for n in range(16)]
NCH = max(len(c) for c in CHIPS)


def lut(index, table):
    value = jnp.int32(table[0])
    for n in range(1, len(table)):
        if table[n] != table[n - 1]:
            value = jnp.where(index >= n, jnp.int32(table[n]), value)
    return value


def device(place, x, core):
    return place * 8 + 2 * x + core


def place_of():
    me = lax.axis_index('cp')
    return me, me % 2, (me // 2) % 4, me // 8


def send(src, dst, ssem, rsem, dev, me):
    @pl.when(dev != me)
    def _():
        pltpu.make_async_remote_copy(src, dst, ssem, rsem, device_id={'cp': dev}, device_id_type=MESH).start()

    @pl.when(dev == me)
    def _():
        pltpu.make_async_copy(src, dst, rsem).start()


def dot(a, b):
    return jnp.dot(a, b, preferred_element_type=F32)


def dot_tn(a, b):
    return lax.dot_general(a, b, (((0,), (0,)), ((), ())), preferred_element_type=F32)


def max8(v):
    return jnp.broadcast_to(jnp.max(v, axis=0, keepdims=True), (8, ROWS))


def sum8(v):
    return jnp.broadcast_to(jnp.sum(v, axis=0, keepdims=True), (8, ROWS))


def sub8(a, b):
    return a.reshape(-1, 8, ROWS) - b[None]


def turn(v, cs, sign):
    cos = jnp.concatenate([cs[:, :HH], cs[:, :HH]], axis=1)
    sin = jnp.concatenate([-cs[:, HH:], cs[:, HH:]], axis=1)
    v = v.reshape(BLK, HEADS, HEAD)
    other = jnp.concatenate([v[..., HH:], v[..., :HH]], axis=-1)
    if sign > 0:
        out = v * cos[:, None, :] + other * sin[:, None, :]
    else:
        out = v * cos[:, None, :] - other * sin[:, None, :]
    return out.astype(BF).reshape(ROWS, HEAD)


def nr(slot, n):
    return SLOT1 // HALF * slot + n


def landed(ref, sem):
    pltpu.make_async_copy(ref, ref, sem).wait()


def sel(t, values):
    out = values[0] + jnp.int32(0)
    for k in range(1, len(values)):
        out = jnp.where(t == k, values[k], out)
    return out


def whole_step(q, do, key, value, pos32, freq, att, gq, gk, gv,
               qraw, dor, csr, kvr, qn, qa, dot_t, hot, mk, sc, mx, mst, lst, dst, ot, dp_ref, csl,
               acc, peer, xr, zs, home, keyl, kv, posl,
               kr1, kr2, kr3, ts, tr, os_, ar1, ar2, s_one, s_x, s_core, or_, ar3, kl):
    me, c, x, place = place_of()
    p = 2 * place + c
    jme = jnp.minimum(p, 31 - p)
    hi = p // 16
    lims = [lut(place, LIM[slot]) for slot in range(2)]
    seqs = [lut(place, SEQ[slot]) for slot in range(2)]
    nths = [lut(place, NTH[slot]) for slot in range(2)]
    half_me = place // HALF
    jg = [lut(p, [META[n][g] for n in range(len(META))]) for g in range(3)]
    slot_g = [lut(p, [META[n][3 + g] for n in range(len(META))]) for g in range(3)]
    seq_g = [lut(p, [META[n][7 + g] for n in range(len(META))]) for g in range(3)]
    pos = [v for g in range(3) for v in (jg[g], 31 - jg[g])]
    nch = [v // 2 + 1 for v in pos]
    par = [v % 2 for v in pos]
    ebase = [SLOT1 * slot_g[t // 2] for t in range(6)]
    partner = me + 1 - 2 * c

    def landed_many(ref, counts, sem):
        many = lut(place, counts)
        for k in sorted(set(counts)):
            @pl.when(many == k)
            def _(k=k):
                landed(ref.at[pl.ds(0, k)], sem)

    def remote(src, dst, ssem, rsem, dev):
        return pltpu.make_async_remote_copy(src, dst, ssem, rsem, device_id={'cp': dev}, device_id_type=MESH)

    fetch = [pltpu.make_async_copy(pos32, posl, kl.at[2]), pltpu.make_async_copy(key, keyl, kl.at[0]),
             pltpu.make_async_copy(value, kv.at[:, :, HEAD:], kl.at[1])]
    for copy in fetch:
        copy.start()
    barrier = pltpu.get_barrier_semaphore()

    def greet(dev):
        pl.semaphore_signal(barrier, inc=1, device_id={'cp': dev}, device_id_type=MESH)

    @pl.loop(0, 16)
    def _(other):
        greet(device(other, x, 1 - c))

        @pl.when(other != place)
        def _():
            greet(device(other, x, c))
    for d in range(1, 4):
        greet(device(place, (x + d) % 4, c))
    for copy in fetch:
        copy.wait()
    inv = freq[...]
    for t in range(BLK):
        csl[t:t + 1, :HH] = posl[t].astype(F32) * inv
    ang = csl[:, :HH]
    csl[:, :HH] = jnp.cos(ang)
    csl[:, HH:] = jnp.sin(ang)
    tab = csl[...]
    cos = jnp.concatenate([tab[:, :HH], tab[:, :HH]], axis=1)
    sin = jnp.concatenate([-tab[:, HH:], tab[:, HH:]], axis=1)
    for s in range(SEQS):
        kf = keyl[s].astype(F32)
        kv[s, :, :HEAD] = (kf * cos + jnp.concatenate([kf[:, HH:], kf[:, :HH]], axis=1) * sin).astype(BF)
    pl.semaphore_wait(barrier, 34)

    def work_of(s):
        code = lut(jme, DEST[s])
        return code % 4, 2 * (code % 4) + hi, device(code // 8, x, (code // 4) % 2)

    def send_q():
        for g in range(3):
            for s in range(SEQS):
                when, k, dev = work_of(s)

                @pl.when(when == g)
                def _(s=s, k=k, dev=dev):
                    send(q.at[s], qraw.at[k], ts.at[s, 0], tr.at[k, 0], dev, me)
                    send(csl, csr.at[k], ts.at[s, 1], tr.at[k, 1], dev, me)

    def send_do():
        for s in range(SEQS):
            _, k, dev = work_of(s)
            send(do.at[s], dor.at[k], ts.at[s, 0], tr.at[k, 2], dev, me)

    for s in range(SEQS):
        for (chip, slot, last) in CHIPS[s]:
            @pl.when(half_me <= last)
            def _(s=s, chip=chip, slot=slot):
                send(kv.at[s], kvr.at[SLOT1 * slot + place, x, c], s_one, kr1.at[nr(slot, half_me)], device(chip, x, c), me)
    send_q()

    @pl.loop(0, ENT)
    def _(e):
        acc[e] = jnp.zeros((4, 2, BLK, TWO), F32)
    row = lax.broadcasted_iota(jnp.int32, (HEAD, ROWS), 0)
    col = lax.broadcasted_iota(jnp.int32, (HEAD, ROWS), 1)
    hot[...] = jnp.where(col // HEADS == row, 1.0, 0.0).astype(BF)
    ki = lax.broadcasted_iota(jnp.int32, (CK, HEAD), 0)
    di = lax.broadcasted_iota(jnp.int32, (CK, HEAD), 1)
    mk[0] = jnp.zeros((CK, HEAD), BF)
    for cc in range(2):
        mk[1 + cc] = jnp.where((di < BLK) & (ki > di + 64 * x + BLK * cc), -BIG, 0.0).astype(BF)

    @pl.loop(0, 6)
    def _(t):
        ot[t] = jnp.zeros((HEAD, ROWS), F32)
        mst[t] = jnp.full((8, ROWS), -BIG, F32)
        lst[t] = jnp.zeros((8, ROWS), F32)

    right = device(place, (x + 1) % 4, c)
    left = device(place, (x + 3) % 4, c)

    def halves(i):
        return [u for h in range(2) for u in half(i, h)]

    def half(i, h):
        slots = 1 if isinstance(i, int) and HALF * (2 * i + h) >= SLOT1 else 2
        return [(slot, (h + slot) % 2, 2 * i + h) for slot in range(slots)]


    def ents(slot, n):
        return pl.ds(SLOT1 * slot + HALF * n, HALF)

    def relay_x(i):
        for slot, h, n in halves(i):
            @pl.when(n <= lims[slot])
            def _(slot=slot, n=n):
                mine = kvr.at[ents(slot, n), x, c]
                landed(mine, kr1.at[nr(slot, n)])
                remote(mine, mine, s_x.at[nr(slot, n)], kr2.at[nr(slot, n), 0], right).start()
                remote(mine, mine, s_x.at[nr(slot, n)], kr2.at[nr(slot, n), 1], left).start()

    def relay_x2(i):
        for slot, h, n in halves(i):
            @pl.when(n <= lims[slot])
            def _(slot=slot, h=h, n=n):
                theirs = kvr.at[ents(slot, n), (x + 3 - 2 * h) % 4, c]
                landed(theirs, kr2.at[nr(slot, n), h])
                remote(theirs, theirs, s_x.at[nr(slot, n)], kr2.at[nr(slot, n), 1 - h], left if h else right).start()

    def relay_core(i):
        for slot, h, n in halves(i):
            @pl.when(n <= lims[slot])
            def _(slot=slot, h=h, n=n):
                landed(kvr.at[ents(slot, n), pl.ds(0, 2), c], kr2.at[nr(slot, n), 1 - h])
                both = kvr.at[ents(slot, n), :, c]
                remote(both, both, s_core.at[nr(slot, n)], kr3.at[nr(slot, n)], partner).start()

    relay_x(0)
    relay_x(1)
    relay_x2(0)
    relay_x(2)
    relay_core(0)
    relay_x2(1)
    relay_x(3)

    def prep_q(t):
        landed(qraw.at[t], tr.at[t, 0])
        landed(csr.at[t], tr.at[t, 1])
        rq = turn(qraw[t].astype(F32), csr[t], 1)
        qn[t] = rq
        qa[t] = rq.T

    def upto(t, lo, hi):
        return jnp.minimum(jnp.maximum(nch[t] - lo, 0), hi - lo)

    def sums(counts):
        out = [jnp.int32(0)]
        for v in counts:
            out.append(out[-1] + v)
        return out

    def tile_of(i, ends):
        t = jnp.int32(0)
        for n in range(1, 6):
            t = t + (i >= ends[n]).astype(jnp.int32)
        return t

    EDGES = (0, 4, 8, 16)
    part = [sums([upto(t, EDGES[k], EDGES[k + 1]) for t in range(6)]) for k in range(3)]
    begin = sums([ends[6] for ends in part])

    def run(count, pair, last, between):
        quads = (count - 1) // 4

        def quad(b):
            for u in range(4):
                pair(4 * b + u, 4 * b, u)
        @pl.loop(0, quads)
        def _(b):
            @pl.when(b == 2)
            def _():
                between()
            quad(b)

        @pl.when(quads <= 2)
        def _():
            between()
        rest = (count - 1) % 4
        for r in range(4):
            @pl.when(rest == r)
            def _(r=r):
                for u in range(r):
                    pair(4 * quads + u, 4 * quads, u)
                last(4 * quads + r, 4 * quads, r)

    def keys(e):
        return kvr[e, :, :, :, :HEAD].reshape(CK, HEAD)

    def values(e):
        return kvr[e, :, :, :, HEAD:].reshape(CK, HEAD)

    @pl.loop(0, 6)
    def _(t):
        prep_q(t)

    @pl.loop(0, 3)
    def _(k):
        @pl.when(k == 0)
        def _():
            send_do()

        @pl.when(k == 1)
        def _():
            relay_core(2)
            relay_core(3)
        for i in range(PIECES):
            for slot, h, n in halves(i):
                @pl.when((n <= lims[slot]) & (k == min(i, 2)))
                def _(slot=slot, n=n):
                    landed(kvr.at[ents(slot, n), :, 1 - c], kr3.at[nr(slot, n)])
        ends = [sel(k, [part[n][t] for n in range(3)]) for t in range(7)]
        start = sel(k, begin[:3])
        count = ends[6]

        def dec(i):
            t = tile_of(i, ends)
            ch = 4 * k + i - sel(t, ends[:6])
            return t, ch, sel(t, ebase) + ch

        def between():
            @pl.when(k == 0)
            def _():
                relay_x2(2)
                relay_core(1)
                relay_x2(3)

        def s_step(i, sb, u):
            t, ch, e = dec(i)
            mask = jnp.where(ch == sel(t, nch) - 1, 1 + sel(t, par), 0)
            ka = jnp.concatenate([keys(e), mk[mask]], axis=1)
            qh = jnp.concatenate([qa[t], hot[...]], axis=0)
            sv = dot(ka, qh) * C2
            sc.at[pl.ds(sb, 5)][u] = sv
            mx.at[pl.ds(sb, 5)][u] = jnp.max(sv.reshape(CK // 8, 8, ROWS), axis=0)

        def o_step(i, sb, u):
            t, ch, e = dec(i)
            mo = mst[t]
            mn = jnp.maximum(mo, max8(mx.at[pl.ds(sb, 5)][u]))
            al = jnp.exp2(mo - mn)
            ev = jnp.exp2(sub8(sc.at[pl.ds(sb, 5)][u], mn))
            mst[t] = mn
            lst[t] = lst[t] * al + jnp.sum(ev, axis=0)
            ot[t] = (ot[t].reshape(-1, 8, ROWS) * al[None]).reshape(HEAD, ROWS) + dot_tn(values(e), ev.reshape(CK, ROWS).astype(BF))

        def pair(i, b, u):
            s_step(i + 1, start + b, u + 1)
            o_step(i, start + b, u)

        @pl.when(count > 0)
        def _():
            s_step(jnp.int32(0), start, 0)
            run(count, pair, lambda i, b, u: o_step(i, start + b, u), between)

    landed_many(mx, N_KV, s_one)
    for slot in range(2):
        @pl.loop(0, lims[slot] + 1)
        def _(n, slot=slot):
            landed(kvr.at[ents(slot, n), pl.ds(0, 3), c], s_x.at[nr(slot, n)])
            landed(kvr.at[ents(slot, n), :, c], s_core.at[nr(slot, n)])

    for t in range(6):
        landed(dor.at[t], tr.at[t, 2])
        dot_t[t] = dor[t].T
        l = sum8(lst[t])
        o = (ot[t].reshape(-1, 8, ROWS) / l[None]).reshape(HEAD, ROWS).astype(BF)
        qraw[t] = o.T
        dev = device(pos[t] // 2, x, par[t])
        send(qraw.at[t], att.at[seq_g[t // 2]], os_.at[t], or_, dev, me)
        dst[t] = sum8(jnp.sum((o.astype(F32) * dot_t[t].astype(F32)).reshape(-1, 8, ROWS), axis=0))
        mst[t] = mst[t] + jnp.log2(l)
        ot[t] = jnp.zeros((HEAD, ROWS), F32)

    def sum_core(units):
        for slot, h, n in units:
            @pl.when(n <= lims[slot])
            def _(slot=slot, n=n):
                remote(acc.at[ents(slot, n), :, 1 - c], peer.at[ents(slot, n)], s_core.at[nr(slot, n)], ar1.at[nr(slot, n)], partner).start()

    def sum_x(units):
        for slot, h, n in units:
            @pl.when(n <= lims[slot])
            def _(slot=slot, h=h, n=n):
                es = ents(slot, n)
                add_peer(slot, n)
                one, other = (left, right) if h else (right, left)
                remote(acc.at[es, (x + 2) % 4, c], xr.at[2, es], s_x.at[nr(slot, n)], ar2.at[nr(slot, n), 0], one).start()
                remote(acc.at[es, (x + 3 - 2 * h) % 4, c], xr.at[1 - h, es], s_x.at[nr(slot, n)], ar2.at[nr(slot, n), 1], other).start()

    def add_peer(slot, n):
        landed(peer.at[ents(slot, n)], ar1.at[nr(slot, n)])
        for v in range(HALF):
            e = SLOT1 * slot + HALF * n + v
            acc[e, :, c] += peer[e]

    def sum_direct(units):
        for slot, h, n in units:
            @pl.when(n <= lims[slot])
            def _(slot=slot, n=n):
                es = ents(slot, n)
                add_peer(slot, n)
                for d in range(3):
                    to = (x + d + 1) % 4
                    remote(acc.at[es, to, c], xr.at[d, es], s_x.at[nr(slot, n)], ar2.at[nr(slot, n), 1], device(place, to, c)).start()

    def home_direct(units):
        for slot, h, n in units:
            @pl.when(n <= lims[slot])
            def _(slot=slot, n=n):
                landed(xr.at[:, ents(slot, n)], ar2.at[nr(slot, n), 1])
                go_home(slot, n, (0, 1, 2))

    def go_home(slot, n, parts):
        for v in range(HALF):
            to = HALF * n + v
            e = SLOT1 * slot + to
            total = acc[e, x, c]
            for d in parts:
                total = total + xr[d, e]
            zs[e] = total
            send(zs.at[e], home.at[seqs[slot], nths[slot]], s_one, ar3, device(to, x, c), me)

    def sum_x2(units):
        for slot, h, n in units:
            @pl.when(n <= lims[slot])
            def _(slot=slot, h=h, n=n):
                es = ents(slot, n)
                to = (x + 1 + 2 * h) % 4
                landed(xr.at[2, es], ar2.at[nr(slot, n), 0])
                acc[es, to, c] += xr[2, es]
                remote(acc.at[es, to, c], xr.at[h, es], s_x.at[nr(slot, n)], ar2.at[nr(slot, n), 1], left if h else right).start()

    def sum_home(units):
        for slot, h, n in units:
            @pl.when(n <= lims[slot])
            def _(slot=slot, h=h, n=n):
                landed(xr.at[pl.ds(0, 2), ents(slot, n)], ar2.at[nr(slot, n), 1])
                go_home(slot, n, (0, 1))

    at = [half(n // 2, n % 2) for n in range(HALVES)]
    swap = lut(place, SWAP)
    last_but_one = [(slot, slot, 2 + swap) for slot in range(2)]
    last = [(slot, 0, 3 - swap) for slot in range(2)]
    FROM = (12, 8, 2, 0, 4 + 2 * swap, 6 - 2 * swap)
    CORE = (at[7] + at[6], at[5] + at[4], at[1], at[0], last_but_one, (), (), last)
    HOOKS = (
        (), ((sum_x, at[7] + at[6]),), ((sum_x, at[5] + at[4]),), ((sum_x2, at[7] + at[6]), (sum_x, at[1])),
        ((sum_x2, at[5] + at[4]), (sum_x, at[0])), ((sum_home, at[7] + at[6]), (sum_x2, at[1])),
        ((sum_direct, last_but_one),), ((sum_x2, at[0]), (sum_home, at[5] + at[4])))

    def segment(back):
        lo = sel(jnp.minimum(back, 5), FROM)
        hi = lo + jnp.where(back < 2, 4, 2)
        steps = sums([jnp.where((back < 5) | (back == 5 + t // 2), upto(t, lo, hi), 0) for t in range(6)])

        def dec(i):
            t = tile_of(i, steps)
            ch = lo + i - sel(t, steps[:6])
            k = jnp.minimum(lo // 4, 2)
            where = sel(k, [begin[n] + sel(t, part[n][:6]) - EDGES[n] for n in range(3)])
            return t, ch, sel(t, ebase) + ch, where + ch
        return steps[6], dec

    def d_step(u, t, ch, e, si):
        dp_ref[u % 2] = dot(values(e), dot_t[t])

    skip = segment(0)[0] == 0
    d_step(0, *segment(skip.astype(jnp.int32))[1](0))

    @pl.loop(0, 8)
    def _(back):
        count, dec = segment(back)
        _, dec_next = segment(jnp.minimum(back + 1, 7))

        def between():
            for n in range(1, 8):
                @pl.when(back == n)
                def _(n=n):
                    for job, units in HOOKS[n]:
                        job(units)

        def g_step(i, u, ahead, after):
            t, ch, e, si = dec(i)
            pr = jnp.exp2(sub8(sc[si], mst[t]))
            prb = pr.reshape(CK, ROWS).astype(BF)
            acc[e, :, :, :, HEAD:] += dot(prb, dor[t]).reshape(4, 2, BLK, HEAD)
            ahead()
            ds = (pr * sub8(dp_ref[u % 2], dst[t])).reshape(CK, ROWS).astype(BF)
            ot[t] += dot_tn(keys(e), ds)
            acc[e, :, :, :, :HEAD] += dot(ds, qn[t]).reshape(4, 2, BLK, HEAD)
            after()

        def nothing():
            pass

        @pl.when(count > 0)
        def _():
            run(count, lambda i, b, u: g_step(i, u, lambda: d_step(u + 1, *dec(i + 1)), nothing),
                lambda i, b, u: g_step(i, u, nothing, lambda: d_step(0, *dec_next(0))), between)
        for n in range(8):
            @pl.when(back == n)
            def _(n=n):
                sum_core(CORE[n])

        @pl.when(back >= 5)
        def _():
            for tl in range(2):
                t = 2 * (back - 5) + tl
                seq = sel(back - 5, seq_g)
                qn[t] = turn((ot[t] * SCALE).T, csr[t], -1)
                dev = device(sel(t, pos) // 2, x, sel(t, par))
                send(qn.at[t], gq.at[seq], os_.at[t], or_, dev, me)

    sum_direct(last)
    sum_home(at[1])
    sum_home(at[0])
    for s in range(SEQS):
        _, _, dev = work_of(s)

        @pl.when(dev != me)
        def _(s=s):
            landed(q.at[pl.ds(0, 2)], ts.at[s, 0])
            landed(csl, ts.at[s, 1])
    home_direct(last_but_one)
    home_direct(last)
    landed_many(zs, N_HOME, ar3)
    for s in range(SEQS):
        for m, (chip, slot, last) in enumerate(CHIPS[s]):
            @pl.when(half_me > last)
            def _(s=s, m=m):
                home[s, m] = jnp.zeros((BLK, TWO), F32)
        total = home[s, 0]
        for m in range(1, len(CHIPS[s])):
            total = total + home[s, m]
        dk = total[:, :HEAD] * SCALE
        other = jnp.concatenate([dk[:, HH:], dk[:, :HH]], axis=1)
        gk[s] = (dk * cos - other * sin).astype(BF)
        gv[s] = total[:, HEAD:].astype(BF)

    landed(sc.at[pl.ds(0, 3)], or_)
    for slot in range(2):
        @pl.loop(0, lims[slot] + 1)
        def _(n, slot=slot):
            landed(peer.at[ents(slot, n)], s_core.at[nr(slot, n)])
            landed(xr.at[:, ents(slot, n)], s_x.at[nr(slot, n)])
    landed_many(zs, N_SUMS, s_one)
    for t in range(6):
        @pl.when(pos[t] != p)
        def _(t=t):
            landed(qraw.at[pl.ds(0, 2)], os_.at[t])


def run_whole(q, do, key, value, pos32, freq):
    dma = pltpu.SemaphoreType.DMA
    nh = ENT // HALF
    any_ = pl.BlockSpec(memory_space=pl.ANY)
    vm = pl.BlockSpec(memory_space=pltpu.VMEM)
    v = pltpu.VMEM
    return pl.pallas_call(
        whole_step,
        in_specs=[any_] * 5 + [vm], out_specs=[vm] * 4,
        out_shape=[v((6, ROWS, HEAD), BF), v((6, ROWS, HEAD), BF), v((6, BLK, HEAD), BF), v((6, BLK, HEAD), BF)],
        scratch_shapes=[
            v((6, ROWS, HEAD), BF), v((6, ROWS, HEAD), BF), v((6, BLK, HEAD), F32), v((ENT, 4, 2, BLK, TWO), BF),
            v((6, ROWS, HEAD), BF), v((6, HEAD, ROWS), BF), v((6, HEAD, ROWS), BF), v((HEAD, ROWS), BF), v((3, CK, HEAD), BF),
            v((SIDX, CK, ROWS), F32), v((SIDX, 8, ROWS), F32), v((6, 8, ROWS), F32), v((6, 8, ROWS), F32), v((6, 8, ROWS), F32),
            v((6, HEAD, ROWS), F32), v((2, CK, ROWS), F32), v((BLK, HEAD), F32),
            v((ENT, 4, 2, BLK, TWO), F32), v((ENT, 4, BLK, TWO), F32), v((3, ENT, BLK, TWO), F32), v((ENT, BLK, TWO), F32),
            v((SEQS, NCH, BLK, TWO), F32), v((SEQS, BLK, HEAD), BF), v((SEQS, BLK, TWO), BF), pltpu.SMEM((BLK,), jnp.int32),
            dma((nh,)), dma((nh, 2)), dma((nh,)), dma((6, 2)), dma((6, 3)), dma((6,)), dma((nh,)), dma((nh, 2)),
            dma(()), dma((nh,)), dma((nh,)), dma(()), dma(()), dma((3,))],
        compiler_params=pltpu.CompilerParams(has_side_effects=True, collective_id=0, vmem_limit_bytes=62500000),
        name='whole_step')(q, do, key, value, pos32, pltpu.with_memory_space_constraint(freq, pltpu.VMEM))


def put(*refs):
    here, there, sem = refs[:4], refs[4:8], refs[8]
    copies = [pltpu.make_async_copy(a, b, sem.at[n]) for n, (a, b) in enumerate(zip(here, there))]
    for copy in copies:
        copy.start()
    for copy in copies:
        copy.wait()


def run_put(*arrays):
    any_ = pl.BlockSpec(memory_space=pl.ANY)
    return pl.pallas_call(
        put, in_specs=[any_] * 4, out_specs=[any_] * 4,
        out_shape=[jax.ShapeDtypeStruct(a.shape, a.dtype) for a in arrays],
        scratch_shapes=[pltpu.SemaphoreType.DMA((4,))], name='put')(*[pltpu.with_memory_space_constraint(a, pltpu.VMEM) for a in arrays])


def solution(mesh):
    query_spec = PS('dp', 'cp', None, None)
    kv_spec = PS('dp', 'cp', None)
    pos_spec = PS(('dp', 'cp'))

    def per_device(query, key, value, positions, grad_out):
        inv_freq = jnp.power(jnp.float32(ROPE_BASE), -2.0 * jnp.arange(HH, dtype=F32) / HEAD)
        att, gq, gk, gv = run_whole(query.reshape(6, ROWS, HEAD), grad_out.reshape(6, ROWS, HEAD), key, value, positions, inv_freq[None])
        att, gq, gk, gv = run_put(att, gq, gk, gv)
        return att.reshape(query.shape), gq.reshape(query.shape), gk, gv

    return jax.shard_map(per_device, mesh=mesh, in_specs=(query_spec, kv_spec, kv_spec, pos_spec, query_spec),
                         out_specs=(query_spec, query_spec, kv_spec, kv_spec), check_vma=False)
```

```python
import jax
import jax.numpy as jnp
from jax import lax
from jax.experimental import pallas as pl
from jax.experimental.pallas import tpu as pltpu
from jax.sharding import PartitionSpec as PS

ROPE_BASE = 10000
SEQS, HEADS, HEAD, BLK = 6, 16, 128, 32
ROWS = BLK * HEADS
CK = 256
ENT = 20
SLOT1 = 10
SIDX = 55
SCALE = HEAD ** -0.5
C2 = SCALE * 1.4426950408889634
BIG = 1e30
HH, TWO = HEAD // 2, 2 * HEAD
BF, F32 = jnp.bfloat16, jnp.float32
MESH = pl.DeviceIdType.MESH

PLACE = [int(d, 16) for d in 'E47B1560328CDA9F']
ORDER = [[int(d, 16) for d in row] for row in (
    '5423018967BAFECD',
    'EF8967BA542301DC',
    'CDFEBA9854760123',
    '1076982345BAFEDC',
    'FE1076893245BACD',
    'CDFEBA8945671032')]
PIECES = 4
PP = 16 // PIECES
HALF = PP // 2
HALVES = 16 // HALF


def _tables():
    work = {}
    dest = [[0] * 16 for _ in range(SEQS)]
    limit = {}
    slots = {}
    for s in range(SEQS):
        for i, j in enumerate(ORDER[s]):
            q = 16 * (s % 3) + i
            f, core, g = q // 6, q % 2, q % 6 // 2
            big_c = 8 * (s // 3) + f
            slot = s % 3 - (6 * f) // 16
            slots[big_c, s] = slot
            work[PLACE[big_c], core, g] = (s, j, slot)
            dest[s][j] = PLACE[big_c] * 8 + core * 4 + g
            limit[big_c, s] = max(limit.get((big_c, s), 0), ((31 - j) // 2) // HALF)
    chips = [[(PLACE[c], slots[c, t], limit[c, t]) for (c, t) in sorted(slots) if t == s] for s in range(SEQS)]
    lim = [[-1] * 16, [-1] * 16]
    seq = [[0] * 16, [0] * 16]
    nth = [[0] * 16, [0] * 16]
    for s in range(SEQS):
        for n, (place, slot, last) in enumerate(chips[s]):
            lim[slot][place], seq[slot][place], nth[slot][place] = last, s, n
    meta = []
    for p in range(32):
        w = [work[p // 2, p % 2, g] for g in range(3)]
        meta.append([t[1] for t in w] + [t[2] for t in w] + [2 if lim[1][p // 2] >= 0 else 1] + [t[0] for t in w])
    return dest, chips, lim, seq, nth, meta


DEST, CHIPS, LIM, SEQ, NTH, META = _tables()
SWAP = [PLACE.index(n) // 8 for n in range(16)]
N_HOME = [sum(n // HALF <= last for row in CHIPS for _, _, last in row) for n in range(16)]
N_KV = [N_HOME[n] - sum(n // HALF <= last for row in CHIPS for chip, _, last in row if chip == n) for n in range(16)]
N_SUMS = [sum(HALF * (row[n] + 1) - (n < HALF * (row[n] + 1)) for row in LIM) for n in range(16)]
NCH = max(len(c) for c in CHIPS)


def lut(index, table):
    value = jnp.int32(table[0])
    for n in range(1, len(table)):
        if table[n] != table[n - 1]:
            value = jnp.where(index >= n, jnp.int32(table[n]), value)
    return value


def device(place, x, core):
    return place * 8 + 2 * x + core


def dispatch(i, jobs, first=0):
    if len(jobs) == 1:
        jobs[0]()
        return
    cut = len(jobs) // 2
    for part, at, test in ((jobs[:cut], first, i < first + cut), (jobs[cut:], first + cut, i >= first + cut)):
        if any(part):
            @pl.when(test)
            def _(part=part, at=at):
                dispatch(i, part, at)


def place_of():
    me = lax.axis_index('cp')
    return me, me % 2, (me // 2) % 4, me // 8


def send(src, dst, ssem, rsem, dev, me):
    @pl.when(dev != me)
    def _():
        pltpu.make_async_remote_copy(src, dst, ssem, rsem, device_id={'cp': dev}, device_id_type=MESH).start()

    @pl.when(dev == me)
    def _():
        pltpu.make_async_copy(src, dst, rsem).start()


def dot(a, b):
    return jnp.dot(a, b, preferred_element_type=F32)


def dot_tn(a, b):
    return lax.dot_general(a, b, (((0,), (0,)), ((), ())), preferred_element_type=F32)


def max8(v):
    return jnp.broadcast_to(jnp.max(v, axis=0, keepdims=True), (8, ROWS))


def sum8(v):
    return jnp.broadcast_to(jnp.sum(v, axis=0, keepdims=True), (8, ROWS))


def sub8(a, b):
    return a.reshape(-1, 8, ROWS) - b[None]


def turn(v, cs, sign):
    cos = jnp.concatenate([cs[:, :HH], cs[:, :HH]], axis=1)
    sin = jnp.concatenate([-cs[:, HH:], cs[:, HH:]], axis=1)
    v = v.reshape(BLK, HEADS, HEAD)
    other = jnp.concatenate([v[..., HH:], v[..., :HH]], axis=-1)
    if sign > 0:
        out = v * cos[:, None, :] + other * sin[:, None, :]
    else:
        out = v * cos[:, None, :] - other * sin[:, None, :]
    return out.astype(BF).reshape(ROWS, HEAD)


def nr(slot, n):
    return SLOT1 // HALF * slot + n


def landed(ref, sem):
    pltpu.make_async_copy(ref, ref, sem).wait()


def sel(t, values):
    out = values[0] + jnp.int32(0)
    for k in range(1, len(values)):
        out = jnp.where(t == k, values[k], out)
    return out


def whole_step(q, do, key, value, pos32, freq, att, gq, gk, gv,
               qraw, dor, csr, kvr, qn, qa, dot_t, hot, mk, sc, mx, mst, lst, dst, ot, dp_ref, csl,
               acc, peer, xr, zs, home, keyl, kv, posl,
               kr1, kr2, kr3, ts, tr, os_, ar1, ar2, s_one, s_x, s_core, or_, ar3, kl):
    me, c, x, place = place_of()
    p = 2 * place + c
    jme = jnp.minimum(p, 31 - p)
    hi = p // 16
    lims = [lut(place, LIM[slot]) for slot in range(2)]
    seqs = [lut(place, SEQ[slot]) for slot in range(2)]
    nths = [lut(place, NTH[slot]) for slot in range(2)]
    half_me = place // HALF
    jg = [lut(p, [META[n][g] for n in range(len(META))]) for g in range(3)]
    slot_g = [lut(p, [META[n][3 + g] for n in range(len(META))]) for g in range(3)]
    seq_g = [lut(p, [META[n][7 + g] for n in range(len(META))]) for g in range(3)]
    pos = [v for g in range(3) for v in (jg[g], 31 - jg[g])]
    nch = [v // 2 + 1 for v in pos]
    par = [v % 2 for v in pos]
    ebase = [SLOT1 * slot_g[t // 2] for t in range(6)]
    partner = me + 1 - 2 * c

    def landed_many(ref, counts, sem):
        many = lut(place, counts)
        for k in sorted(set(counts)):
            @pl.when(many == k)
            def _(k=k):
                landed(ref.at[pl.ds(0, k)], sem)

    def remote(src, dst, ssem, rsem, dev):
        return pltpu.make_async_remote_copy(src, dst, ssem, rsem, device_id={'cp': dev}, device_id_type=MESH)

    fetch = [pltpu.make_async_copy(pos32, posl, kl.at[2]), pltpu.make_async_copy(key, keyl, kl.at[0]),
             pltpu.make_async_copy(value, kv.at[:, :, HEAD:], kl.at[1])]
    for copy in fetch:
        copy.start()
    barrier = pltpu.get_barrier_semaphore()

    def greet(dev):
        pl.semaphore_signal(barrier, inc=1, device_id={'cp': dev}, device_id_type=MESH)

    @pl.loop(0, 16)
    def _(other):
        greet(device(other, x, 1 - c))

        @pl.when(other != place)
        def _():
            greet(device(other, x, c))
    for d in range(1, 4):
        greet(device(place, (x + d) % 4, c))
    for copy in fetch:
        copy.wait()
    inv = freq[...]
    for t in range(BLK):
        csl[t:t + 1, :HH] = posl[t].astype(F32) * inv
    ang = csl[:, :HH]
    csl[:, :HH] = jnp.cos(ang)
    csl[:, HH:] = jnp.sin(ang)
    tab = csl[...]
    cos = jnp.concatenate([tab[:, :HH], tab[:, :HH]], axis=1)
    sin = jnp.concatenate([-tab[:, HH:], tab[:, HH:]], axis=1)
    for s in range(SEQS):
        kf = keyl[s].astype(F32)
        kv[s, :, :HEAD] = (kf * cos + jnp.concatenate([kf[:, HH:], kf[:, :HH]], axis=1) * sin).astype(BF)
    pl.semaphore_wait(barrier, 34)

    def work_of(s):
        code = lut(jme, DEST[s])
        return code % 4, 2 * (code % 4) + hi, device(code // 8, x, (code // 4) % 2)

    def send_q():
        for g in range(3):
            for s in range(SEQS):
                when, k, dev = work_of(s)

                @pl.when(when == g)
                def _(s=s, k=k, dev=dev):
                    send(q.at[s], qraw.at[k], ts.at[s, 0], tr.at[k, 0], dev, me)
                    send(csl, csr.at[k], ts.at[s, 1], tr.at[k, 1], dev, me)

    def send_do():
        for s in range(SEQS):
            _, k, dev = work_of(s)
            send(do.at[s], dor.at[k], ts.at[s, 0], tr.at[k, 2], dev, me)

    for s in range(SEQS):
        for (chip, slot, last) in CHIPS[s]:
            @pl.when(half_me <= last)
            def _(s=s, chip=chip, slot=slot):
                send(kv.at[s], kvr.at[SLOT1 * slot + place, x, c], s_one, kr1.at[nr(slot, half_me)], device(chip, x, c), me)
    send_q()

    @pl.loop(0, ENT)
    def _(e):
        acc[e] = jnp.zeros((4, 2, BLK, TWO), F32)
    row = lax.broadcasted_iota(jnp.int32, (HEAD, ROWS), 0)
    col = lax.broadcasted_iota(jnp.int32, (HEAD, ROWS), 1)
    hot[...] = jnp.where(col // HEADS == row, 1.0, 0.0).astype(BF)
    ki = lax.broadcasted_iota(jnp.int32, (CK, HEAD), 0)
    di = lax.broadcasted_iota(jnp.int32, (CK, HEAD), 1)
    mk[0] = jnp.zeros((CK, HEAD), BF)
    for cc in range(2):
        mk[1 + cc] = jnp.where((di < BLK) & (ki > di + 64 * x + BLK * cc), -BIG, 0.0).astype(BF)

    @pl.loop(0, 6)
    def _(t):
        ot[t] = jnp.zeros((HEAD, ROWS), F32)
        mst[t] = jnp.full((8, ROWS), -BIG, F32)
        lst[t] = jnp.zeros((8, ROWS), F32)

    right = device(place, (x + 1) % 4, c)
    left = device(place, (x + 3) % 4, c)

    def halves(i):
        return [u for h in range(2) for u in half(i, h)]

    def half(i, h):
        slots = 1 if isinstance(i, int) and HALF * (2 * i + h) >= SLOT1 else 2
        return [(slot, (h + slot) % 2, 2 * i + h) for slot in range(slots)]


    def ents(slot, n):
        return pl.ds(SLOT1 * slot + HALF * n, HALF)

    def relay_x(i):
        for slot, h, n in halves(i):
            @pl.when(n <= lims[slot])
            def _(slot=slot, n=n):
                mine = kvr.at[ents(slot, n), x, c]
                landed(mine, kr1.at[nr(slot, n)])
                remote(mine, mine, s_x.at[nr(slot, n)], kr2.at[nr(slot, n), 0], right).start()
                remote(mine, mine, s_x.at[nr(slot, n)], kr2.at[nr(slot, n), 1], left).start()

    def relay_x2(i):
        for slot, h, n in halves(i):
            @pl.when(n <= lims[slot])
            def _(slot=slot, h=h, n=n):
                theirs = kvr.at[ents(slot, n), (x + 3 - 2 * h) % 4, c]
                landed(theirs, kr2.at[nr(slot, n), h])
                remote(theirs, theirs, s_x.at[nr(slot, n)], kr2.at[nr(slot, n), 1 - h], left if h else right).start()

    def relay_core(i):
        for slot, h, n in halves(i):
            @pl.when(n <= lims[slot])
            def _(slot=slot, h=h, n=n):
                landed(kvr.at[ents(slot, n), pl.ds(0, 2), c], kr2.at[nr(slot, n), 1 - h])
                both = kvr.at[ents(slot, n), :, c]
                remote(both, both, s_core.at[nr(slot, n)], kr3.at[nr(slot, n)], partner).start()

    relay_x(0)
    relay_x(1)
    relay_x2(0)
    relay_x(2)
    relay_core(0)
    relay_x2(1)
    relay_x(3)

    def prep_q(t):
        landed(qraw.at[t], tr.at[t, 0])
        landed(csr.at[t], tr.at[t, 1])
        rq = turn(qraw[t].astype(F32), csr[t], 1)
        qn[t] = rq
        qa[t] = rq.T

    def upto(t, lo, hi):
        return jnp.minimum(jnp.maximum(nch[t] - lo, 0), hi - lo)

    def sums(counts):
        out = [jnp.int32(0)]
        for v in counts:
            out.append(out[-1] + v)
        return out

    def tile_of(i, ends):
        t = jnp.int32(0)
        for n in range(1, 6):
            t = t + (i >= ends[n]).astype(jnp.int32)
        return t

    EDGES = (0, 4, 8, 16)
    part = [sums([upto(t, EDGES[k], EDGES[k + 1]) for t in range(6)]) for k in range(3)]
    begin = sums([ends[6] for ends in part])

    def run(count, pair, last, between):
        eights = (count - 1) // 8
        rest = (count - 1) % 8

        def several(n, base):
            for u in range(n):
                pair(base + u, base, u, n + 1)

        @pl.loop(0, eights)
        def _(b):
            @pl.when(b == 1)
            def _():
                between()
            several(8, 8 * b)

        @pl.when(eights <= 1)
        def _():
            between()

        @pl.when(rest >= 4)
        def _():
            several(4, 8 * eights)
        base = 8 * eights + rest // 4 * 4
        for r in range(4):
            @pl.when(rest % 4 == r)
            def _(r=r):
                several(r, base)
                last(base + r, base, r, r + 1)

    def keys(e):
        return kvr[e, :, :, :, :HEAD].reshape(CK, HEAD)

    def values(e):
        return kvr[e, :, :, :, HEAD:].reshape(CK, HEAD)

    @pl.loop(0, 6)
    def _(t):
        prep_q(t)

    @pl.loop(0, 3)
    def _(k):
        @pl.when(k == 0)
        def _():
            send_do()

        @pl.when(k == 1)
        def _():
            relay_core(2)
            relay_core(3)
        for i in range(PIECES):
            for slot, h, n in halves(i):
                @pl.when((n <= lims[slot]) & (k == min(i, 2)))
                def _(slot=slot, n=n):
                    landed(kvr.at[ents(slot, n), :, 1 - c], kr3.at[nr(slot, n)])
        ends = [sel(k, [part[n][t] for n in range(3)]) for t in range(7)]
        start = sel(k, begin[:3])
        count = ends[6]

        def dec(i):
            t = tile_of(i, ends)
            ch = 4 * k + i - sel(t, ends[:6])
            return t, ch, sel(t, ebase) + ch

        def between():
            @pl.when(k == 0)
            def _():
                relay_x2(2)
                relay_core(1)
                relay_x2(3)

        def s_step(i, sb, u, w):
            t, ch, e = dec(i)
            mask = jnp.where(ch == sel(t, nch) - 1, 1 + sel(t, par), 0)
            ka = jnp.concatenate([keys(e), mk[mask]], axis=1)
            qh = jnp.concatenate([qa[t], hot[...]], axis=0)
            sv = dot(ka, qh) * C2
            sc.at[pl.ds(sb, w)][u] = sv
            mx.at[pl.ds(sb, w)][u] = jnp.max(sv.reshape(CK // 8, 8, ROWS), axis=0)

        def o_step(i, sb, u, w):
            t, ch, e = dec(i)
            mo = mst[t]
            mn = jnp.maximum(mo, max8(mx.at[pl.ds(sb, w)][u]))
            al = jnp.exp2(mo - mn)
            ev = jnp.exp2(sub8(sc.at[pl.ds(sb, w)][u], mn))
            mst[t] = mn
            lst[t] = lst[t] * al + jnp.sum(ev, axis=0)
            ot[t] = (ot[t].reshape(-1, 8, ROWS) * al[None]).reshape(HEAD, ROWS) + dot_tn(values(e), ev.reshape(CK, ROWS).astype(BF))

        def pair(i, b, u, w):
            s_step(i + 1, start + b, u + 1, w)
            o_step(i, start + b, u, w)

        @pl.when(count > 0)
        def _():
            s_step(jnp.int32(0), start, 0, 1)
            run(count, pair, lambda i, b, u, w: o_step(i, start + b, u, w), between)

    landed_many(mx, N_KV, s_one)
    for slot in range(2):
        @pl.loop(0, lims[slot] + 1)
        def _(n, slot=slot):
            landed(kvr.at[ents(slot, n), pl.ds(0, 3), c], s_x.at[nr(slot, n)])
            landed(kvr.at[ents(slot, n), :, c], s_core.at[nr(slot, n)])

    for t in range(6):
        landed(dor.at[t], tr.at[t, 2])
        dot_t[t] = dor[t].T
        l = sum8(lst[t])
        o = (ot[t].reshape(-1, 8, ROWS) / l[None]).reshape(HEAD, ROWS).astype(BF)
        qraw[t] = o.T
        dev = device(pos[t] // 2, x, par[t])
        send(qraw.at[t], att.at[seq_g[t // 2]], os_.at[t], or_, dev, me)
        dst[t] = sum8(jnp.sum((o.astype(F32) * dot_t[t].astype(F32)).reshape(-1, 8, ROWS), axis=0))
        mst[t] = mst[t] + jnp.log2(l)
        ot[t] = jnp.zeros((HEAD, ROWS), F32)

    def sum_core(units):
        for slot, h, n in units:
            @pl.when(n <= lims[slot])
            def _(slot=slot, n=n):
                remote(acc.at[ents(slot, n), :, 1 - c], peer.at[ents(slot, n)], s_core.at[nr(slot, n)], ar1.at[nr(slot, n)], partner).start()

    def sum_x(units):
        for slot, h, n in units:
            @pl.when(n <= lims[slot])
            def _(slot=slot, h=h, n=n):
                es = ents(slot, n)
                add_peer(slot, n)
                one, other = (left, right) if h else (right, left)
                remote(acc.at[es, (x + 2) % 4, c], xr.at[2, es], s_x.at[nr(slot, n)], ar2.at[nr(slot, n), 0], one).start()
                remote(acc.at[es, (x + 3 - 2 * h) % 4, c], xr.at[1 - h, es], s_x.at[nr(slot, n)], ar2.at[nr(slot, n), 1], other).start()

    def add_peer(slot, n):
        landed(peer.at[ents(slot, n)], ar1.at[nr(slot, n)])
        for v in range(HALF):
            e = SLOT1 * slot + HALF * n + v
            acc[e, :, c] += peer[e]

    def sum_direct(units):
        for slot, h, n in units:
            @pl.when(n <= lims[slot])
            def _(slot=slot, n=n):
                es = ents(slot, n)
                add_peer(slot, n)
                for d in range(3):
                    to = (x + d + 1) % 4
                    remote(acc.at[es, to, c], xr.at[d, es], s_x.at[nr(slot, n)], ar2.at[nr(slot, n), 1], device(place, to, c)).start()

    def home_direct(units):
        for slot, h, n in units:
            @pl.when(n <= lims[slot])
            def _(slot=slot, n=n):
                landed(xr.at[:, ents(slot, n)], ar2.at[nr(slot, n), 1])
                go_home(slot, n, (0, 1, 2))

    def go_home(slot, n, parts):
        for v in range(HALF):
            to = HALF * n + v
            e = SLOT1 * slot + to
            total = acc[e, x, c]
            for d in parts:
                total = total + xr[d, e]
            zs[e] = total
            send(zs.at[e], home.at[seqs[slot], nths[slot]], s_one, ar3, device(to, x, c), me)

    def sum_x2(units):
        for slot, h, n in units:
            @pl.when(n <= lims[slot])
            def _(slot=slot, h=h, n=n):
                es = ents(slot, n)
                to = (x + 1 + 2 * h) % 4
                landed(xr.at[2, es], ar2.at[nr(slot, n), 0])
                acc[es, to, c] += xr[2, es]
                remote(acc.at[es, to, c], xr.at[h, es], s_x.at[nr(slot, n)], ar2.at[nr(slot, n), 1], left if h else right).start()

    def sum_home(units):
        for slot, h, n in units:
            @pl.when(n <= lims[slot])
            def _(slot=slot, h=h, n=n):
                landed(xr.at[pl.ds(0, 2), ents(slot, n)], ar2.at[nr(slot, n), 1])
                go_home(slot, n, (0, 1))

    at = [half(n // 2, n % 2) for n in range(HALVES)]
    swap = lut(place, SWAP)
    last_but_one = [(slot, slot, 2 + swap) for slot in range(2)]
    last = [(slot, 0, 3 - swap) for slot in range(2)]
    FROM = (12, 8, 2, 0, 4 + 2 * swap, 6 - 2 * swap)
    CORE = (at[7] + at[6], at[5] + at[4], at[1], at[0], last_but_one, (), (), last)
    two = lims[1] >= 0
    one = jnp.logical_not(two)
    HOOKS = (
        (), ((sum_x, at[7] + at[6], None),), ((sum_x, at[5] + at[4], None),), ((sum_x2, at[7] + at[6], None), (sum_x, at[1], None)),
        ((sum_x2, at[5] + at[4], one), (sum_x, at[0], None)), ((sum_home, at[7] + at[6], None), (sum_x2, at[1], one)),
        ((sum_direct, last_but_one, one),), ((sum_x2, at[0], one), (sum_home, at[5] + at[4], None)))
    AFTER = (None, None, None, (sum_x2, at[4]), (sum_x2, at[1]), (sum_x, last_but_one), (sum_x2, at[0]), None)

    def segment(back):
        lo = sel(jnp.minimum(back, 5), FROM)
        hi = lo + jnp.where(back < 2, 4, 2)
        steps = sums([jnp.where((back < 5) | (back == 5 + t // 2), upto(t, lo, hi), 0) for t in range(6)])

        def dec(i):
            t = tile_of(i, steps)
            ch = lo + i - sel(t, steps[:6])
            k = jnp.minimum(lo // 4, 2)
            where = sel(k, [begin[n] + sel(t, part[n][:6]) - EDGES[n] for n in range(3)])
            return t, ch, sel(t, ebase) + ch, where + ch
        return steps[6], dec

    def d_step(u, t, ch, e, si):
        dp_ref[u % 2] = dot(values(e), dot_t[t])

    skip = segment(0)[0] == 0
    d_step(0, *segment(skip.astype(jnp.int32))[1](0))

    @pl.loop(0, 8)
    def _(back):
        count, dec = segment(back)
        _, dec_next = segment(jnp.minimum(back + 1, 7))

        def between():
            def all_of(n):
                def run_all():
                    for job, units, who in HOOKS[n]:
                        if who is None:
                            job(units)
                        else:
                            pl.when(who)(lambda job=job, units=units: job(units))
                return run_all if HOOKS[n] else None
            dispatch(back, [all_of(n) for n in range(8)])

        def g_step(i, u, ahead, after):
            t, ch, e, si = dec(i)
            pr = jnp.exp2(sub8(sc[si], mst[t]))
            prb = pr.reshape(CK, ROWS).astype(BF)
            acc[e, :, :, :, HEAD:] += dot(prb, dor[t]).reshape(4, 2, BLK, HEAD)
            ahead()
            ds = (pr * sub8(dp_ref[u % 2], dst[t])).reshape(CK, ROWS).astype(BF)
            ot[t] += dot_tn(keys(e), ds)
            acc[e, :, :, :, :HEAD] += dot(ds, qn[t]).reshape(4, 2, BLK, HEAD)
            after()

        def nothing():
            pass

        @pl.when(count > 0)
        def _():
            run(count, lambda i, b, u, w: g_step(i, u, lambda: d_step(u + 1, *dec(i + 1)), nothing),
                lambda i, b, u, w: g_step(i, u, nothing, lambda: d_step(0, *dec_next(0))), between)
        @pl.when(two)
        def _():
            dispatch(back, [AFTER[n] and (lambda n=n: AFTER[n][0](AFTER[n][1])) for n in range(8)])

        def core_of(n):
            return (lambda: sum_core(CORE[n])) if CORE[n] else None
        dispatch(back, [core_of(n) for n in range(8)])

        def turn_back(g, tl):
            t = 2 * g + tl
            qn[t] = turn((ot[t] * SCALE).T, csr[t], -1)
            dev = device(sel(t, pos) // 2, x, sel(t, par))
            send(qn.at[t], gq.at[sel(g, seq_g)], os_.at[t], or_, dev, me)

        @pl.when(back == 3)
        def _():
            @pl.loop(0, 3)
            def _(g):
                @pl.when(sel(g, nch[::2]) <= 4)
                def _():
                    turn_back(g, 0)

        @pl.when(back >= 5)
        def _():
            g = back - 5

            @pl.when(sel(g, nch[::2]) > 4)
            def _():
                turn_back(g, 0)
            turn_back(g, 1)

    @pl.when(two)
    def _():
        sum_x2(last_but_one)
    sum_direct(last)
    sum_home(at[1])
    sum_home(at[0])
    for s in range(SEQS):
        _, _, dev = work_of(s)

        @pl.when(dev != me)
        def _(s=s):
            landed(q.at[pl.ds(0, 2)], ts.at[s, 0])
            landed(csl, ts.at[s, 1])
    @pl.when(two)
    def _():
        sum_home(last_but_one)

    @pl.when(one)
    def _():
        home_direct(last_but_one)
    home_direct(last)
    landed_many(zs, N_HOME, ar3)
    for s in range(SEQS):
        for m, (chip, slot, last) in enumerate(CHIPS[s]):
            @pl.when(half_me > last)
            def _(s=s, m=m):
                home[s, m] = jnp.zeros((BLK, TWO), F32)
        total = home[s, 0]
        for m in range(1, len(CHIPS[s])):
            total = total + home[s, m]
        dk = total[:, :HEAD] * SCALE
        other = jnp.concatenate([dk[:, HH:], dk[:, :HH]], axis=1)
        gk[s] = (dk * cos - other * sin).astype(BF)
        gv[s] = total[:, HEAD:].astype(BF)

    landed(sc.at[pl.ds(0, 3)], or_)
    for slot in range(2):
        @pl.loop(0, lims[slot] + 1)
        def _(n, slot=slot):
            landed(peer.at[ents(slot, n)], s_core.at[nr(slot, n)])
            landed(xr.at[:, ents(slot, n)], s_x.at[nr(slot, n)])
    landed_many(zs, N_SUMS, s_one)
    for t in range(6):
        @pl.when(pos[t] != p)
        def _(t=t):
            landed(qraw.at[pl.ds(0, 2)], os_.at[t])


def run_whole(q, do, key, value, pos32, freq):
    dma = pltpu.SemaphoreType.DMA
    nh = ENT // HALF
    any_ = pl.BlockSpec(memory_space=pl.ANY)
    vm = pl.BlockSpec(memory_space=pltpu.VMEM)
    v = pltpu.VMEM
    return pl.pallas_call(
        whole_step,
        in_specs=[any_] * 5 + [vm], out_specs=[vm] * 4,
        out_shape=[v((6, ROWS, HEAD), BF), v((6, ROWS, HEAD), BF), v((6, BLK, HEAD), BF), v((6, BLK, HEAD), BF)],
        scratch_shapes=[
            v((6, ROWS, HEAD), BF), v((6, ROWS, HEAD), BF), v((6, BLK, HEAD), F32), v((ENT, 4, 2, BLK, TWO), BF),
            v((6, ROWS, HEAD), BF), v((6, HEAD, ROWS), BF), v((6, HEAD, ROWS), BF), v((HEAD, ROWS), BF), v((3, CK, HEAD), BF),
            v((SIDX, CK, ROWS), F32), v((SIDX, 8, ROWS), F32), v((6, 8, ROWS), F32), v((6, 8, ROWS), F32), v((6, 8, ROWS), F32),
            v((6, HEAD, ROWS), F32), v((2, CK, ROWS), F32), v((BLK, HEAD), F32),
            v((ENT, 4, 2, BLK, TWO), F32), v((ENT, 4, BLK, TWO), F32), v((3, ENT, BLK, TWO), F32), v((ENT, BLK, TWO), F32),
            v((SEQS, NCH, BLK, TWO), F32), v((SEQS, BLK, HEAD), BF), v((SEQS, BLK, TWO), BF), pltpu.SMEM((BLK,), jnp.int32),
            dma((nh,)), dma((nh, 2)), dma((nh,)), dma((6, 2)), dma((6, 3)), dma((6,)), dma((nh,)), dma((nh, 2)),
            dma(()), dma((nh,)), dma((nh,)), dma(()), dma(()), dma((3,))],
        compiler_params=pltpu.CompilerParams(has_side_effects=True, collective_id=0, vmem_limit_bytes=62500000),
        name='whole_step')(q, do, key, value, pos32, pltpu.with_memory_space_constraint(freq, pltpu.VMEM))


def put(*refs):
    here, there, sem = refs[:4], refs[4:8], refs[8]
    copies = [pltpu.make_async_copy(a, b, sem.at[n]) for n, (a, b) in enumerate(zip(here, there))]
    for copy in copies:
        copy.start()
    for copy in copies:
        copy.wait()


def run_put(*arrays):
    any_ = pl.BlockSpec(memory_space=pl.ANY)
    return pl.pallas_call(
        put, in_specs=[any_] * 4, out_specs=[any_] * 4,
        out_shape=[jax.ShapeDtypeStruct(a.shape, a.dtype) for a in arrays],
        scratch_shapes=[pltpu.SemaphoreType.DMA((4,))], name='put')(*[pltpu.with_memory_space_constraint(a, pltpu.VMEM) for a in arrays])


def solution(mesh):
    query_spec = PS('dp', 'cp', None, None)
    kv_spec = PS('dp', 'cp', None)
    pos_spec = PS(('dp', 'cp'))

    def per_device(query, key, value, positions, grad_out):
        inv_freq = jnp.power(jnp.float32(ROPE_BASE), -2.0 * jnp.arange(HH, dtype=F32) / HEAD)
        att, gq, gk, gv = run_whole(query.reshape(6, ROWS, HEAD), grad_out.reshape(6, ROWS, HEAD), key, value, positions, inv_freq[None])
        att, gq, gk, gv = run_put(att, gq, gk, gv)
        return att.reshape(query.shape), gq.reshape(query.shape), gk, gv

    return jax.shard_map(per_device, mesh=mesh, in_specs=(query_spec, kv_spec, kv_spec, pos_spec, query_spec),
                         out_specs=(query_spec, query_spec, kv_spec, kv_spec), check_vma=False)
```

```python
import jax
import jax.numpy as jnp
from jax import lax
from jax.experimental import pallas as pl
from jax.experimental.pallas import tpu as pltpu
from jax.sharding import PartitionSpec as PS

ROPE_BASE = 10000
SEQS, HEADS, HEAD, BLK = 6, 16, 128, 32
ROWS = BLK * HEADS
CK = 256
ENT = 20
SLOT1 = 10
SIDX = 55
SCALE = HEAD ** -0.5
C2 = SCALE * 1.4426950408889634
BIG = 1e30
HH, TWO = HEAD // 2, 2 * HEAD
BF, F32 = jnp.bfloat16, jnp.float32
MESH = pl.DeviceIdType.MESH

PLACE = [int(d, 16) for d in 'E47B1560328CDA9F']
ORDER = [[int(d, 16) for d in row] for row in (
    '5423018967BAFECD',
    'EF8967BA542301DC',
    'CDFEBA9854760123',
    '1076982345BAFEDC',
    'FE1076893245BACD',
    'CDFEBA8945671032')]
PIECES = 4
PP = 16 // PIECES
HALF = PP // 2
HALVES = 16 // HALF


def _tables():
    work = {}
    dest = [[0] * 16 for _ in range(SEQS)]
    limit = {}
    slots = {}
    for s in range(SEQS):
        for i, j in enumerate(ORDER[s]):
            q = 16 * (s % 3) + i
            f, core, g = q // 6, q % 2, q % 6 // 2
            big_c = 8 * (s // 3) + f
            slot = s % 3 - (6 * f) // 16
            slots[big_c, s] = slot
            work[PLACE[big_c], core, g] = (s, j, slot)
            dest[s][j] = PLACE[big_c] * 8 + core * 4 + g
            limit[big_c, s] = max(limit.get((big_c, s), 0), ((31 - j) // 2) // HALF)
    chips = [[(PLACE[c], slots[c, t], limit[c, t]) for (c, t) in sorted(slots) if t == s] for s in range(SEQS)]
    lim = [[-1] * 16, [-1] * 16]
    seq = [[0] * 16, [0] * 16]
    nth = [[0] * 16, [0] * 16]
    for s in range(SEQS):
        for n, (place, slot, last) in enumerate(chips[s]):
            lim[slot][place], seq[slot][place], nth[slot][place] = last, s, n
    meta = []
    for p in range(32):
        w = [work[p // 2, p % 2, g] for g in range(3)]
        meta.append([t[1] for t in w] + [t[2] for t in w] + [2 if lim[1][p // 2] >= 0 else 1] + [t[0] for t in w])
    return dest, chips, lim, seq, nth, meta


DEST, CHIPS, LIM, SEQ, NTH, META = _tables()
SWAP = [PLACE.index(n) // 8 for n in range(16)]
N_HOME = [sum(n // HALF <= last for row in CHIPS for _, _, last in row) for n in range(16)]
N_KV = [N_HOME[n] - sum(n // HALF <= last for row in CHIPS for chip, _, last in row if chip == n) for n in range(16)]
N_SUMS = [sum(HALF * (row[n] + 1) - (n < HALF * (row[n] + 1)) for row in LIM) for n in range(16)]
NCH = max(len(c) for c in CHIPS)


def lut(index, table):
    value = jnp.int32(table[0])
    for n in range(1, len(table)):
        if table[n] != table[n - 1]:
            value = jnp.where(index >= n, jnp.int32(table[n]), value)
    return value


def device(place, x, core):
    return place * 8 + 2 * x + core


def dispatch(i, jobs, first=0):
    if len(jobs) == 1:
        jobs[0]()
        return
    cut = len(jobs) // 2
    for part, at, test in ((jobs[:cut], first, i < first + cut), (jobs[cut:], first + cut, i >= first + cut)):
        if any(part):
            @pl.when(test)
            def _(part=part, at=at):
                dispatch(i, part, at)


def place_of():
    me = lax.axis_index('cp')
    return me, me % 2, (me // 2) % 4, me // 8


def send(src, dst, ssem, rsem, dev, me):
    @pl.when(dev != me)
    def _():
        pltpu.make_async_remote_copy(src, dst, ssem, rsem, device_id={'cp': dev}, device_id_type=MESH).start()

    @pl.when(dev == me)
    def _():
        pltpu.make_async_copy(src, dst, rsem).start()


def dot(a, b):
    return jnp.dot(a, b, preferred_element_type=F32)


def dot_tn(a, b):
    return lax.dot_general(a, b, (((0,), (0,)), ((), ())), preferred_element_type=F32)


def max8(v):
    return jnp.broadcast_to(jnp.max(v, axis=0, keepdims=True), (8, ROWS))


def sum8(v):
    return jnp.broadcast_to(jnp.sum(v, axis=0, keepdims=True), (8, ROWS))


def sub8(a, b):
    return a.reshape(-1, 8, ROWS) - b[None]


def turn(v, cs, sign):
    cos = jnp.concatenate([cs[:, :HH], cs[:, :HH]], axis=1)
    sin = jnp.concatenate([-cs[:, HH:], cs[:, HH:]], axis=1)
    v = v.reshape(BLK, HEADS, HEAD)
    other = jnp.concatenate([v[..., HH:], v[..., :HH]], axis=-1)
    if sign > 0:
        out = v * cos[:, None, :] + other * sin[:, None, :]
    else:
        out = v * cos[:, None, :] - other * sin[:, None, :]
    return out.astype(BF).reshape(ROWS, HEAD)


def nr(slot, n):
    return SLOT1 // HALF * slot + n


def landed(ref, sem):
    pltpu.make_async_copy(ref, ref, sem).wait()


def sel(t, values):
    out = values[0] + jnp.int32(0)
    for k in range(1, len(values)):
        out = jnp.where(t == k, values[k], out)
    return out


def whole_step(q, do, key, value, pos32, freq, att, gq, gk, gv,
               qraw, dor, csr, kvr, qn, qa, dot_t, hot, mk, sc, mx, mst, lst, dst, ot, dp_ref, csl,
               acc, peer, xr, zs, home, keyl, kv, posl,
               kr1, kr2, kr3, ts, tr, os_, ar1, ar2, s_one, s_x, s_core, or_, ar3, kl):
    me, c, x, place = place_of()
    p = 2 * place + c
    jme = jnp.minimum(p, 31 - p)
    hi = p // 16
    lims = [lut(place, LIM[slot]) for slot in range(2)]
    seqs = [lut(place, SEQ[slot]) for slot in range(2)]
    nths = [lut(place, NTH[slot]) for slot in range(2)]
    half_me = place // HALF
    jg = [lut(p, [META[n][g] for n in range(len(META))]) for g in range(3)]
    slot_g = [lut(p, [META[n][3 + g] for n in range(len(META))]) for g in range(3)]
    seq_g = [lut(p, [META[n][7 + g] for n in range(len(META))]) for g in range(3)]
    pos = [v for g in range(3) for v in (jg[g], 31 - jg[g])]
    nch = [v // 2 + 1 for v in pos]
    par = [v % 2 for v in pos]
    ebase = [SLOT1 * slot_g[t // 2] for t in range(6)]
    partner = me + 1 - 2 * c

    def landed_many(ref, counts, sem):
        many = lut(place, counts)
        for k in sorted(set(counts)):
            @pl.when(many == k)
            def _(k=k):
                landed(ref.at[pl.ds(0, k)], sem)

    def remote(src, dst, ssem, rsem, dev):
        return pltpu.make_async_remote_copy(src, dst, ssem, rsem, device_id={'cp': dev}, device_id_type=MESH)

    fetch = [pltpu.make_async_copy(pos32, posl, kl.at[2]), pltpu.make_async_copy(key, keyl, kl.at[0]),
             pltpu.make_async_copy(value, kv.at[:, :, HEAD:], kl.at[1])]
    for copy in fetch:
        copy.start()
    barrier = pltpu.get_barrier_semaphore()

    def greet(dev):
        pl.semaphore_signal(barrier, inc=1, device_id={'cp': dev}, device_id_type=MESH)

    @pl.loop(0, 16)
    def _(other):
        greet(device(other, x, 1 - c))

        @pl.when(other != place)
        def _():
            greet(device(other, x, c))
    for d in range(1, 4):
        greet(device(place, (x + d) % 4, c))
    for copy in fetch:
        copy.wait()
    inv = freq[...]
    for t in range(BLK):
        csl[t:t + 1, :HH] = posl[t].astype(F32) * inv
    ang = csl[:, :HH]
    csl[:, :HH] = jnp.cos(ang)
    csl[:, HH:] = jnp.sin(ang)
    tab = csl[...]
    cos = jnp.concatenate([tab[:, :HH], tab[:, :HH]], axis=1)
    sin = jnp.concatenate([-tab[:, HH:], tab[:, HH:]], axis=1)
    for s in range(SEQS):
        kf = keyl[s].astype(F32)
        kv[s, :, :HEAD] = (kf * cos + jnp.concatenate([kf[:, HH:], kf[:, :HH]], axis=1) * sin).astype(BF)
    pl.semaphore_wait(barrier, 34)

    def work_of(s):
        code = lut(jme, DEST[s])
        return code % 4, 2 * (code % 4) + hi, device(code // 8, x, (code // 4) % 2)

    def send_q():
        for g in range(3):
            for s in range(SEQS):
                when, k, dev = work_of(s)

                @pl.when(when == g)
                def _(s=s, k=k, dev=dev):
                    send(q.at[s], qraw.at[k], ts.at[s, 0], tr.at[k, 0], dev, me)
                    send(csl, csr.at[k], ts.at[s, 1], tr.at[k, 1], dev, me)

    def send_do():
        for s in range(SEQS):
            _, k, dev = work_of(s)
            send(do.at[s], dor.at[k], ts.at[s, 0], tr.at[k, 2], dev, me)

    for s in range(SEQS):
        for (chip, slot, last) in CHIPS[s]:
            @pl.when(half_me <= last)
            def _(s=s, chip=chip, slot=slot):
                send(kv.at[s], kvr.at[SLOT1 * slot + place, x, c], s_one, kr1.at[nr(slot, half_me)], device(chip, x, c), me)
    send_q()

    @pl.loop(0, ENT)
    def _(e):
        acc[e] = jnp.zeros((4, 2, BLK, TWO), F32)
    row = lax.broadcasted_iota(jnp.int32, (HEAD, ROWS), 0)
    col = lax.broadcasted_iota(jnp.int32, (HEAD, ROWS), 1)
    hot[...] = jnp.where(col // HEADS == row, 1.0, 0.0).astype(BF)
    ki = lax.broadcasted_iota(jnp.int32, (CK, HEAD), 0)
    di = lax.broadcasted_iota(jnp.int32, (CK, HEAD), 1)
    mk[0] = jnp.zeros((CK, HEAD), BF)
    for cc in range(2):
        mk[1 + cc] = jnp.where((di < BLK) & (ki > di + 64 * x + BLK * cc), -BIG, 0.0).astype(BF)

    @pl.loop(0, 6)
    def _(t):
        ot[t] = jnp.zeros((HEAD, ROWS), F32)
        mst[t] = jnp.full((8, ROWS), -BIG, F32)
        lst[t] = jnp.zeros((8, ROWS), F32)

    right = device(place, (x + 1) % 4, c)
    left = device(place, (x + 3) % 4, c)

    def halves(i):
        return [u for h in range(2) for u in half(i, h)]

    def half(i, h):
        slots = 1 if isinstance(i, int) and HALF * (2 * i + h) >= SLOT1 else 2
        return [(slot, (h + slot) % 2, 2 * i + h) for slot in range(slots)]


    def ents(slot, n):
        return pl.ds(SLOT1 * slot + HALF * n, HALF)

    def relay_x(i):
        for slot, h, n in halves(i):
            @pl.when(n <= lims[slot])
            def _(slot=slot, n=n):
                mine = kvr.at[ents(slot, n), x, c]
                landed(mine, kr1.at[nr(slot, n)])
                remote(mine, mine, s_x.at[nr(slot, n)], kr2.at[nr(slot, n), 0], right).start()
                remote(mine, mine, s_x.at[nr(slot, n)], kr2.at[nr(slot, n), 1], left).start()

    def relay_x2(i):
        for slot, h, n in halves(i):
            @pl.when(n <= lims[slot])
            def _(slot=slot, h=h, n=n):
                theirs = kvr.at[ents(slot, n), (x + 3 - 2 * h) % 4, c]
                landed(theirs, kr2.at[nr(slot, n), h])
                remote(theirs, theirs, s_x.at[nr(slot, n)], kr2.at[nr(slot, n), 1 - h], left if h else right).start()

    def relay_core(i):
        for slot, h, n in halves(i):
            @pl.when(n <= lims[slot])
            def _(slot=slot, h=h, n=n):
                landed(kvr.at[ents(slot, n), pl.ds(0, 2), c], kr2.at[nr(slot, n), 1 - h])
                both = kvr.at[ents(slot, n), :, c]
                remote(both, both, s_core.at[nr(slot, n)], kr3.at[nr(slot, n)], partner).start()

    relay_x(0)
    relay_x(1)
    relay_x2(0)
    relay_x(2)
    relay_core(0)
    relay_x2(1)
    relay_x(3)

    def prep_q(t):
        landed(qraw.at[t], tr.at[t, 0])
        landed(csr.at[t], tr.at[t, 1])
        rq = turn(qraw[t].astype(F32), csr[t], 1)
        qn[t] = rq
        qa[t] = rq.T

    def upto(t, lo, hi):
        return jnp.minimum(jnp.maximum(nch[t] - lo, 0), hi - lo)

    def sums(counts):
        out = [jnp.int32(0)]
        for v in counts:
            out.append(out[-1] + v)
        return out

    def tile_of(i, ends):
        t = jnp.int32(0)
        for n in range(1, 6):
            t = t + (i >= ends[n]).astype(jnp.int32)
        return t

    EDGES = (0, 4, 8, 16)
    part = [sums([upto(t, EDGES[k], EDGES[k + 1]) for t in range(6)]) for k in range(3)]
    begin = sums([ends[6] for ends in part])

    def run(count, pair, last, between):
        eights = (count - 1) // 8
        rest = (count - 1) % 8

        def several(n, base):
            for u in range(n):
                pair(base + u, base, u, n + 1)

        @pl.loop(0, eights)
        def _(b):
            @pl.when(b == 1)
            def _():
                between()
            several(8, 8 * b)

        @pl.when(eights <= 1)
        def _():
            between()

        @pl.when(rest >= 4)
        def _():
            several(4, 8 * eights)
        base = 8 * eights + rest // 4 * 4
        for r in range(4):
            @pl.when(rest % 4 == r)
            def _(r=r):
                several(r, base)
                last(base + r, base, r, r + 1)

    def keys(e):
        return kvr[e, :, :, :, :HEAD].reshape(CK, HEAD)

    def values(e):
        return kvr[e, :, :, :, HEAD:].reshape(CK, HEAD)

    @pl.loop(0, 6)
    def _(t):
        prep_q(t)

    @pl.loop(0, 3)
    def _(k):
        @pl.when(k == 0)
        def _():
            send_do()

        @pl.when(k == 1)
        def _():
            relay_core(2)
            relay_core(3)
        for i in range(PIECES):
            for slot, h, n in halves(i):
                @pl.when((n <= lims[slot]) & (k == min(i, 2)))
                def _(slot=slot, n=n):
                    landed(kvr.at[ents(slot, n), :, 1 - c], kr3.at[nr(slot, n)])
        ends = [sel(k, [part[n][t] for n in range(3)]) for t in range(7)]
        start = sel(k, begin[:3])
        count = ends[6]

        def dec(i):
            t = tile_of(i, ends)
            ch = 4 * k + i - sel(t, ends[:6])
            return t, ch, sel(t, ebase) + ch

        def between():
            @pl.when(k == 0)
            def _():
                relay_x2(2)
                relay_core(1)
                relay_x2(3)

        def s_step(i, sb, u, w):
            t, ch, e = dec(i)
            mask = jnp.where(ch == sel(t, nch) - 1, 1 + sel(t, par), 0)
            ka = jnp.concatenate([keys(e), mk[mask]], axis=1)
            qh = jnp.concatenate([qa[t], hot[...]], axis=0)
            sv = dot(ka, qh) * C2
            sc.at[pl.ds(sb, w)][u] = sv
            mx.at[pl.ds(sb, w)][u] = jnp.max(sv.reshape(CK // 8, 8, ROWS), axis=0)

        def o_step(i, sb, u, w):
            t, ch, e = dec(i)
            mo = mst[t]
            mn = jnp.maximum(mo, max8(mx.at[pl.ds(sb, w)][u]))
            al = jnp.exp2(mo - mn)
            ev = jnp.exp2(sub8(sc.at[pl.ds(sb, w)][u], mn))
            mst[t] = mn
            lst[t] = lst[t] * al + jnp.sum(ev, axis=0)
            ot[t] = (ot[t].reshape(-1, 8, ROWS) * al[None]).reshape(HEAD, ROWS) + dot_tn(values(e), ev.reshape(CK, ROWS).astype(BF))

        def pair(i, b, u, w):
            s_step(i + 1, start + b, u + 1, w)
            o_step(i, start + b, u, w)

        @pl.when(count > 0)
        def _():
            s_step(jnp.int32(0), start, 0, 1)
            run(count, pair, lambda i, b, u, w: o_step(i, start + b, u, w), between)

    landed_many(mx, N_KV, s_one)
    for slot in range(2):
        @pl.loop(0, lims[slot] + 1)
        def _(n, slot=slot):
            landed(kvr.at[ents(slot, n), pl.ds(0, 3), c], s_x.at[nr(slot, n)])
            landed(kvr.at[ents(slot, n), :, c], s_core.at[nr(slot, n)])

    for t in range(6):
        landed(dor.at[t], tr.at[t, 2])
        dot_t[t] = dor[t].T
        l = sum8(lst[t])
        o = (ot[t].reshape(-1, 8, ROWS) / l[None]).reshape(HEAD, ROWS).astype(BF)
        qraw[t] = o.T
        dev = device(pos[t] // 2, x, par[t])
        send(qraw.at[t], att.at[seq_g[t // 2]], os_.at[t], or_, dev, me)
        dst[t] = sum8(jnp.sum((o.astype(F32) * dot_t[t].astype(F32)).reshape(-1, 8, ROWS), axis=0))
        mst[t] = mst[t] + jnp.log2(l)
        ot[t] = jnp.zeros((HEAD, ROWS), F32)

    def sum_core(units):
        for slot, h, n in units:
            @pl.when(n <= lims[slot])
            def _(slot=slot, n=n):
                remote(acc.at[ents(slot, n), :, 1 - c], peer.at[ents(slot, n)], s_core.at[nr(slot, n)], ar1.at[nr(slot, n)], partner).start()

    def sum_x(units):
        for slot, h, n in units:
            @pl.when(n <= lims[slot])
            def _(slot=slot, h=h, n=n):
                es = ents(slot, n)
                add_peer(slot, n)
                one, other = (left, right) if h else (right, left)
                remote(acc.at[es, (x + 2) % 4, c], xr.at[2, es], s_x.at[nr(slot, n)], ar2.at[nr(slot, n), 0], one).start()
                remote(acc.at[es, (x + 3 - 2 * h) % 4, c], xr.at[1 - h, es], s_x.at[nr(slot, n)], ar2.at[nr(slot, n), 1], other).start()

    def add_peer(slot, n):
        landed(peer.at[ents(slot, n)], ar1.at[nr(slot, n)])
        for v in range(HALF):
            e = SLOT1 * slot + HALF * n + v
            acc[e, :, c] += peer[e]

    def sum_direct(units):
        for slot, h, n in units:
            @pl.when(n <= lims[slot])
            def _(slot=slot, n=n):
                es = ents(slot, n)
                add_peer(slot, n)
                for d in range(3):
                    to = (x + d + 1) % 4
                    remote(acc.at[es, to, c], xr.at[d, es], s_x.at[nr(slot, n)], ar2.at[nr(slot, n), 1], device(place, to, c)).start()

    def home_direct(units):
        for slot, h, n in units:
            @pl.when(n <= lims[slot])
            def _(slot=slot, n=n):
                landed(xr.at[:, ents(slot, n)], ar2.at[nr(slot, n), 1])
                go_home(slot, n, (0, 1, 2))

    def go_home(slot, n, parts):
        for v in range(HALF):
            to = HALF * n + v
            e = SLOT1 * slot + to
            total = acc[e, x, c]
            for d in parts:
                total = total + xr[d, e]
            zs[e] = total
            send(zs.at[e], home.at[seqs[slot], nths[slot]], s_one, ar3, device(to, x, c), me)

    def sum_x2(units):
        for slot, h, n in units:
            @pl.when(n <= lims[slot])
            def _(slot=slot, h=h, n=n):
                es = ents(slot, n)
                to = (x + 1 + 2 * h) % 4
                landed(xr.at[2, es], ar2.at[nr(slot, n), 0])
                acc[es, to, c] += xr[2, es]
                remote(acc.at[es, to, c], xr.at[h, es], s_x.at[nr(slot, n)], ar2.at[nr(slot, n), 1], left if h else right).start()

    def sum_home(units):
        for slot, h, n in units:
            @pl.when(n <= lims[slot])
            def _(slot=slot, h=h, n=n):
                landed(xr.at[pl.ds(0, 2), ents(slot, n)], ar2.at[nr(slot, n), 1])
                go_home(slot, n, (0, 1))

    at = [half(n // 2, n % 2) for n in range(HALVES)]
    swap = lut(place, SWAP)
    last_but_one = [(slot, slot, 2 + swap) for slot in range(2)]
    last = [(slot, 0, 3 - swap) for slot in range(2)]
    FROM = (12, 8, 2, 0, 4 + 2 * swap, 6 - 2 * swap)
    CORE = (at[7] + at[6], at[5] + at[4], at[1], at[0], last_but_one, (), (), last)
    two = lims[1] >= 0
    one = jnp.logical_not(two)
    HOOKS = (
        (), ((sum_x, at[7] + at[6], None),), ((sum_x, at[5] + at[4], None),), ((sum_x2, at[7] + at[6], None), (sum_x, at[1], None)),
        ((sum_x2, at[5] + at[4], one), (sum_x, at[0], None)), ((sum_home, at[7] + at[6], None), (sum_x2, at[1], one)),
        ((sum_direct, last_but_one, one), (sum_home, at[5] + at[4], None)), ((sum_x2, at[0], one),))
    AFTER = (None, None, None, (sum_x2, at[4]), (sum_x2, at[1]), (sum_x, last_but_one), (sum_x2, at[0]), None)

    def segment(back):
        lo = sel(jnp.minimum(back, 5), FROM)
        hi = lo + jnp.where(back < 2, 4, 2)
        steps = sums([jnp.where((back < 5) | (back == 5 + t // 2), upto(t, lo, hi), 0) for t in range(6)])

        def dec(i):
            t = tile_of(i, steps)
            ch = lo + i - sel(t, steps[:6])
            k = jnp.minimum(lo // 4, 2)
            where = sel(k, [begin[n] + sel(t, part[n][:6]) - EDGES[n] for n in range(3)])
            return t, ch, sel(t, ebase) + ch, where + ch
        return steps[6], dec

    def d_step(u, t, ch, e, si):
        dp_ref[u % 2] = dot(values(e), dot_t[t])

    skip = segment(0)[0] == 0
    d_step(0, *segment(skip.astype(jnp.int32))[1](0))

    @pl.loop(0, 8)
    def _(back):
        count, dec = segment(back)
        _, dec_next = segment(jnp.minimum(back + 1, 7))

        def between():
            def all_of(n):
                def run_all():
                    for job, units, who in HOOKS[n]:
                        if who is None:
                            job(units)
                        else:
                            pl.when(who)(lambda job=job, units=units: job(units))
                return run_all if HOOKS[n] else None
            dispatch(back, [all_of(n) for n in range(8)])

        def g_step(i, u, ahead, after):
            t, ch, e, si = dec(i)
            pr = jnp.exp2(sub8(sc[si], mst[t]))
            prb = pr.reshape(CK, ROWS).astype(BF)
            acc[e, :, :, :, HEAD:] += dot(prb, dor[t]).reshape(4, 2, BLK, HEAD)
            ahead()
            ds = (pr * sub8(dp_ref[u % 2], dst[t])).reshape(CK, ROWS).astype(BF)
            ot[t] += dot_tn(keys(e), ds)
            acc[e, :, :, :, :HEAD] += dot(ds, qn[t]).reshape(4, 2, BLK, HEAD)
            after()

        def nothing():
            pass

        @pl.when(count > 0)
        def _():
            run(count, lambda i, b, u, w: g_step(i, u, lambda: d_step(u + 1, *dec(i + 1)), nothing),
                lambda i, b, u, w: g_step(i, u, nothing, lambda: d_step(0, *dec_next(0))), between)
        @pl.when(two)
        def _():
            dispatch(back, [AFTER[n] and (lambda n=n: AFTER[n][0](AFTER[n][1])) for n in range(8)])

        def core_of(n):
            return (lambda: sum_core(CORE[n])) if CORE[n] else None
        dispatch(back, [core_of(n) for n in range(8)])

        def turn_back(g, tl):
            t = 2 * g + tl
            qn[t] = turn((ot[t] * SCALE).T, csr[t], -1)
            dev = device(sel(t, pos) // 2, x, sel(t, par))
            send(qn.at[t], gq.at[sel(g, seq_g)], os_.at[t], or_, dev, me)

        @pl.when(back == 3)
        def _():
            @pl.loop(0, 3)
            def _(g):
                @pl.when(sel(g, nch[::2]) <= 4)
                def _():
                    turn_back(g, 0)

        @pl.when(back >= 5)
        def _():
            g = back - 5

            @pl.when(sel(g, nch[::2]) > 4)
            def _():
                turn_back(g, 0)
            turn_back(g, 1)

    @pl.when(two)
    def _():
        sum_x2(last_but_one)
    sum_direct(last)
    sum_home(at[1])
    sum_home(at[0])
    for s in range(SEQS):
        _, _, dev = work_of(s)

        @pl.when(dev != me)
        def _(s=s):
            landed(q.at[pl.ds(0, 2)], ts.at[s, 0])
            landed(csl, ts.at[s, 1])
    @pl.when(two)
    def _():
        sum_home(last_but_one)

    @pl.when(one)
    def _():
        home_direct(last_but_one)
    home_direct(last)
    landed_many(zs, N_HOME, ar3)
    for s in range(SEQS):
        for m, (chip, slot, last) in enumerate(CHIPS[s]):
            @pl.when(half_me > last)
            def _(s=s, m=m):
                home[s, m] = jnp.zeros((BLK, TWO), F32)
        total = home[s, 0]
        for m in range(1, len(CHIPS[s])):
            total = total + home[s, m]
        dk = total[:, :HEAD] * SCALE
        other = jnp.concatenate([dk[:, HH:], dk[:, :HH]], axis=1)
        gk[s] = (dk * cos - other * sin).astype(BF)
        gv[s] = total[:, HEAD:].astype(BF)

    landed(sc.at[pl.ds(0, 3)], or_)
    for slot in range(2):
        @pl.loop(0, lims[slot] + 1)
        def _(n, slot=slot):
            landed(peer.at[ents(slot, n)], s_core.at[nr(slot, n)])
            landed(xr.at[:, ents(slot, n)], s_x.at[nr(slot, n)])
    landed_many(zs, N_SUMS, s_one)
    for t in range(6):
        @pl.when(pos[t] != p)
        def _(t=t):
            landed(qraw.at[pl.ds(0, 2)], os_.at[t])


def run_whole(q, do, key, value, pos32, freq):
    dma = pltpu.SemaphoreType.DMA
    nh = ENT // HALF
    any_ = pl.BlockSpec(memory_space=pl.ANY)
    vm = pl.BlockSpec(memory_space=pltpu.VMEM)
    v = pltpu.VMEM
    return pl.pallas_call(
        whole_step,
        in_specs=[any_] * 5 + [vm], out_specs=[vm] * 4,
        out_shape=[v((6, ROWS, HEAD), BF), v((6, ROWS, HEAD), BF), v((6, BLK, HEAD), BF), v((6, BLK, HEAD), BF)],
        scratch_shapes=[
            v((6, ROWS, HEAD), BF), v((6, ROWS, HEAD), BF), v((6, BLK, HEAD), F32), v((ENT, 4, 2, BLK, TWO), BF),
            v((6, ROWS, HEAD), BF), v((6, HEAD, ROWS), BF), v((6, HEAD, ROWS), BF), v((HEAD, ROWS), BF), v((3, CK, HEAD), BF),
            v((SIDX, CK, ROWS), F32), v((SIDX, 8, ROWS), F32), v((6, 8, ROWS), F32), v((6, 8, ROWS), F32), v((6, 8, ROWS), F32),
            v((6, HEAD, ROWS), F32), v((2, CK, ROWS), F32), v((BLK, HEAD), F32),
            v((ENT, 4, 2, BLK, TWO), F32), v((ENT, 4, BLK, TWO), F32), v((3, ENT, BLK, TWO), F32), v((ENT, BLK, TWO), F32),
            v((SEQS, NCH, BLK, TWO), F32), v((SEQS, BLK, HEAD), BF), v((SEQS, BLK, TWO), BF), pltpu.SMEM((BLK,), jnp.int32),
            dma((nh,)), dma((nh, 2)), dma((nh,)), dma((6, 2)), dma((6, 3)), dma((6,)), dma((nh,)), dma((nh, 2)),
            dma(()), dma((nh,)), dma((nh,)), dma(()), dma(()), dma((3,))],
        compiler_params=pltpu.CompilerParams(has_side_effects=True, collective_id=0, vmem_limit_bytes=62500000),
        name='whole_step')(q, do, key, value, pos32, pltpu.with_memory_space_constraint(freq, pltpu.VMEM))


def put(*refs):
    here, there, sem = refs[:4], refs[4:8], refs[8]
    copies = [pltpu.make_async_copy(a, b, sem.at[n]) for n, (a, b) in enumerate(zip(here, there))]
    for copy in copies:
        copy.start()
    for copy in copies:
        copy.wait()


def run_put(*arrays):
    any_ = pl.BlockSpec(memory_space=pl.ANY)
    return pl.pallas_call(
        put, in_specs=[any_] * 4, out_specs=[any_] * 4,
        out_shape=[jax.ShapeDtypeStruct(a.shape, a.dtype) for a in arrays],
        scratch_shapes=[pltpu.SemaphoreType.DMA((4,))], name='put')(*[pltpu.with_memory_space_constraint(a, pltpu.VMEM) for a in arrays])


def solution(mesh):
    query_spec = PS('dp', 'cp', None, None)
    kv_spec = PS('dp', 'cp', None)
    pos_spec = PS(('dp', 'cp'))

    def per_device(query, key, value, positions, grad_out):
        inv_freq = jnp.power(jnp.float32(ROPE_BASE), -2.0 * jnp.arange(HH, dtype=F32) / HEAD)
        att, gq, gk, gv = run_whole(query.reshape(6, ROWS, HEAD), grad_out.reshape(6, ROWS, HEAD), key, value, positions, inv_freq[None])
        att, gq, gk, gv = run_put(att, gq, gk, gv)
        return att.reshape(query.shape), gq.reshape(query.shape), gk, gv

    return jax.shard_map(per_device, mesh=mesh, in_specs=(query_spec, kv_spec, kv_spec, pos_spec, query_spec),
                         out_specs=(query_spec, query_spec, kv_spec, kv_spec), check_vma=False)
```

```python
import jax
import jax.numpy as jnp
from jax import lax
from jax.experimental import pallas as pl
from jax.experimental.pallas import tpu as pltpu
from jax.sharding import PartitionSpec as PS

ROPE_BASE = 10000
SEQS, HEADS, HEAD, BLK = 6, 16, 128, 32
ROWS = BLK * HEADS
CK = 256
ENT = 20
SLOT1 = 10
SIDX = 55
SCALE = HEAD ** -0.5
C2 = SCALE * 1.4426950408889634
BIG = 3e38
HH, TWO = HEAD // 2, 2 * HEAD
BF, F32 = jnp.bfloat16, jnp.float32
MESH = pl.DeviceIdType.MESH

PLACE = [int(d, 16) for d in 'E47B1560328CDA9F']
ORDER = [[int(d, 16) for d in row] for row in (
    '5423018967BAFECD',
    'EF8967BA542301DC',
    'CDFEBA9854760123',
    '1076982345BAFEDC',
    'FE1076893245BACD',
    'CDFEBA8945671032')]
PIECES = 4
PP = 16 // PIECES
HALF = PP // 2
HALVES = 16 // HALF


def _tables():
    work = {}
    dest = [[0] * 16 for _ in range(SEQS)]
    limit = {}
    slots = {}
    for s in range(SEQS):
        for i, j in enumerate(ORDER[s]):
            q = 16 * (s % 3) + i
            f, core, g = q // 6, q % 2, q % 6 // 2
            big_c = 8 * (s // 3) + f
            slot = s % 3 - (6 * f) // 16
            slots[big_c, s] = slot
            work[PLACE[big_c], core, g] = (s, j, slot)
            dest[s][j] = PLACE[big_c] * 8 + core * 4 + g
            limit[big_c, s] = max(limit.get((big_c, s), 0), ((31 - j) // 2) // HALF)
    chips = [[(PLACE[c], slots[c, t], limit[c, t]) for (c, t) in sorted(slots) if t == s] for s in range(SEQS)]
    lim = [[-1] * 16, [-1] * 16]
    seq = [[0] * 16, [0] * 16]
    nth = [[0] * 16, [0] * 16]
    for s in range(SEQS):
        for n, (place, slot, last) in enumerate(chips[s]):
            lim[slot][place], seq[slot][place], nth[slot][place] = last, s, n
    meta = []
    for p in range(32):
        w = [work[p // 2, p % 2, g] for g in range(3)]
        meta.append([t[1] for t in w] + [t[2] for t in w] + [2 if lim[1][p // 2] >= 0 else 1] + [t[0] for t in w])
    return dest, chips, lim, seq, nth, meta


DEST, CHIPS, LIM, SEQ, NTH, META = _tables()
SWAP = [PLACE.index(n) // 8 for n in range(16)]
N_HOME = [sum(n // HALF <= last for row in CHIPS for _, _, last in row) for n in range(16)]
N_KV = [N_HOME[n] - sum(n // HALF <= last for row in CHIPS for chip, _, last in row if chip == n) for n in range(16)]
N_SUMS = [sum(HALF * (row[n] + 1) - (n < HALF * (row[n] + 1)) for row in LIM) for n in range(16)]
NCH = max(len(c) for c in CHIPS)


def lut(index, table):
    value = jnp.int32(table[0])
    for n in range(1, len(table)):
        if table[n] != table[n - 1]:
            value = jnp.where(index >= n, jnp.int32(table[n]), value)
    return value


def device(place, x, core):
    return place * 8 + 2 * x + core


def dispatch(i, jobs, first=0):
    if len(jobs) == 1:
        jobs[0]()
        return
    cut = len(jobs) // 2
    for part, at, test in ((jobs[:cut], first, i < first + cut), (jobs[cut:], first + cut, i >= first + cut)):
        if any(part):
            @pl.when(test)
            def _(part=part, at=at):
                dispatch(i, part, at)


def place_of():
    me = lax.axis_index('cp')
    return me, me % 2, (me // 2) % 4, me // 8


def send(src, dst, ssem, rsem, dev, me):
    @pl.when(dev != me)
    def _():
        pltpu.make_async_remote_copy(src, dst, ssem, rsem, device_id={'cp': dev}, device_id_type=MESH).start()

    @pl.when(dev == me)
    def _():
        pltpu.make_async_copy(src, dst, rsem).start()


def dot(a, b):
    return jnp.dot(a, b, preferred_element_type=F32)


def dot_tn(a, b):
    return lax.dot_general(a, b, (((0,), (0,)), ((), ())), preferred_element_type=F32)


def max8(v):
    return jnp.broadcast_to(jnp.max(v, axis=0, keepdims=True), (8, ROWS))


def sum8(v):
    return jnp.broadcast_to(jnp.sum(v, axis=0, keepdims=True), (8, ROWS))


def sub8(a, b):
    return a.reshape(-1, 8, ROWS) - b[None]


def turn(v, cs, sign):
    cos = jnp.concatenate([cs[:, :HH], cs[:, :HH]], axis=1)
    sin = jnp.concatenate([-cs[:, HH:], cs[:, HH:]], axis=1)
    v = v.reshape(BLK, HEADS, HEAD)
    other = jnp.concatenate([v[..., HH:], v[..., :HH]], axis=-1)
    if sign > 0:
        out = v * cos[:, None, :] + other * sin[:, None, :]
    else:
        out = v * cos[:, None, :] - other * sin[:, None, :]
    return out.astype(BF).reshape(ROWS, HEAD)


def nr(slot, n):
    return SLOT1 // HALF * slot + n


def landed(ref, sem):
    pltpu.make_async_copy(ref, ref, sem).wait()


def sel(t, values):
    out = values[0] + jnp.int32(0)
    for k in range(1, len(values)):
        out = jnp.where(t == k, values[k], out)
    return out


def whole_step(q, do, key, value, pos32, freq, att, gq, gk, gv,
               qraw, dor, csr, kvr, qn, qa, dot_t, hot, mk, sc, mx, mst, lst, dst, ot, dp_ref, csl,
               acc, peer, xr, zs, home, keyl, kv, posl,
               kr1, kr2, kr3, ts, tr, os_, ar1, ar2, s_one, s_x, s_core, or_, ar3, kl):
    me, c, x, place = place_of()
    p = 2 * place + c
    jme = jnp.minimum(p, 31 - p)
    hi = p // 16
    lims = [lut(place, LIM[slot]) for slot in range(2)]
    seqs = [lut(place, SEQ[slot]) for slot in range(2)]
    nths = [lut(place, NTH[slot]) for slot in range(2)]
    half_me = place // HALF
    jg = [lut(p, [META[n][g] for n in range(len(META))]) for g in range(3)]
    slot_g = [lut(p, [META[n][3 + g] for n in range(len(META))]) for g in range(3)]
    seq_g = [lut(p, [META[n][7 + g] for n in range(len(META))]) for g in range(3)]
    pos = [v for g in range(3) for v in (jg[g], 31 - jg[g])]
    nch = [v // 2 + 1 for v in pos]
    par = [v % 2 for v in pos]
    ebase = [SLOT1 * slot_g[t // 2] for t in range(6)]
    partner = me + 1 - 2 * c

    def landed_many(ref, counts, sem):
        many = lut(place, counts)
        for k in sorted(set(counts)):
            @pl.when(many == k)
            def _(k=k):
                landed(ref.at[pl.ds(0, k)], sem)

    def remote(src, dst, ssem, rsem, dev):
        return pltpu.make_async_remote_copy(src, dst, ssem, rsem, device_id={'cp': dev}, device_id_type=MESH)

    fetch = [pltpu.make_async_copy(pos32, posl, kl.at[2]), pltpu.make_async_copy(key, keyl, kl.at[0]),
             pltpu.make_async_copy(value, kv.at[:, :, HEAD:], kl.at[1])]
    for copy in fetch:
        copy.start()
    barrier = pltpu.get_barrier_semaphore()

    def greet(dev):
        pl.semaphore_signal(barrier, inc=1, device_id={'cp': dev}, device_id_type=MESH)

    @pl.loop(0, 16)
    def _(other):
        greet(device(other, x, 1 - c))

        @pl.when(other != place)
        def _():
            greet(device(other, x, c))
    for d in range(1, 4):
        greet(device(place, (x + d) % 4, c))
    for copy in fetch:
        copy.wait()
    inv = freq[...]
    for t in range(BLK):
        csl[t:t + 1, :HH] = posl[t].astype(F32) * inv
    ang = csl[:, :HH]
    csl[:, :HH] = jnp.cos(ang)
    csl[:, HH:] = jnp.sin(ang)
    tab = csl[...]
    cos = jnp.concatenate([tab[:, :HH], tab[:, :HH]], axis=1)
    sin = jnp.concatenate([-tab[:, HH:], tab[:, HH:]], axis=1)
    for s in range(SEQS):
        kf = keyl[s].astype(F32)
        kv[s, :, :HEAD] = (kf * cos + jnp.concatenate([kf[:, HH:], kf[:, :HH]], axis=1) * sin).astype(BF)
    pl.semaphore_wait(barrier, 34)

    def work_of(s):
        code = lut(jme, DEST[s])
        return code % 4, 2 * (code % 4) + hi, device(code // 8, x, (code // 4) % 2)

    def send_q():
        for g in range(3):
            for s in range(SEQS):
                when, k, dev = work_of(s)

                @pl.when(when == g)
                def _(s=s, k=k, dev=dev):
                    send(q.at[s], qraw.at[k], ts.at[s, 0], tr.at[k, 0], dev, me)
                    send(csl, csr.at[k], ts.at[s, 1], tr.at[k, 1], dev, me)

    def send_do():
        for s in range(SEQS):
            _, k, dev = work_of(s)
            send(do.at[s], dor.at[k], ts.at[s, 0], tr.at[k, 2], dev, me)

    for s in range(SEQS):
        for (chip, slot, last) in CHIPS[s]:
            @pl.when(half_me <= last)
            def _(s=s, chip=chip, slot=slot):
                send(kv.at[s], kvr.at[SLOT1 * slot + place, x, c], s_one, kr1.at[nr(slot, half_me)], device(chip, x, c), me)
    send_q()

    @pl.loop(0, ENT)
    def _(e):
        acc[e] = jnp.zeros((4, 2, BLK, TWO), F32)
    row = lax.broadcasted_iota(jnp.int32, (HEAD, ROWS), 0)
    col = lax.broadcasted_iota(jnp.int32, (HEAD, ROWS), 1)
    hot[...] = jnp.where(col // HEADS == row, 1.0, 0.0).astype(BF)
    ki = lax.broadcasted_iota(jnp.int32, (CK, HEAD), 0)
    di = lax.broadcasted_iota(jnp.int32, (CK, HEAD), 1)
    mk[0] = jnp.zeros((CK, HEAD), BF)
    for cc in range(2):
        mk[1 + cc] = jnp.where((di < BLK) & (ki > di + 64 * x + BLK * cc), -BIG, 0.0).astype(BF)

    @pl.loop(0, 6)
    def _(t):
        ot[t] = jnp.zeros((HEAD, ROWS), F32)
        mst[t] = jnp.full((8, ROWS), -BIG, F32)
        lst[t] = jnp.zeros((8, ROWS), F32)

    right = device(place, (x + 1) % 4, c)
    left = device(place, (x + 3) % 4, c)

    def halves(i):
        return [u for h in range(2) for u in half(i, h)]

    def half(i, h):
        slots = 1 if isinstance(i, int) and HALF * (2 * i + h) >= SLOT1 else 2
        return [(slot, (h + slot) % 2, 2 * i + h) for slot in range(slots)]


    def ents(slot, n):
        return pl.ds(SLOT1 * slot + HALF * n, HALF)

    def relay_x(i):
        for slot, h, n in halves(i):
            @pl.when(n <= lims[slot])
            def _(slot=slot, n=n):
                mine = kvr.at[ents(slot, n), x, c]
                landed(mine, kr1.at[nr(slot, n)])
                remote(mine, mine, s_x.at[nr(slot, n)], kr2.at[nr(slot, n), 0], right).start()
                remote(mine, mine, s_x.at[nr(slot, n)], kr2.at[nr(slot, n), 1], left).start()

    def relay_x2(i):
        for slot, h, n in halves(i):
            @pl.when(n <= lims[slot])
            def _(slot=slot, h=h, n=n):
                theirs = kvr.at[ents(slot, n), (x + 3 - 2 * h) % 4, c]
                landed(theirs, kr2.at[nr(slot, n), h])
                remote(theirs, theirs, s_x.at[nr(slot, n)], kr2.at[nr(slot, n), 1 - h], left if h else right).start()

    def relay_core(i):
        for slot, h, n in halves(i):
            @pl.when(n <= lims[slot])
            def _(slot=slot, h=h, n=n):
                landed(kvr.at[ents(slot, n), pl.ds(0, 2), c], kr2.at[nr(slot, n), 1 - h])
                both = kvr.at[ents(slot, n), :, c]
                remote(both, both, s_core.at[nr(slot, n)], kr3.at[nr(slot, n)], partner).start()

    relay_x(0)
    relay_x(1)
    relay_x2(0)
    relay_x(2)
    relay_core(0)
    relay_x2(1)
    relay_x(3)

    def prep_q(t):
        landed(qraw.at[t], tr.at[t, 0])
        landed(csr.at[t], tr.at[t, 1])
        rq = turn(qraw[t].astype(F32), csr[t], 1)
        qn[t] = rq
        qa[t] = rq.T

    def upto(t, lo, hi):
        return jnp.minimum(jnp.maximum(nch[t] - lo, 0), hi - lo)

    def sums(counts):
        out = [jnp.int32(0)]
        for v in counts:
            out.append(out[-1] + v)
        return out

    def tile_of(i, ends):
        t = jnp.int32(0)
        for n in range(1, 6):
            t = t + (i >= ends[n]).astype(jnp.int32)
        return t

    EDGES = (0, 4, 8, 16)
    part = [sums([upto(t, EDGES[k], EDGES[k + 1]) for t in range(6)]) for k in range(3)]
    begin = sums([ends[6] for ends in part])

    def run(count, pair, last, between):
        eights = (count - 1) // 8
        rest = (count - 1) % 8

        def several(n, base):
            for u in range(n):
                pair(base + u, base, u, n + 1)

        @pl.loop(0, eights)
        def _(b):
            @pl.when(b == 1)
            def _():
                between()
            several(8, 8 * b)

        @pl.when(eights <= 1)
        def _():
            between()

        @pl.when(rest >= 4)
        def _():
            several(4, 8 * eights)
        base = 8 * eights + rest // 4 * 4
        for r in range(4):
            @pl.when(rest % 4 == r)
            def _(r=r):
                several(r, base)
                last(base + r, base, r, r + 1)

    def keys(e):
        return kvr[e, :, :, :, :HEAD].reshape(CK, HEAD)

    def values(e):
        return kvr[e, :, :, :, HEAD:].reshape(CK, HEAD)

    @pl.loop(0, 6)
    def _(t):
        prep_q(t)

    @pl.loop(0, 3)
    def _(k):
        @pl.when(k == 0)
        def _():
            send_do()

        @pl.when(k == 1)
        def _():
            relay_core(2)
            relay_core(3)
        for i in range(PIECES):
            for slot, h, n in halves(i):
                @pl.when((n <= lims[slot]) & (k == min(i, 2)))
                def _(slot=slot, n=n):
                    landed(kvr.at[ents(slot, n), :, 1 - c], kr3.at[nr(slot, n)])
        ends = [sel(k, [part[n][t] for n in range(3)]) for t in range(7)]
        start = sel(k, begin[:3])
        count = ends[6]

        def dec(i):
            t = tile_of(i, ends)
            ch = 4 * k + i - sel(t, ends[:6])
            return t, ch, sel(t, ebase) + ch

        def between():
            @pl.when(k == 0)
            def _():
                relay_x2(2)
                relay_core(1)
                relay_x2(3)

        def s_step(i, sb, u, w):
            t, ch, e = dec(i)
            mask = jnp.where(ch == sel(t, nch) - 1, 1 + sel(t, par), 0)
            ka = jnp.concatenate([keys(e), mk[mask]], axis=1)
            qh = jnp.concatenate([qa[t], hot[...]], axis=0)
            sv = dot(ka, qh) * C2
            sc.at[pl.ds(sb, w)][u] = sv
            mx.at[pl.ds(sb, w)][u] = jnp.max(sv.reshape(CK // 8, 8, ROWS), axis=0)

        def o_step(i, sb, u, w):
            t, ch, e = dec(i)
            mo = mst[t]
            mn = jnp.maximum(mo, max8(mx.at[pl.ds(sb, w)][u]))
            al = jnp.exp2(mo - mn)
            ev = jnp.exp2(sub8(sc.at[pl.ds(sb, w)][u], mn))
            mst[t] = mn
            lst[t] = lst[t] * al + jnp.sum(ev, axis=0)
            ot[t] = (ot[t].reshape(-1, 8, ROWS) * al[None]).reshape(HEAD, ROWS) + dot_tn(values(e), ev.reshape(CK, ROWS).astype(BF))

        def pair(i, b, u, w):
            s_step(i + 1, start + b, u + 1, w)
            o_step(i, start + b, u, w)

        @pl.when(count > 0)
        def _():
            s_step(jnp.int32(0), start, 0, 1)
            run(count, pair, lambda i, b, u, w: o_step(i, start + b, u, w), between)

    landed_many(mx, N_KV, s_one)
    for slot in range(2):
        @pl.loop(0, lims[slot] + 1)
        def _(n, slot=slot):
            landed(kvr.at[ents(slot, n), pl.ds(0, 3), c], s_x.at[nr(slot, n)])
            landed(kvr.at[ents(slot, n), :, c], s_core.at[nr(slot, n)])

    for t in range(6):
        landed(dor.at[t], tr.at[t, 2])
        dot_t[t] = dor[t].T
        l = sum8(lst[t])
        o = (ot[t].reshape(-1, 8, ROWS) / l[None]).reshape(HEAD, ROWS).astype(BF)
        qraw[t] = o.T
        dev = device(pos[t] // 2, x, par[t])
        send(qraw.at[t], att.at[seq_g[t // 2]], os_.at[t], or_, dev, me)
        dst[t] = sum8(jnp.sum((o.astype(F32) * dot_t[t].astype(F32)).reshape(-1, 8, ROWS), axis=0))
        mst[t] = mst[t] + jnp.log2(l)
        ot[t] = jnp.zeros((HEAD, ROWS), F32)

    def sum_core(units):
        for slot, h, n in units:
            @pl.when(n <= lims[slot])
            def _(slot=slot, n=n):
                remote(acc.at[ents(slot, n), :, 1 - c], peer.at[ents(slot, n)], s_core.at[nr(slot, n)], ar1.at[nr(slot, n)], partner).start()

    def sum_x(units):
        for slot, h, n in units:
            @pl.when(n <= lims[slot])
            def _(slot=slot, h=h, n=n):
                es = ents(slot, n)
                add_peer(slot, n)
                one, other = (left, right) if h else (right, left)
                remote(acc.at[es, (x + 2) % 4, c], xr.at[2, es], s_x.at[nr(slot, n)], ar2.at[nr(slot, n), 0], one).start()
                remote(acc.at[es, (x + 3 - 2 * h) % 4, c], xr.at[1 - h, es], s_x.at[nr(slot, n)], ar2.at[nr(slot, n), 1], other).start()

    def add_peer(slot, n):
        landed(peer.at[ents(slot, n)], ar1.at[nr(slot, n)])
        for v in range(HALF):
            e = SLOT1 * slot + HALF * n + v
            acc[e, :, c] += peer[e]

    def sum_direct(units):
        for slot, h, n in units:
            @pl.when(n <= lims[slot])
            def _(slot=slot, n=n):
                es = ents(slot, n)
                add_peer(slot, n)
                for d in range(3):
                    to = (x + d + 1) % 4
                    remote(acc.at[es, to, c], xr.at[d, es], s_x.at[nr(slot, n)], ar2.at[nr(slot, n), 1], device(place, to, c)).start()

    def home_direct(units):
        for slot, h, n in units:
            @pl.when(n <= lims[slot])
            def _(slot=slot, n=n):
                landed(xr.at[:, ents(slot, n)], ar2.at[nr(slot, n), 1])
                go_home(slot, n, (0, 1, 2))

    def go_home(slot, n, parts):
        for v in range(HALF):
            to = HALF * n + v
            e = SLOT1 * slot + to
            total = acc[e, x, c]
            for d in parts:
                total = total + xr[d, e]
            zs[e] = total
            send(zs.at[e], home.at[seqs[slot], nths[slot]], s_one, ar3, device(to, x, c), me)

    def sum_x2(units):
        for slot, h, n in units:
            @pl.when(n <= lims[slot])
            def _(slot=slot, h=h, n=n):
                es = ents(slot, n)
                to = (x + 1 + 2 * h) % 4
                landed(xr.at[2, es], ar2.at[nr(slot, n), 0])
                acc[es, to, c] += xr[2, es]
                remote(acc.at[es, to, c], xr.at[h, es], s_x.at[nr(slot, n)], ar2.at[nr(slot, n), 1], left if h else right).start()

    def sum_home(units):
        for slot, h, n in units:
            @pl.when(n <= lims[slot])
            def _(slot=slot, h=h, n=n):
                landed(xr.at[pl.ds(0, 2), ents(slot, n)], ar2.at[nr(slot, n), 1])
                go_home(slot, n, (0, 1))

    at = [half(n // 2, n % 2) for n in range(HALVES)]
    swap = lut(place, SWAP)
    last_but_one = [(slot, slot, 2 + swap) for slot in range(2)]
    last = [(slot, 0, 3 - swap) for slot in range(2)]
    FROM = (12, 8, 2, 0, 4 + 2 * swap, 6 - 2 * swap)
    CORE = (at[7] + at[6], at[5] + at[4], at[1], at[0], last_but_one, (), (), last)
    two = lims[1] >= 0
    one = jnp.logical_not(two)
    HOOKS = (
        (), ((sum_x, at[7] + at[6], None),), ((sum_x, at[5] + at[4], None),), ((sum_x2, at[7] + at[6], None), (sum_x, at[1], None)),
        ((sum_x2, at[5] + at[4], one), (sum_x, at[0], None)), ((sum_home, at[7] + at[6], None), (sum_x2, at[1], one)),
        ((sum_direct, last_but_one, one), (sum_home, at[5] + at[4], None)), ((sum_x2, at[0], one),))
    AFTER = (None, None, None, (sum_x2, at[4]), (sum_x2, at[1]), (sum_x, last_but_one), (sum_x2, at[0]), None)

    def segment(back):
        lo = sel(jnp.minimum(back, 5), FROM)
        hi = lo + jnp.where(back < 2, 4, 2)
        steps = sums([jnp.where((back < 5) | (back == 5 + t // 2), upto(t, lo, hi), 0) for t in range(6)])

        def dec(i):
            t = tile_of(i, steps)
            ch = lo + i - sel(t, steps[:6])
            k = jnp.minimum(lo // 4, 2)
            where = sel(k, [begin[n] + sel(t, part[n][:6]) - EDGES[n] for n in range(3)])
            return t, ch, sel(t, ebase) + ch, where + ch
        return steps[6], dec

    def d_step(u, t, ch, e, si):
        dp_ref[u % 2] = dot(values(e), dot_t[t])

    skip = segment(0)[0] == 0
    d_step(0, *segment(skip.astype(jnp.int32))[1](0))

    @pl.loop(0, 8)
    def _(back):
        count, dec = segment(back)
        _, dec_next = segment(jnp.minimum(back + 1, 7))

        def between():
            def all_of(n):
                def run_all():
                    for job, units, who in HOOKS[n]:
                        if who is None:
                            job(units)
                        else:
                            pl.when(who)(lambda job=job, units=units: job(units))
                return run_all if HOOKS[n] else None
            dispatch(back, [all_of(n) for n in range(8)])

        def g_step(i, u, ahead, after):
            t, ch, e, si = dec(i)
            pr = jnp.exp2(sub8(sc[si], mst[t]))
            prb = pr.reshape(CK, ROWS).astype(BF)
            acc[e, :, :, :, HEAD:] += dot(prb, dor[t]).reshape(4, 2, BLK, HEAD)
            ahead()
            ds = (pr * sub8(dp_ref[u % 2], dst[t])).reshape(CK, ROWS).astype(BF)
            ot[t] += dot_tn(keys(e), ds)
            acc[e, :, :, :, :HEAD] += dot(ds, qn[t]).reshape(4, 2, BLK, HEAD)
            after()

        def nothing():
            pass

        @pl.when(count > 0)
        def _():
            run(count, lambda i, b, u, w: g_step(i, u, lambda: d_step(u + 1, *dec(i + 1)), nothing),
                lambda i, b, u, w: g_step(i, u, nothing, lambda: d_step(0, *dec_next(0))), between)
        @pl.when(two)
        def _():
            dispatch(back, [AFTER[n] and (lambda n=n: AFTER[n][0](AFTER[n][1])) for n in range(8)])

        def core_of(n):
            return (lambda: sum_core(CORE[n])) if CORE[n] else None
        dispatch(back, [core_of(n) for n in range(8)])

        def turn_back(g, tl):
            t = 2 * g + tl
            qn[t] = turn((ot[t] * SCALE).T, csr[t], -1)
            dev = device(sel(t, pos) // 2, x, sel(t, par))
            send(qn.at[t], gq.at[sel(g, seq_g)], os_.at[t], or_, dev, me)

        @pl.when(back == 3)
        def _():
            @pl.loop(0, 3)
            def _(g):
                @pl.when(sel(g, nch[::2]) <= 4)
                def _():
                    turn_back(g, 0)

        @pl.when(back >= 5)
        def _():
            g = back - 5

            @pl.when(sel(g, nch[::2]) > 4)
            def _():
                turn_back(g, 0)
            turn_back(g, 1)

    @pl.when(two)
    def _():
        sum_x2(last_but_one)
    sum_direct(last)
    sum_home(at[1])
    sum_home(at[0])
    for s in range(SEQS):
        _, _, dev = work_of(s)

        @pl.when(dev != me)
        def _(s=s):
            landed(q.at[pl.ds(0, 2)], ts.at[s, 0])
            landed(csl, ts.at[s, 1])
    @pl.when(two)
    def _():
        sum_home(last_but_one)

    @pl.when(one)
    def _():
        home_direct(last_but_one)
    home_direct(last)
    landed_many(zs, N_HOME, ar3)
    for s in range(SEQS):
        for m, (chip, slot, last) in enumerate(CHIPS[s]):
            @pl.when(half_me > last)
            def _(s=s, m=m):
                home[s, m] = jnp.zeros((BLK, TWO), F32)
        total = home[s, 0]
        for m in range(1, len(CHIPS[s])):
            total = total + home[s, m]
        dk = total[:, :HEAD] * SCALE
        other = jnp.concatenate([dk[:, HH:], dk[:, :HH]], axis=1)
        gk[s] = (dk * cos - other * sin).astype(BF)
        gv[s] = total[:, HEAD:].astype(BF)

    landed(sc.at[pl.ds(0, 3)], or_)
    for slot in range(2):
        @pl.loop(0, lims[slot] + 1)
        def _(n, slot=slot):
            landed(peer.at[ents(slot, n)], s_core.at[nr(slot, n)])
            landed(xr.at[:, ents(slot, n)], s_x.at[nr(slot, n)])
    landed_many(zs, N_SUMS, s_one)
    for t in range(6):
        @pl.when(pos[t] != p)
        def _(t=t):
            landed(qraw.at[pl.ds(0, 2)], os_.at[t])


def run_whole(q, do, key, value, pos32, freq):
    dma = pltpu.SemaphoreType.DMA
    nh = ENT // HALF
    any_ = pl.BlockSpec(memory_space=pl.ANY)
    vm = pl.BlockSpec(memory_space=pltpu.VMEM)
    v = pltpu.VMEM
    return pl.pallas_call(
        whole_step,
        in_specs=[any_] * 5 + [vm], out_specs=[vm] * 4,
        out_shape=[v((6, ROWS, HEAD), BF), v((6, ROWS, HEAD), BF), v((6, BLK, HEAD), BF), v((6, BLK, HEAD), BF)],
        scratch_shapes=[
            v((6, ROWS, HEAD), BF), v((6, ROWS, HEAD), BF), v((6, BLK, HEAD), F32), v((ENT, 4, 2, BLK, TWO), BF),
            v((6, ROWS, HEAD), BF), v((6, HEAD, ROWS), BF), v((6, HEAD, ROWS), BF), v((HEAD, ROWS), BF), v((3, CK, HEAD), BF),
            v((SIDX, CK, ROWS), F32), v((SIDX, 8, ROWS), F32), v((6, 8, ROWS), F32), v((6, 8, ROWS), F32), v((6, 8, ROWS), F32),
            v((6, HEAD, ROWS), F32), v((2, CK, ROWS), F32), v((BLK, HEAD), F32),
            v((ENT, 4, 2, BLK, TWO), F32), v((ENT, 4, BLK, TWO), F32), v((3, ENT, BLK, TWO), F32), v((ENT, BLK, TWO), F32),
            v((SEQS, NCH, BLK, TWO), F32), v((SEQS, BLK, HEAD), BF), v((SEQS, BLK, TWO), BF), pltpu.SMEM((BLK,), jnp.int32),
            dma((nh,)), dma((nh, 2)), dma((nh,)), dma((6, 2)), dma((6, 3)), dma((6,)), dma((nh,)), dma((nh, 2)),
            dma(()), dma((nh,)), dma((nh,)), dma(()), dma(()), dma((3,))],
        compiler_params=pltpu.CompilerParams(has_side_effects=True, collective_id=0, vmem_limit_bytes=62500000),
        name='whole_step')(q, do, key, value, pos32, pltpu.with_memory_space_constraint(freq, pltpu.VMEM))


def put(*refs):
    here, there, sem = refs[:4], refs[4:8], refs[8]
    copies = [pltpu.make_async_copy(a, b, sem.at[n]) for n, (a, b) in enumerate(zip(here, there))]
    for copy in copies:
        copy.start()
    for copy in copies:
        copy.wait()


def run_put(*arrays):
    any_ = pl.BlockSpec(memory_space=pl.ANY)
    return pl.pallas_call(
        put, in_specs=[any_] * 4, out_specs=[any_] * 4,
        out_shape=[jax.ShapeDtypeStruct(a.shape, a.dtype) for a in arrays],
        scratch_shapes=[pltpu.SemaphoreType.DMA((4,))], name='put')(*[pltpu.with_memory_space_constraint(a, pltpu.VMEM) for a in arrays])


def solution(mesh):
    query_spec = PS('dp', 'cp', None, None)
    kv_spec = PS('dp', 'cp', None)
    pos_spec = PS(('dp', 'cp'))

    def per_device(query, key, value, positions, grad_out):
        inv_freq = jnp.power(jnp.float32(ROPE_BASE), -2.0 * jnp.arange(HH, dtype=F32) / HEAD)
        att, gq, gk, gv = run_whole(query.reshape(6, ROWS, HEAD), grad_out.reshape(6, ROWS, HEAD), key, value, positions, inv_freq[None])
        att, gq, gk, gv = run_put(att, gq, gk, gv)
        return att.reshape(query.shape), gq.reshape(query.shape), gk, gv

    return jax.shard_map(per_device, mesh=mesh, in_specs=(query_spec, kv_spec, kv_spec, pos_spec, query_spec),
                         out_specs=(query_spec, query_spec, kv_spec, kv_spec), check_vma=False)
```
